512 devices in a mesh: gx: 4 (over x), gy: 8 (over y), gz: 16 (over z, core).
Axes of the slice: x: 4, y: 8, z: 8, core: 2. Of those that a mesh axis runs over, the one named last changes fastest.
Arguments:
- right_side: float32 [32, 128, 2048], P('gx', 'gy', 'gz'), may hold values from -6 to 6
- conductance: float32 [32, 128, 2048], P('gx', 'gy', 'gz'), may hold values from 0.25 to 4
- extents: int32 [4, 8, 16], P('gx', 'gy', 'gz'), may hold values from 64 to 128, as said below
- coarse_factor: bfloat16 [512, 512], replicated, may hold values from -1 to 3, as said below
Outputs:
- solution_field: float32 [32, 128, 2048], P('gx', 'gy', 'gz')
- residual: float32 [32, 128, 2048], P('gx', 'gy', 'gz')
The draws below stay inside these ranges and needn't reach their ends.
Inputs may be any that keep to these rules, and one draw needn't show every extreme that they name: `extents`: cells of a block whose third local index is below its count are fluid, the others padding; in every draw some block has all 128 layers fluid. `coarse_factor`: lower triangular with a positive diagonal.
All inputs are finite; a program needn't handle non-finite values.
Results may differ from the reference program's by a relative error of at most 0.0003.
Values sent between devices are 32-bit elements; how exact they have to be, the bound alone decides.
No kernel may reach another device: no remote copies, remote signals or barrier semaphores. Data moves between devices by JAX's collectives and lax.ppermute only.
A program may use at most 64 MiB of HBM per device.

```python
import math
import jax
import jax.numpy as jnp
from jax import lax

CX = 8
CY = 16
CZ = 128
ITERS = 2
NX = 32
NY = 128
NZ = 2048
NB = 512
N_GX = 4
N_GY = 8
N_GZ = 16


def draw_right_side(key, part):
    key_cells, key_blocks = jax.random.split(jax.random.fold_in(key, 11), 2)
    blocks = (NX // CX, NY // CY, NZ // CZ)
    values = jnp.clip(jax.random.normal(key_cells, (NX, NY, NZ), jnp.float32), -4.0, 4.0)
    offsets = jax.random.uniform(key_blocks, blocks, jnp.float32, -1.5, 1.5)
    spread = jnp.repeat(jnp.repeat(jnp.repeat(offsets, CX, axis=0), CY, axis=1), CZ, axis=2)
    return values + spread


def draw_extents(key, part):
    key_counts, key_full = jax.random.split(jax.random.fold_in(key, 23))
    blocks = (NX // CX, NY // CY, NZ // CZ)
    counts = jax.random.randint(key_counts, blocks, CZ // 2, CZ + 1).reshape(-1)
    chosen = jax.random.randint(key_full, (), 0, counts.shape[0])
    counts = jnp.where(jnp.arange(counts.shape[0]) == chosen, CZ, counts)
    return counts.reshape(blocks).astype(jnp.int32)


def draw_coarse_factor(key, part):
    key_diag, key_low = jax.random.split(jax.random.fold_in(key, 37))
    diagonal = jax.random.uniform(key_diag, (NB,), jnp.float32, 1.0, 2.0)
    lower = jnp.clip(jax.random.normal(key_low, (NB, NB), jnp.float32), -6.0, 6.0)
    lower = jnp.tril(lower, -1) * (0.5 / math.sqrt(NB))
    return (lower + jnp.diag(diagonal)).astype(jnp.bfloat16)


def shard_levels(rng, shape, cuts, low, top_value):
    def one(axis_at, shards_of):
        steps = jax.random.uniform(jax.random.fold_in(jax.random.fold_in(rng, 6), axis_at), (shards_of,), jnp.float32, low / len(cuts), top_value / len(cuts))
        return jnp.repeat(jnp.exp(steps), shape[axis_at] // shards_of).reshape((-1,) + (1,) * (len(shape) - axis_at - 1))

    loudness = one(*cuts[0])
    for cut in cuts[1:]:
        loudness = loudness * one(*cut)
    return loudness


def setup_inputs(seed: int = 0) -> dict:
    streams_of = jax.random.split(jax.random.key(seed), 5)
    right_side = draw_right_side(jax.random.fold_in(streams_of[4], 71), 0)
    conductance = jnp.clip(jnp.exp(math.log(4.0) - 2.7725887 * jax.random.uniform(streams_of[1], (NX, NY, NZ), jnp.float32) ** shard_levels(streams_of[1], (NX, NY, NZ), ((0, 4), (1, 8), (2, 16)), -0.2, 0.2)), 0.25, 4.0)
    extents = draw_extents(jax.random.fold_in(streams_of[4], 71), 0)
    coarse_factor = draw_coarse_factor(jax.random.fold_in(streams_of[4], 71), 0)
    return dict(right_side=right_side, conductance=conductance, extents=extents, coarse_factor=coarse_factor)


OMEGA = 0.8

def neighbour_slices():
    inner = slice(1, -1)
    return [(slice(2, None), inner, inner), (slice(None, -2), inner, inner), (inner, slice(2, None), inner), (inner, slice(None, -2), inner), (inner, inner, slice(2, None)), (inner, inner, slice(None, -2))]

def face_terms(padded, cond_padded):
    centre = (slice(1, -1), slice(1, -1), slice(1, -1))
    value_mid = padded[centre]
    cond_mid = cond_padded[centre]
    summed = jnp.zeros_like(value_mid)
    for place in neighbour_slices():
        summed = summed + 0.5 * (cond_mid + cond_padded[place]) * (value_mid - padded[place])
    return summed

def coef_total(cond_padded):
    centre = (slice(1, -1), slice(1, -1), slice(1, -1))
    cond_mid = cond_padded[centre]
    summed = jnp.zeros_like(cond_mid)
    for place in neighbour_slices():
        summed = summed + 0.5 * (cond_mid + cond_padded[place])
    return summed

def pool_sum(field):
    first, second, third = field.shape
    return field.reshape(first // 2, 2, second // 2, 2, third // 2, 2).sum(axis=(1, 3, 5))

def pool_max(field):
    first, second, third = field.shape
    return field.reshape(first // 2, 2, second // 2, 2, third // 2, 2).max(axis=(1, 3, 5))

def expand(field):
    first, second, third = field.shape
    wide = jnp.broadcast_to(field[:, None, :, None, :, None], (first, 2, second, 2, third, 2))
    return wide.reshape(2 * first, 2 * second, 2 * third)

def make_level(cond_padded, fluid, scale):
    inverse = fluid / (scale * coef_total(cond_padded) + 1.0 - fluid)
    return (cond_padded, fluid, scale, inverse)

def apply_level(field, level):
    padded = jnp.pad(field, 1)
    return level[2] * level[1] * face_terms(padded, level[0])

def cycle(resid, levels, depth):
    level = levels[depth]
    first = OMEGA * level[3] * resid
    if depth == len(levels) - 1:
        return first
    image = apply_level(first, level)
    below = cycle(pool_sum(resid - image), levels, depth + 1)
    second = first + level[1] * expand(below)
    return second + OMEGA * level[3] * (resid - apply_level(second, level))

def reference(right_side, conductance, extents, coarse_factor):
    factor = coarse_factor.astype(jnp.float32)
    layer = lax.broadcasted_iota(jnp.int32, right_side.shape, 2) % CZ
    limit = jnp.repeat(jnp.repeat(jnp.repeat(extents, CX, axis=0), CY, axis=1), CZ, axis=2)
    fluid = (layer < limit).astype(jnp.float32)
    fluid_mid = pool_max(fluid)
    cond_mid = pool_sum(conductance) / 8.0
    levels = [make_level(jnp.pad(conductance, 1), fluid, 1.0), make_level(jnp.pad(cond_mid, 1), fluid_mid, 4.0)]
    block_cells = CX * CY * CZ

    def precondition(resid):
        smoothed = cycle(resid, levels, 0)
        means = resid.reshape(N_GX, CX, N_GY, CY, N_GZ, CZ).sum(axis=(1, 3, 5)).reshape(-1) / block_cells
        coarse = jax.scipy.linalg.cho_solve((factor, True), means)
        blockwise = coarse.reshape(N_GX, N_GY, N_GZ)
        spread = jnp.repeat(jnp.repeat(jnp.repeat(blockwise, CX, axis=0), CY, axis=1), CZ, axis=2)
        return smoothed + fluid * spread
    resid = fluid * right_side
    solution = jnp.zeros_like(resid)
    precond = precondition(resid)
    inner_now = jnp.sum(resid * precond)
    direction = precond
    for step in range(ITERS):
        image = apply_level(direction, levels[0])
        alpha = inner_now / jnp.sum(direction * image)
        solution = solution + alpha * direction
        resid = resid - alpha * image
        if step + 1 < ITERS:
            precond = precondition(resid)
            inner_next = jnp.sum(resid * precond)
            direction = precond + inner_next / inner_now * direction
            inner_now = inner_next
    return (solution, resid)
```

```python
import functools

import jax
import jax.numpy as jnp
from jax import lax
from jax.experimental import pallas as pl
from jax.experimental.pallas import tpu as pltpu
from jax.sharding import PartitionSpec as P

F32 = jnp.float32
OMEGA = 0.8
CX, CY, CZ = 8, 16, 128
CELLS = CX * CY * CZ
H = 8
EX, EY, EZ = CX + 2 * H, CY + 2 * H, 2 * CZ
SLOT = 16
VMEM = pl.BlockSpec(memory_space=pltpu.VMEM)
SMEM = pl.BlockSpec(memory_space=pltpu.SMEM)


def call(kernel, out_shapes, n_in, scratch=(), in_specs=None, name=None):
    outs = [jax.ShapeDtypeStruct(s, F32) for s in out_shapes]
    return pl.pallas_call(
        kernel,
        out_shape=outs,
        in_specs=in_specs or [VMEM] * n_in,
        out_specs=[VMEM] * len(outs),
        scratch_shapes=[pltpu.VMEM(s, F32) for s in scratch],
        compiler_params=pltpu.CompilerParams(vmem_limit_bytes=48 * 1024 * 1024),
        name=name,
    )


def roll(x, shift, axis):
    return pltpu.roll(x, shift % x.shape[axis], axis)


def iota(shape, dim):
    return lax.broadcasted_iota(jnp.int32, shape, dim)


def total(x):
    return jnp.sum(jnp.sum(x, axis=0, keepdims=True), axis=1, keepdims=True)


def pack_kernel(rhs, cond, ext, to_low, to_high, msg):
    lane = iota((CY, CZ), 1)
    a = jnp.zeros((CY, CZ), F32)
    b = jnp.zeros((CY, CZ), F32)
    acc = jnp.zeros((CY, CZ), F32)
    inside = lane < ext[0, 0, 0]
    for x in range(CX):
        k = cond[x]
        r = rhs[x]
        acc = acc + jnp.where(inside, r, 0.0)
        hi = (lane >= 16 * x) & (lane < 16 * x + H)
        start = (16 * x - H) % CZ
        lo = (lane >= start) & (lane < start + H)
        a = jnp.where(hi, roll(k, 16 * x, 1), jnp.where(lo, roll(r, 16 * x - H, 1), a))
        b = jnp.where(lo, roll(k, 16 * x, 1), jnp.where(hi, roll(r, 16 * x + H, 1), b))
    to_low[...] = a
    to_high[...] = b
    mean = total(acc) / CELLS
    at = iota((1, CZ), 1)
    z = lax.axis_index("gz")
    count = jnp.full((1, CZ), ext[0, 0, 0], jnp.int32).astype(F32)
    row = jnp.where(at == z, mean, 0.0) + jnp.where(at == SLOT + z, count, 0.0)
    msg[...] = jnp.broadcast_to(row[None], msg.shape)


def y_kernel(rhs, cond, from_high, from_low, zh, to_low, to_high):
    low_half = iota((CY, CZ), 1) % 16 < H
    a = from_high[...]
    b = from_low[...]
    zk = jnp.where(low_half, a, b)
    zr = jnp.where(low_half, roll(a, H, 1), roll(b, -H, 1))
    zh[0] = zk
    zh[1] = zr
    to_low[0:CX] = cond[:, 0:H, :]
    to_low[CX : 2 * CX] = rhs[:, 0:H, :]
    to_low[2 * CX] = zk[0:H]
    to_low[2 * CX + 1] = zr[0:H]
    to_high[0:CX] = cond[:, CY - H : CY, :]
    to_high[CX : 2 * CX] = rhs[:, CY - H : CY, :]
    to_high[2 * CX] = zk[CY - H : CY]
    to_high[2 * CX + 1] = zr[CY - H : CY]


def x_kernel(rhs, cond, zh, from_high, from_low, slab):
    slab[0:CX, 0:CY] = cond[...]
    slab[CX : 2 * CX, 0:CY] = rhs[...]
    slab[2 * CX : 2 * CX + 2, 0:CY] = zh[...]
    slab[:, CY : CY + H] = from_high[...]
    slab[:, CY + H : EY] = from_low[...]


def spread_kernel(rows, nz, part, msg):
    at = iota((1, CZ), 1)
    s = jnp.sum(part[...], axis=0)
    y = lax.axis_index("gy")
    here = (at >= y * nz) & (at < y * nz + nz)
    out = []
    for i in range(min(rows, 6)):
        moved = pltpu.roll(s, (y * nz + CZ - SLOT * i) % CZ, 1)
        out.append(jnp.where(here, moved, 0.0))
    if rows > 6:
        out.append(jnp.where(at >= 6 * SLOT, s, 0.0))
        out.append(jnp.zeros((1, CZ), F32))
    for i, row in enumerate(out):
        msg[:, i : i + 1, :] = jnp.broadcast_to(row[None], (msg.shape[0], 1, CZ))


def dot(a, b):
    return jnp.dot(a, b, precision=lax.Precision.HIGHEST, preferred_element_type=F32)


def inverse_kernel(factor, out):
    n = factor.shape[0]
    bs = CZ
    nb = n // bs
    i = iota((bs, bs), 0)
    j = iota((bs, bs), 1)
    eye = i == j
    low = [factor[b * bs : (b + 1) * bs, b * bs : (b + 1) * bs].astype(F32) for b in range(nb)]
    inv = []
    for lb in low:
        diag = jnp.where(eye, lb, 0.0)
        col = 1.0 / jnp.sum(diag, axis=1, keepdims=True)
        row = 1.0 / jnp.sum(diag, axis=0, keepdims=True)
        pair = (i // 2 == j // 2) & (i > j)
        inv.append(jnp.where(eye, col, 0.0) - jnp.where(pair, col * lb * row, 0.0))
    s = 2
    while s < bs:
        mask = (i // (2 * s) == j // (2 * s)) & (i // s > j // s)
        mid = [dot(jnp.where(mask, lb, 0.0), x) for lb, x in zip(low, inv)]
        inv = [x - dot(x, m) for x, m in zip(inv, mid)]
        s *= 2
    out[...] = jnp.zeros((n, n), F32)
    for b in range(nb):
        out[b * bs : (b + 1) * bs, b * bs : (b + 1) * bs] = inv[b]
    s = bs
    while s < n:
        for at in range(0, n, 2 * s):
            mid = dot(factor[at + s : at + 2 * s, at : at + s].astype(F32), out[at : at + s, at : at + s])
            out[at + s : at + 2 * s, at : at + s] = -dot(out[at + s : at + 2 * s, at + s : at + 2 * s], mid)
        s *= 2


def coarse_inverse(factor, gx):
    n = factor.shape[0]
    return call(inverse_kernel, [(n, n)], 1, name="inverse")(factor)[0]


def coarse_solve(inv, means):
    nb = len(means)
    bs = CZ
    rows = [jnp.zeros((1, bs), F32) for _ in range(nb)]
    for a in range(nb):
        acc = inv[a * bs : (a + 1) * bs, 0:bs] * means[0]
        for c in range(1, a + 1):
            acc = acc + inv[a * bs : (a + 1) * bs, c * bs : (c + 1) * bs] * means[c]
        u = jnp.sum(acc, axis=1, keepdims=True)
        for c in range(a + 1):
            rows[c] = rows[c] + jnp.sum(inv[a * bs : (a + 1) * bs, c * bs : (c + 1) * bs] * u, axis=0, keepdims=True)
    return rows


def neighbours(rows, nz, ny):
    nx = len(rows)
    x = lax.axis_index("gx")
    y = lax.axis_index("gy")
    z = lax.axis_index("gz")
    zero = jnp.zeros((1, CZ), F32)
    picked = []
    for dx in (-1, 0, 1):
        v = zero
        for r in range(nx):
            v = v + jnp.where(jnp.full((1, CZ), x + dx, jnp.int32) == r, rows[r], 0.0)
        picked.append(v)
    row = iota((8, CZ), 0)
    stack = jnp.where(row == 0, picked[0], jnp.where(row == 1, picked[1], jnp.where(row == 2, picked[2], 0.0)))
    lane = iota((8, CZ), 1)
    out = {}
    for dy in (-1, 0, 1):
        for dz in (-1, 0, 1):
            ok = (y + dy >= 0) & (y + dy < ny) & (z + dz >= 0) & (z + dz < nz)
            target = jnp.where(ok, (y + dy) * nz + z + dz, -1)
            out[dy, dz] = jnp.sum(jnp.where(lane == target, stack, 0.0), axis=1, keepdims=True)
    return out


def planes(low, high, body, unroll=2):
    assert (high - low) % unroll == 0

    def step(i, carry):
        for u in range(unroll):
            body(low + i * unroll + u)
        return carry

    lax.fori_loop(0, (high - low) // unroll, step, 0)


ROW_PARTS = ((0, 0), (8, 0), (16, 1), (24, -1))


def main_kernel(
    nx, ny, nz, left, own, right, gathered, inv,
    d_out, t_out, n_out, an_out, r_out, e0_out, ey_out, ez_out, ex_out, f_out, msg,
    kap, rr, cx, cy, cz, i0, k1, i1, u1, u2, dd, tt, ff, f1, fy,
):
    means, counts = [], []
    for x in range(nx):
        both = jnp.sum(gathered[x * ny : (x + 1) * ny], axis=0)
        means.append(both[0:1])
        counts.append(both[1:2])
    lane8 = iota((8, CZ), 1)
    lane8f = lane8.astype(F32)
    even8f = (lane8 - lane8 % 2).astype(F32)
    valid = (lane8 < H) | (lane8 >= CZ - H)
    ext = neighbours(counts, nz, ny)
    y0 = neighbours(coarse_solve(inv, means), nz, ny)
    for bx in range(3):
        for r, dy in ROW_PARTS:
            e = {dz: jnp.broadcast_to(ext[dy, dz][bx : bx + 1], (8, CZ)) for dz in (-1, 0, 1)}
            v = {dz: jnp.broadcast_to(y0[dy, dz][bx : bx + 1], (8, CZ)) for dz in (-1, 0, 1)}
            far = jnp.where(lane8 < CZ // 2, e[1], e[-1])
            m0 = jnp.where(lane8f < e[0], 1.0, 0.0)
            m1 = jnp.where(valid & (lane8f < far), 1.0, 0.0)
            ff[bx, r : r + 8, 0:CZ] = m0
            ff[bx, r : r + 8, CZ:EZ] = m1
            f1[bx, r : r + 8, 0:CZ] = jnp.where(even8f < e[0], 1.0, 0.0)
            f1[bx, r : r + 8, CZ:EZ] = jnp.where(valid & (even8f < far), 1.0, 0.0)
            fy[bx, r : r + 8, 0:CZ] = m0 * v[0]
            fy[bx, r : r + 8, CZ:EZ] = m1 * jnp.where(lane8 < CZ // 2, v[1], v[-1])
    for bx, src in enumerate((left, own, right)):
        for x in range(CX):
            at = bx * CX + x
            kap[at, :, 0:CZ] = src[x]
            kap[at, :, CZ:EZ] = roll(src[2 * CX], -16 * x, 1)
            rr[at, :, 0:CZ] = src[CX + x] * ff[bx, :, 0:CZ]
            rr[at, :, CZ:EZ] = roll(src[2 * CX + 1], -16 * x, 1) * ff[bx, :, CZ:EZ]
    row_even = iota((EY, EZ), 0) % 2 == 0
    lane_even = iota((EY, EZ), 1) % 2 == 0

    def pooled(s):
        s = s + jnp.where(row_even, roll(s, -1, 0), roll(s, 1, 0))
        return s + jnp.where(lane_even, roll(s, -1, 1), roll(s, 1, 1))

    def coefs(x):
        k = kap[x]
        cx[x] = 0.5 * (k + kap[jnp.minimum(x + 1, EX - 1)])
        cy[x] = 0.5 * (k + roll(k, -1, 0))
        cz[x] = 0.5 * (k + roll(k, -1, 1))

    planes(0, EX, coefs)

    def inverses(x):
        f = ff[x >> 3]
        b, c = cy[x], cz[x]
        s = cx[x] + cx[x - 1] + b + roll(b, 1, 0) + c + roll(c, 1, 1)
        i0[x] = OMEGA * f / (s + 1.0 - f)

    planes(1, EX - 1, inverses)

    def coarse_cond(i):
        k1[i] = pooled(kap[2 * i] + kap[2 * i + 1]) * 0.125

    planes(0, EX // 2, coarse_cond)

    def coarse_inv(i):
        k = k1[i]
        f = f1[i >> 2]
        s = k1[i - 1] + k1[i + 1] + roll(k, 2, 0) + roll(k, -2, 0) + roll(k, 2, 1) + roll(k, -2, 1)
        s = 3.0 * k + 0.5 * s
        i1[i] = OMEGA * f / (4.0 * s + 1.0 - f)

    planes(1, EX // 2 - 1, coarse_inv)

    def image(u, x):
        c = u[x]
        gx = cx[x] * (c - u[x + 1]) - cx[x - 1] * (u[x - 1] - c)
        gy = cy[x] * (c - roll(c, -1, 0))
        gz = cz[x] * (c - roll(c, -1, 1))
        return ff[x >> 3] * (gx + (gy - roll(gy, 1, 0)) + (gz - roll(gz, 1, 1)))

    def smooth(src, first_range, pair_range, out_range, put):
        def first(x):
            u1[x] = i0[x] * src[x]

        planes(*first_range, first)

        def pair(i):
            x = 2 * i
            s = (src[x] - image(u1, x)) + (src[x + 1] - image(u1, x + 1))
            below = ff[x >> 3] * (i1[i] * pooled(s))
            u2[x] = u1[x] + below
            u2[x + 1] = u1[x + 1] + below

        planes(*pair_range, pair, 1)

        def last(x):
            put(x, u2[x] + i0[x] * (src[x] - image(u2, x)))

        planes(*out_range, last)

    def put_d(x, v):
        dd[x] = v + fy[x >> 3]

    smooth(rr, (1, EX - 1), (1, EX // 2 - 1), (3, EX - 3), put_d)

    def put_t(x):
        tt[x] = image(dd, x)

    planes(4, EX - 4, put_t)
    for x in range(CX):
        d_out[x] = dd[H + x, 0:CY, 0:CZ]

    def put_n(x, v):
        dd[x] = v

    zero = jnp.zeros((CY, CZ), F32)
    s_rz, s_dad = zero, zero
    for x in range(CX):
        s_rz = s_rz + rr[H + x, 0:CY, 0:CZ] * d_out[x]
        s_dad = s_dad + tt[H + x, 0:CY, 0:CZ] * d_out[x]
    smooth(tt, (4, EX - 4), (3, EX // 2 - 3), (7, EX - 7), put_n)
    s_x, s_y, s_tau, s_om, s_d, s_cy, s_cz = (zero,) * 7
    f = ff[1]
    row = iota((EY, EZ), 0)
    lane = iota((EY, EZ), 1)
    mine = jnp.where((row < CY) & (lane < CZ), f, 0.0)
    own_f = f[0:CY, 0:CZ]
    row_o = iota((CY, CZ), 0)
    lane_o = iota((CY, CZ), 1)
    f_out[...] = own_f
    f_up_y = roll(f, -1, 0)
    f_up_z = roll(f, -1, 1)
    dif_y = mine - roll(mine, -1, 0)
    dif_z = mine - roll(mine, -1, 1)
    for x in range(CX):
        at = H + x
        an = image(dd, at)[0:CY, 0:CZ]
        n = dd[at, 0:CY, 0:CZ]
        t = tt[at, 0:CY, 0:CZ]
        an_out[x] = an
        n_out[x] = n
        t_out[x] = t
        r_out[x] = rr[at, 0:CY, 0:CZ]
        b, c = cy[at], cz[at]
        gy = b * dif_y
        gz = c * dif_z
        e = ((gy - roll(gy, 1, 0)) + (gz - roll(gz, 1, 1)))[0:CY, 0:CZ]
        if x == 0:
            e = e + cx[H - 1, 0:CY, 0:CZ] * own_f
        if x == CX - 1:
            e = e + cx[at, 0:CY, 0:CZ] * own_f
        e = e * own_f
        e0_out[x] = e
        cut_y = jnp.where(
            row_o == CY - 1, (b * f_up_y)[0:CY, 0:CZ], jnp.where(row_o == 0, roll(b * f, 1, 0)[0:CY, 0:CZ], 0.0)
        ) * own_f
        cut_z = jnp.where(
            lane_o == CZ - 1, (c * f_up_z)[0:CY, 0:CZ], jnp.where(lane_o == 0, roll(c * f, 1, 1)[0:CY, 0:CZ], 0.0)
        ) * own_f
        ey_out[x] = cut_y
        ez_out[x] = cut_z
        s_x = s_x + t * n
        s_y = s_y + n * an
        s_tau = s_tau + t
        s_om = s_om + an
        s_d = s_d + e * own_f
        s_cy = s_cy + cut_y
        s_cz = s_cz + cut_z
    ex0 = cx[H - 1, 0:CY, 0:CZ] * own_f * ff[0, 0:CY, 0:CZ]
    ex1 = cx[H + CX - 1, 0:CY, 0:CZ] * own_f * ff[2, 0:CY, 0:CZ]
    ex_out[0] = ex0
    ex_out[1] = ex1
    at = iota((1, CZ), 1)
    z = lax.axis_index("gz")
    vectors = (
        s_tau, s_om, s_d, ex1,
        jnp.where(row_o == CY - 1, s_cy, 0.0), jnp.where(lane_o == CZ - 1, s_cz, 0.0),
    )
    line = jnp.zeros((1, CZ), F32)
    for i, v in enumerate(vectors):
        line = line + jnp.where(at == SLOT * i + z, total(v), 0.0)
    for i, v in enumerate((s_rz, s_dad, s_x, s_y)):
        line = line + jnp.where(at == 6 * SLOT + i, total(v), 0.0)
    msg[...] = jnp.broadcast_to(line[None], msg.shape)


def final_kernel(nx, ny, nz, gathered, inv, d_in, t_in, n_in, an_in, r_in, e0, ey, ez, ex, f_in, sol, res):
    tables = [jnp.sum(gathered[x * ny : (x + 1) * ny], axis=0) for x in range(nx)]
    sums = tables[0][6:7]
    for t in tables[1:]:
        sums = sums + t[6:7]
    at = iota((1, CZ), 1)

    def scalar(i):
        return jnp.sum(jnp.where(at == 6 * SLOT + i, sums, 0.0), axis=1, keepdims=True)

    rz, dad, xx, yy = (scalar(i) for i in range(4))
    tau = [t[0:1] for t in tables]
    yt = coarse_solve(inv, [v * (1.0 / CELLS) for v in tau])
    add_x = jnp.zeros((1, CZ), F32)
    add_y = jnp.zeros((1, CZ), F32)
    for x in range(nx):
        y = yt[x]
        t = tables[x]
        add_x = add_x + t[0:1] * y
        cross = t[4:5] * roll(y, -nz, 1) + t[5:6] * roll(y, -1, 1)
        if x + 1 < nx:
            cross = cross + t[3:4] * yt[x + 1]
        add_y = add_y + y * (2.0 * t[1:2] + t[2:3] * y - 2.0 * cross)
    xx = xx + jnp.sum(add_x, axis=1, keepdims=True)
    yy = yy + jnp.sum(add_y, axis=1, keepdims=True)
    a0 = rz / dad
    new = a0 * a0 * xx - rz
    beta = new / rz
    zaz = dad - 2.0 * a0 * xx + a0 * a0 * yy
    a1 = new / (zaz - beta * beta * dad)
    near = neighbours(yt, nz, ny)
    shape = (CY, CZ)

    def wide(v, bx=1):
        return jnp.broadcast_to(v[bx : bx + 1], shape)

    y_own = wide(near[0, 0])
    y_y = jnp.where(iota(shape, 0) < CY // 2, wide(near[-1, 0]), wide(near[1, 0]))
    y_z = jnp.where(iota(shape, 1) < CZ // 2, wide(near[0, -1]), wide(near[0, 1]))
    f = f_in[...]
    c_d = jnp.broadcast_to(a0 + a1 * (1.0 + beta), shape)
    c_n = jnp.broadcast_to(a0 * a1, shape)
    for x in range(CX):
        n = n_in[x] + f * y_own
        an = an_in[x] + e0[x] * y_own - ey[x] * y_y - ez[x] * y_z
        if x == 0:
            an = an - ex[0] * wide(near[0, 0], 0)
        if x == CX - 1:
            an = an - ex[1] * wide(near[0, 0], 2)
        sol[x] = c_d * d_in[x] - c_n * n
        res[x] = r_in[x] - c_d * t_in[x] + c_n * an


def exchange(axis, to_low, to_high):
    size = lax.axis_size(axis)
    up = [(i, i + 1) for i in range(size - 1)]
    down = [(b, a) for a, b in up]
    return lax.ppermute(to_low, axis, down), lax.ppermute(to_high, axis, up)


def gathered_rows(msg, rows, nx, ny, nz):
    part = lax.all_to_all(msg, "gz", 0, 0, tiled=True)
    spread = call(functools.partial(spread_kernel, rows, nz), [(nx * ny, rows, CZ)], 1, name="spread")(part)[0]
    return lax.all_to_all(spread, ("gx", "gy"), 0, 0, tiled=True)


def on_device(right_side, conductance, extents, coarse_factor):
    nx, ny, nz = (lax.axis_size(a) for a in ("gx", "gy", "gz"))
    inv = coarse_inverse(coarse_factor, nx)
    to_low, to_high, msg = call(
        pack_kernel, [(CY, CZ), (CY, CZ), (nz, 1, CZ)], 3, in_specs=[VMEM, VMEM, SMEM], name="pack"
    )(right_side, conductance, extents)
    z_high, z_low = exchange("gz", to_low, to_high)
    first = gathered_rows(msg, 2, nx, ny, nz)
    depth = 2 * CX + 2
    zh, to_low, to_high = call(y_kernel, [(2, CY, CZ), (depth, H, CZ), (depth, H, CZ)], 4, name="rows")(
        right_side, conductance, z_high, z_low
    )
    y_high, y_low = exchange("gy", to_low, to_high)
    slab = call(x_kernel, [(depth, EY, CZ)], 5, name="slab")(right_side, conductance, zh, y_high, y_low)[0]
    x_high, x_low = exchange("gx", slab, slab)
    block = (CX, CY, CZ)
    wide = (EX, EY, EZ)
    half = (EX // 2, EY, EZ)
    third = (3, EY, EZ)
    outs = call(
        functools.partial(main_kernel, nx, ny, nz),
        [block] * 8 + [(2, CY, CZ), (CY, CZ), (nz, 1, CZ)],
        5,
        scratch=[wide] * 6 + [half] * 2 + [wide] * 4 + [third] * 3,
        name="fields",
    )(x_low, slab, x_high, first, inv)
    second = gathered_rows(outs[-1], 8, nx, ny, nz)
    sol, res = call(functools.partial(final_kernel, nx, ny, nz), [block] * 2, 12, name="final")(
        second, inv, *outs[:-1]
    )
    return sol, res


def solution(mesh):
    spec = P("gx", "gy", "gz")
    return jax.shard_map(
        on_device, mesh=mesh, in_specs=(spec, spec, spec, P()), out_specs=(spec, spec), check_vma=False
    )
```

```python
import functools

import jax
import jax.numpy as jnp
from jax import lax
from jax.experimental import pallas as pl
from jax.experimental.pallas import tpu as pltpu
from jax.sharding import PartitionSpec as P

F32 = jnp.float32
OMEGA = 0.8
CX, CY, CZ = 8, 16, 128
CELLS = CX * CY * CZ
H = 8
EX, EY, EZ = CX + 2 * H, CY + 2 * H, 2 * CZ
SLOT = 16
VMEM = pl.BlockSpec(memory_space=pltpu.VMEM)
SMEM = pl.BlockSpec(memory_space=pltpu.SMEM)


def call(kernel, out_shapes, n_in, scratch=(), in_specs=None, name=None):
    outs = [jax.ShapeDtypeStruct(s, F32) for s in out_shapes]
    return pl.pallas_call(
        kernel,
        out_shape=outs,
        in_specs=in_specs or [VMEM] * n_in,
        out_specs=[VMEM] * len(outs),
        scratch_shapes=[pltpu.VMEM(s, F32) for s in scratch],
        compiler_params=pltpu.CompilerParams(vmem_limit_bytes=48 * 1024 * 1024),
        name=name,
    )


def roll(x, shift, axis):
    return pltpu.roll(x, shift % x.shape[axis], axis)


def iota(shape, dim):
    return lax.broadcasted_iota(jnp.int32, shape, dim)


def total(x):
    return jnp.sum(jnp.sum(x, axis=0, keepdims=True), axis=1, keepdims=True)


def pack_kernel(ext, rhs, cond, own, msg, sems):
    copies = [
        pltpu.make_async_copy(cond, own.at[0:CX], sems.at[0]),
        pltpu.make_async_copy(rhs, own.at[CX : 2 * CX], sems.at[1]),
    ]
    for c in copies:
        c.start()
    nz = msg.shape[0]
    lane = iota((CY, CZ), 1)
    row = iota((CY, CZ), 0)
    a = jnp.zeros((CY, CZ), F32)
    b = jnp.zeros((CY, CZ), F32)
    acc = jnp.zeros((CY, CZ), F32)
    inside = lane < ext[0, 0, 0]
    count = jnp.full((CY, CZ), ext[0, 0, 0], jnp.int32).astype(F32)
    z = lax.axis_index("gz")
    for c in copies:
        c.wait()
    for x in range(CX):
        k = own[x]
        r = own[CX + x]
        acc = acc + jnp.where(inside, r, 0.0)
        hi = (lane >= 16 * x) & (lane < 16 * x + H)
        start = (16 * x - H) % CZ
        lo = (lane >= start) & (lane < start + H)
        a = jnp.where(hi, roll(k, 16 * x, 1), jnp.where(lo, roll(r, 16 * x - H, 1), a))
        b = jnp.where(lo, roll(k, 16 * x, 1), jnp.where(hi, roll(r, 16 * x + H, 1), b))
    info = jnp.where(row == 0, total(acc) / CELLS, count)
    a = jnp.where((lane == CZ - 1) & (row < 2), info, a)
    b = jnp.where((lane == 0) & (row < 2), info, b)
    for i in range(nz):
        msg[i] = b

    @pl.when(z > 0)
    def _():
        msg[z - 1] = a


def rows_kernel(own, got, zh, to_low, to_high, line):
    nz = got.shape[0]
    z = lax.axis_index("gz")
    low_half = iota((CY, CZ), 1) % 16 < H
    up = jnp.minimum(z + 1, nz - 1)
    a = jnp.where(jnp.full((CY, CZ), z, jnp.int32) < nz - 1, got[up], 0.0)
    b = jnp.where(jnp.full((CY, CZ), z, jnp.int32) > 0, got[jnp.maximum(z - 1, 0)], 0.0)
    lane = iota((8, CZ), 1)
    info = jnp.zeros((8, CZ), F32)
    for i in range(nz):
        v = got[i, 0:8]
        info = jnp.where(lane == i, roll(v, i, 1), info)
    info = jnp.where(lane == z + 1, pltpu.roll(a[0:8], z + 2, 1), info)
    info = jnp.where(lane < nz, info, 0.0)
    line[...] = jnp.broadcast_to((info[0:1] + roll(info[1:2], SLOT, 1))[None], line.shape)
    zk = jnp.where(low_half, a, b)
    zr = jnp.where(low_half, roll(a, H, 1), roll(b, -H, 1))
    zh[0] = zk
    zh[1] = zr
    to_low[0 : 2 * CX] = own[:, 0:H, :]
    to_low[2 * CX] = zk[0:H]
    to_low[2 * CX + 1] = zr[0:H]
    to_high[0 : 2 * CX] = own[:, CY - H : CY, :]
    to_high[2 * CX] = zk[CY - H : CY]
    to_high[2 * CX + 1] = zr[CY - H : CY]


def slab_kernel(own, zh, from_high, from_low, after, slab):
    slab[0 : 2 * CX, 0:CY] = own[...]
    slab[2 * CX : 2 * CX + 2, 0:CY] = zh[...]
    slab[:, CY : CY + H] = from_high[...]
    slab[:, CY + H : EY] = from_low[...]


def sum_kernel(part, line):
    line[...] = jnp.broadcast_to(jnp.sum(part[...], axis=0, keepdims=True), line.shape)


def table(rows, i, nx, ny, nz):
    out = []
    for x in range(nx):
        v = rows[x * ny : (x + 1) * ny].reshape(ny, CZ)
        v = jnp.where(iota((ny, CZ), 1) < nz, roll(v, -SLOT * i, 1), 0.0)
        v = pltpu.roll(v, 0, 1, stride=nz, stride_axis=0)
        out.append(jnp.sum(v, axis=0, keepdims=True))
    return out


def dot(a, b):
    return jnp.dot(a, b, precision=lax.Precision.HIGHEST, preferred_element_type=F32)


def diagonal_kernel(factor, out):
    n = factor.shape[0]
    bs = CZ
    nb = n // bs
    i = iota((bs, bs), 0)
    j = iota((bs, bs), 1)
    eye = i == j
    low = [factor[b * bs : (b + 1) * bs, b * bs : (b + 1) * bs].astype(F32) for b in range(nb)]
    inv = []
    for lb in low:
        diag = jnp.where(eye, lb, 0.0)
        col = 1.0 / jnp.sum(diag, axis=1, keepdims=True)
        row = 1.0 / jnp.sum(diag, axis=0, keepdims=True)
        pair = (i // 2 == j // 2) & (i > j)
        inv.append(jnp.where(eye, col, 0.0) - jnp.where(pair, col * lb * row, 0.0))
    s = 2
    while s < bs:
        mask = (i // (2 * s) == j // (2 * s)) & (i // s > j // s)
        mid = [dot(jnp.where(mask, lb, 0.0), x) for lb, x in zip(low, inv)]
        inv = [x - dot(x, m) for x, m in zip(inv, mid)]
        s *= 2
    for b in range(nb):
        out[b] = inv[b]


def inverse_of(factor, diagonal, out):
    n = factor.shape[0]
    bs = CZ
    for b in range(n // bs):
        out[b * bs : (b + 1) * bs, b * bs : (b + 1) * bs] = diagonal[b]
    s = bs
    while s < n:
        for at in range(0, n, 2 * s):
            for lo in range(s, 2 * s, bs):
                for hi in range(lo - s + bs, s, bs):
                    out[at + lo - s : at + lo - s + bs, at + hi : at + hi + bs] = jnp.zeros((bs, bs), F32)
            if s > bs:
                for lo in range(s, 2 * s, bs):
                    for hi in range(lo + bs, 2 * s, bs):
                        out[at + lo : at + lo + bs, at + hi : at + hi + bs] = jnp.zeros((bs, bs), F32)
            mid = dot(factor[at + s : at + 2 * s, at : at + s].astype(F32), out[at : at + s, at : at + s])
            out[at + s : at + 2 * s, at : at + s] = -dot(out[at + s : at + 2 * s, at + s : at + 2 * s], mid)
        s *= 2


def coarse_solve(inv, means):
    nb = len(means)
    bs = CZ
    rows = [jnp.zeros((1, bs), F32) for _ in range(nb)]
    for a in range(nb):
        acc = inv[a * bs : (a + 1) * bs, 0:bs] * means[0]
        for c in range(1, a + 1):
            acc = acc + inv[a * bs : (a + 1) * bs, c * bs : (c + 1) * bs] * means[c]
        u = jnp.sum(acc, axis=1, keepdims=True)
        for c in range(a + 1):
            rows[c] = rows[c] + jnp.sum(inv[a * bs : (a + 1) * bs, c * bs : (c + 1) * bs] * u, axis=0, keepdims=True)
    return rows


def neighbours(rows, nz, ny):
    nx = len(rows)
    x = lax.axis_index("gx")
    y = lax.axis_index("gy")
    z = lax.axis_index("gz")
    zero = jnp.zeros((1, CZ), F32)
    picked = []
    for dx in (-1, 0, 1):
        v = zero
        for r in range(nx):
            v = v + jnp.where(jnp.full((1, CZ), x + dx, jnp.int32) == r, rows[r], 0.0)
        picked.append(v)
    row = iota((8, CZ), 0)
    stack = jnp.where(row == 0, picked[0], jnp.where(row == 1, picked[1], jnp.where(row == 2, picked[2], 0.0)))
    lane = iota((8, CZ), 1)
    out = {}
    for dy in (-1, 0, 1):
        for dz in (-1, 0, 1):
            ok = (y + dy >= 0) & (y + dy < ny) & (z + dz >= 0) & (z + dz < nz)
            target = jnp.where(ok, (y + dy) * nz + z + dz, -1)
            out[dy, dz] = jnp.sum(jnp.where(lane == target, stack, 0.0), axis=1, keepdims=True)
    return out


def planes(low, high, body, most=4):
    unroll = next(u for u in (most, 5, 4, 3, 2, 1) if (high - low) % u == 0)

    def step(i, carry):
        for u in range(unroll):
            body(low + i * unroll + u)
        return carry

    lax.fori_loop(0, (high - low) // unroll, step, 0)


ROW_PARTS = ((0, 0), (8, 0), (16, 1), (24, -1))


def coarse_kernel(nx, ny, nz, factor, diagonal, gathered, after, inv, ff, f1, fy):
    inverse_of(factor, diagonal, inv)
    lane8 = iota((8, CZ), 1)
    lane8f = lane8.astype(F32)
    even8f = (lane8 - lane8 % 2).astype(F32)
    valid = (lane8 < H) | (lane8 >= CZ - H)
    ext = neighbours(table(gathered, 1, nx, ny, nz), nz, ny)
    y0 = neighbours(coarse_solve(inv, table(gathered, 0, nx, ny, nz)), nz, ny)
    for bx in range(3):
        for r, dy in ROW_PARTS:
            e = {dz: jnp.broadcast_to(ext[dy, dz][bx : bx + 1], (8, CZ)) for dz in (-1, 0, 1)}
            v = {dz: jnp.broadcast_to(y0[dy, dz][bx : bx + 1], (8, CZ)) for dz in (-1, 0, 1)}
            far = jnp.where(lane8 < CZ // 2, e[1], e[-1])
            m0 = jnp.where(lane8f < e[0], 1.0, 0.0)
            m1 = jnp.where(valid & (lane8f < far), 1.0, 0.0)
            ff[bx, r : r + 8, 0:CZ] = m0
            ff[bx, r : r + 8, CZ:EZ] = m1
            f1[bx, r : r + 8, 0:CZ] = jnp.where(even8f < e[0], 1.0, 0.0)
            f1[bx, r : r + 8, CZ:EZ] = jnp.where(valid & (even8f < far), 1.0, 0.0)
            fy[bx, r : r + 8, 0:CZ] = m0 * v[0]
            fy[bx, r : r + 8, CZ:EZ] = m1 * jnp.where(lane8 < CZ // 2, v[1], v[-1])


def main_kernel(
    left, own, right, ff, f1, fy,
    d_out, t_out, n_out, an_out, r_out, e0_out, ey_out, ez_out, ex_out, f_out, msg,
    kap, rr, cx, cy, cz, i0, k1, i1, u1, u2, dd, tt,
):
    for bx, src in enumerate((left, own, right)):
        for x in range(CX):
            at = bx * CX + x
            kap[at, :, 0:CZ] = src[x]
            kap[at, :, CZ:EZ] = roll(src[2 * CX], -16 * x, 1)
            rr[at, :, 0:CZ] = src[CX + x] * ff[bx, :, 0:CZ]
            rr[at, :, CZ:EZ] = roll(src[2 * CX + 1], -16 * x, 1) * ff[bx, :, CZ:EZ]
    row_even = iota((EY, EZ), 0) % 2 == 0
    lane_even = iota((EY, EZ), 1) % 2 == 0

    def pooled(s):
        s = s + jnp.where(row_even, roll(s, -1, 0), roll(s, 1, 0))
        return s + jnp.where(lane_even, roll(s, -1, 1), roll(s, 1, 1))

    def coefs(x):
        k = kap[x]
        cx[x] = 0.5 * (k + kap[jnp.minimum(x + 1, EX - 1)])
        cy[x] = 0.5 * (k + roll(k, -1, 0))
        cz[x] = 0.5 * (k + roll(k, -1, 1))

    planes(0, EX, coefs)

    def inverses(x):
        f = ff[x >> 3]
        b, c = cy[x], cz[x]
        s = cx[x] + cx[x - 1] + b + roll(b, 1, 0) + c + roll(c, 1, 1)
        i0[x] = OMEGA * f / (s + 1.0 - f)

    planes(1, EX - 1, inverses)

    def coarse_cond(i):
        k1[i] = pooled(kap[2 * i] + kap[2 * i + 1]) * 0.125

    planes(0, EX // 2, coarse_cond)

    def coarse_inv(i):
        k = k1[i]
        f = f1[i >> 2]
        s = k1[i - 1] + k1[i + 1] + roll(k, 2, 0) + roll(k, -2, 0) + roll(k, 2, 1) + roll(k, -2, 1)
        s = 3.0 * k + 0.5 * s
        i1[i] = OMEGA * f / (4.0 * s + 1.0 - f)

    planes(1, EX // 2 - 1, coarse_inv)

    def image(u, x):
        c = u[x]
        gx = cx[x] * (c - u[x + 1]) - cx[x - 1] * (u[x - 1] - c)
        gy = cy[x] * (c - roll(c, -1, 0))
        gz = cz[x] * (c - roll(c, -1, 1))
        return ff[x >> 3] * (gx + (gy - roll(gy, 1, 0)) + (gz - roll(gz, 1, 1)))

    def smooth(src, first_range, pair_range, out_range, put):
        def first(x):
            u1[x] = i0[x] * src[x]

        planes(*first_range, first)

        def pair(i):
            x = 2 * i
            s = (src[x] - image(u1, x)) + (src[x + 1] - image(u1, x + 1))
            below = ff[x >> 3] * (i1[i] * pooled(s))
            u2[x] = u1[x] + below
            u2[x + 1] = u1[x + 1] + below

        planes(*pair_range, pair, 2)

        def last(x):
            put(x, u2[x] + i0[x] * (src[x] - image(u2, x)))

        planes(*out_range, last)

    def put_d(x, v):
        dd[x] = v + fy[x >> 3]

    smooth(rr, (1, EX - 1), (1, EX // 2 - 1), (3, EX - 3), put_d)

    def put_t(x):
        tt[x] = image(dd, x)

    planes(4, EX - 4, put_t)
    for x in range(CX):
        d_out[x] = dd[H + x, 0:CY, 0:CZ]

    def put_n(x, v):
        dd[x] = v

    zero = jnp.zeros((CY, CZ), F32)
    s_rz, s_dad = zero, zero
    for x in range(CX):
        s_rz = s_rz + rr[H + x, 0:CY, 0:CZ] * d_out[x]
        s_dad = s_dad + tt[H + x, 0:CY, 0:CZ] * d_out[x]
    smooth(tt, (4, EX - 4), (3, EX // 2 - 3), (7, EX - 7), put_n)
    s_x, s_y, s_tau, s_om, s_d, s_cy, s_cz = (zero,) * 7
    f = ff[1]
    row = iota((EY, EZ), 0)
    lane = iota((EY, EZ), 1)
    mine = jnp.where((row < CY) & (lane < CZ), f, 0.0)
    own_f = f[0:CY, 0:CZ]
    row_o = iota((CY, CZ), 0)
    lane_o = iota((CY, CZ), 1)
    f_out[...] = own_f
    f_up_y = roll(f, -1, 0)
    f_up_z = roll(f, -1, 1)
    dif_y = mine - roll(mine, -1, 0)
    dif_z = mine - roll(mine, -1, 1)
    for x in range(CX):
        at = H + x
        an = image(dd, at)[0:CY, 0:CZ]
        n = dd[at, 0:CY, 0:CZ]
        t = tt[at, 0:CY, 0:CZ]
        an_out[x] = an
        n_out[x] = n
        t_out[x] = t
        r_out[x] = rr[at, 0:CY, 0:CZ]
        b, c = cy[at], cz[at]
        gy = b * dif_y
        gz = c * dif_z
        e = ((gy - roll(gy, 1, 0)) + (gz - roll(gz, 1, 1)))[0:CY, 0:CZ]
        if x == 0:
            e = e + cx[H - 1, 0:CY, 0:CZ] * own_f
        if x == CX - 1:
            e = e + cx[at, 0:CY, 0:CZ] * own_f
        e = e * own_f
        e0_out[x] = e
        cut_y = jnp.where(
            row_o == CY - 1, (b * f_up_y)[0:CY, 0:CZ], jnp.where(row_o == 0, roll(b * f, 1, 0)[0:CY, 0:CZ], 0.0)
        ) * own_f
        cut_z = jnp.where(
            lane_o == CZ - 1, (c * f_up_z)[0:CY, 0:CZ], jnp.where(lane_o == 0, roll(c * f, 1, 1)[0:CY, 0:CZ], 0.0)
        ) * own_f
        ey_out[x] = cut_y
        ez_out[x] = cut_z
        s_x = s_x + t * n
        s_y = s_y + n * an
        s_tau = s_tau + t
        s_om = s_om + an
        s_d = s_d + e * own_f
        s_cy = s_cy + cut_y
        s_cz = s_cz + cut_z
    ex0 = cx[H - 1, 0:CY, 0:CZ] * own_f * ff[0, 0:CY, 0:CZ]
    ex1 = cx[H + CX - 1, 0:CY, 0:CZ] * own_f * ff[2, 0:CY, 0:CZ]
    ex_out[0] = ex0
    ex_out[1] = ex1
    at = iota((1, CZ), 1)
    z = lax.axis_index("gz")
    vectors = (
        s_tau, s_om, s_d, ex1,
        jnp.where(row_o == CY - 1, s_cy, 0.0), jnp.where(lane_o == CZ - 1, s_cz, 0.0),
    )
    line = jnp.zeros((1, CZ), F32)
    for i, v in enumerate(vectors):
        line = line + jnp.where(at == SLOT * i + z, total(v), 0.0)
    for i, v in enumerate((s_rz, s_dad, s_x, s_y)):
        line = line + jnp.where(at == 6 * SLOT + i, total(v), 0.0)
    msg[...] = jnp.broadcast_to(line[None], msg.shape)


def final_kernel(nx, ny, nz, gathered, inv, d_in, t_in, n_in, an_in, r_in, e0, ey, ez, ex, f_in, sol, res):
    vectors = [table(gathered, i, nx, ny, nz) for i in range(6)]
    tables = list(zip(*vectors))
    sums = jnp.sum(gathered[...], axis=0)
    at = iota((1, CZ), 1)

    def scalar(i):
        return jnp.sum(jnp.where(at == 6 * SLOT + i, sums, 0.0), axis=1, keepdims=True)

    rz, dad, xx, yy = (scalar(i) for i in range(4))
    tau = vectors[0]
    yt = coarse_solve(inv, [v * (1.0 / CELLS) for v in tau])
    add_x = jnp.zeros((1, CZ), F32)
    add_y = jnp.zeros((1, CZ), F32)
    for x in range(nx):
        y = yt[x]
        t = tables[x]
        add_x = add_x + t[0] * y
        cross = t[4] * roll(y, -nz, 1) + t[5] * roll(y, -1, 1)
        if x + 1 < nx:
            cross = cross + t[3] * yt[x + 1]
        add_y = add_y + y * (2.0 * t[1] + t[2] * y - 2.0 * cross)
    xx = xx + jnp.sum(add_x, axis=1, keepdims=True)
    yy = yy + jnp.sum(add_y, axis=1, keepdims=True)
    a0 = rz / dad
    new = a0 * a0 * xx - rz
    beta = new / rz
    zaz = dad - 2.0 * a0 * xx + a0 * a0 * yy
    a1 = new / (zaz - beta * beta * dad)
    near = neighbours(yt, nz, ny)
    shape = (CY, CZ)

    def wide(v, bx=1):
        return jnp.broadcast_to(v[bx : bx + 1], shape)

    y_own = wide(near[0, 0])
    y_y = jnp.where(iota(shape, 0) < CY // 2, wide(near[-1, 0]), wide(near[1, 0]))
    y_z = jnp.where(iota(shape, 1) < CZ // 2, wide(near[0, -1]), wide(near[0, 1]))
    f = f_in[...]
    c_d = jnp.broadcast_to(a0 + a1 * (1.0 + beta), shape)
    c_n = jnp.broadcast_to(a0 * a1, shape)
    for x in range(CX):
        n = n_in[x] + f * y_own
        an = an_in[x] + e0[x] * y_own - ey[x] * y_y - ez[x] * y_z
        if x == 0:
            an = an - ex[0] * wide(near[0, 0], 0)
        if x == CX - 1:
            an = an - ex[1] * wide(near[0, 0], 2)
        sol[x] = c_d * d_in[x] - c_n * n
        res[x] = r_in[x] - c_d * t_in[x] + c_n * an


def exchange(axis, to_low, to_high):
    size = lax.axis_size(axis)
    up = [(i, i + 1) for i in range(size - 1)]
    down = [(b, a) for a, b in up]
    return lax.ppermute(to_low, axis, down), lax.ppermute(to_high, axis, up)


def on_device(right_side, conductance, extents, coarse_factor):
    nx, ny, nz = (lax.axis_size(a) for a in ("gx", "gy", "gz"))
    sizes = (nx, ny, nz)
    any_space = pl.BlockSpec(memory_space=pl.ANY)
    own, msg = pl.pallas_call(
        pack_kernel,
        out_shape=[jax.ShapeDtypeStruct(s, F32) for s in ((2 * CX, CY, CZ), (nz, CY, CZ))],
        in_specs=[SMEM, pl.BlockSpec(memory_space=pltpu.HBM), pl.BlockSpec(memory_space=pltpu.HBM)],
        out_specs=[VMEM, VMEM],
        scratch_shapes=[pltpu.SemaphoreType.DMA((2,))],
        compiler_params=pltpu.CompilerParams(vmem_limit_bytes=8 * 1024 * 1024),
        name="pack",
    )(extents, right_side, conductance)
    got = lax.all_to_all(msg, "gz", 0, 0, tiled=True)
    depth = 2 * CX + 2
    zh, to_low, to_high, line = call(
        rows_kernel, [(2, CY, CZ), (depth, H, CZ), (depth, H, CZ), (nx * ny, 1, CZ)], 2, name="rows"
    )(own, got)
    first = lax.all_to_all(line, ("gx", "gy"), 0, 0, tiled=True)
    to_low, to_high, factor, first = lax.optimization_barrier((to_low, to_high, coarse_factor, first))
    y_high, y_low = exchange("gy", to_low, to_high)
    nb = factor.shape[0] // CZ
    diagonal = call(diagonal_kernel, [(nb, CZ, CZ)], 1, name="diagonal")(factor)[0]
    slab = call(
        slab_kernel, [(depth, EY, CZ)], 5, in_specs=[VMEM] * 4 + [any_space], name="slab"
    )(own, zh, y_high, y_low, diagonal)[0]
    x_high, x_low = exchange("gx", slab, slab)
    block = (CX, CY, CZ)
    wide = (EX, EY, EZ)
    half = (EX // 2, EY, EZ)
    third = (3, EY, EZ)
    inv, ff, f1, fy = call(
        functools.partial(coarse_kernel, *sizes), [factor.shape] + [third] * 3, 4,
        in_specs=[VMEM] * 3 + [any_space], name="coarse",
    )(factor, diagonal, first, slab)
    outs = call(
        main_kernel,
        [block] * 8 + [(2, CY, CZ), (CY, CZ), (nz, 1, CZ)],
        6,
        scratch=[wide] * 6 + [half] * 2 + [wide] * 4,
        name="fields",
    )(x_low, slab, x_high, ff, f1, fy)
    part = lax.all_to_all(outs[-1], "gz", 0, 0, tiled=True)
    line = call(sum_kernel, [(nx * ny, 1, CZ)], 1, name="sum")(part)[0]
    second = lax.all_to_all(line, ("gx", "gy"), 0, 0, tiled=True)
    sol, res = call(functools.partial(final_kernel, *sizes), [block] * 2, 12, name="final")(
        second, inv, *outs[:-1]
    )
    return sol, res


def solution(mesh):
    spec = P("gx", "gy", "gz")
    return jax.shard_map(
        on_device, mesh=mesh, in_specs=(spec, spec, spec, P()), out_specs=(spec, spec), check_vma=False
    )
```

```python
import functools

import jax
import jax.numpy as jnp
from jax import lax
from jax.experimental import pallas as pl
from jax.experimental.pallas import tpu as pltpu
from jax.sharding import PartitionSpec as P

F32 = jnp.float32
OMEGA = 0.8
CX, CY, CZ = 8, 16, 128
CELLS = CX * CY * CZ
H = 8
EX, EY, EZ = CX + 2 * H, CY + 2 * H, 2 * CZ
SLOT = 16
VMEM = pl.BlockSpec(memory_space=pltpu.VMEM)
SMEM = pl.BlockSpec(memory_space=pltpu.SMEM)


def call(kernel, out_shapes, n_in, scratch=(), in_specs=None, name=None):
    outs = [jax.ShapeDtypeStruct(s, F32) for s in out_shapes]
    return pl.pallas_call(
        kernel,
        out_shape=outs,
        in_specs=in_specs or [VMEM] * n_in,
        out_specs=[VMEM] * len(outs),
        scratch_shapes=[pltpu.VMEM(s, F32) for s in scratch],
        compiler_params=pltpu.CompilerParams(vmem_limit_bytes=48 * 1024 * 1024),
        name=name,
    )


def roll(x, shift, axis):
    return pltpu.roll(x, shift % x.shape[axis], axis)


def iota(shape, dim):
    return lax.broadcasted_iota(jnp.int32, shape, dim)


def total(x):
    return jnp.sum(jnp.sum(x, axis=0, keepdims=True), axis=1, keepdims=True)


def pack_kernel(ext, rhs, cond, own, msg, sems):
    copies = [
        pltpu.make_async_copy(cond, own.at[0:CX], sems.at[0]),
        pltpu.make_async_copy(rhs, own.at[CX : 2 * CX], sems.at[1]),
    ]
    for c in copies:
        c.start()
    nz = msg.shape[0]
    lane = iota((CY, CZ), 1)
    row = iota((CY, CZ), 0)
    a = jnp.zeros((CY, CZ), F32)
    b = jnp.zeros((CY, CZ), F32)
    acc = jnp.zeros((CY, CZ), F32)
    inside = lane < ext[0, 0, 0]
    count = jnp.full((CY, CZ), ext[0, 0, 0], jnp.int32).astype(F32)
    z = lax.axis_index("gz")
    for c in copies:
        c.wait()
    for x in range(CX):
        k = own[x]
        r = own[CX + x]
        acc = acc + jnp.where(inside, r, 0.0)
        hi = (lane >= 16 * x) & (lane < 16 * x + H)
        start = (16 * x - H) % CZ
        lo = (lane >= start) & (lane < start + H)
        a = jnp.where(hi, roll(k, 16 * x, 1), jnp.where(lo, roll(r, 16 * x - H, 1), a))
        b = jnp.where(lo, roll(k, 16 * x, 1), jnp.where(hi, roll(r, 16 * x + H, 1), b))
    info = jnp.where(row == 0, total(acc) / CELLS, count)
    a = jnp.where((lane == CZ - 1) & (row < 2), info, a)
    b = jnp.where((lane == 0) & (row < 2), info, b)
    for i in range(nz):
        msg[i] = b

    @pl.when(z > 0)
    def _():
        msg[z - 1] = a


def rows_kernel(own, got, zh, to_low, to_high, line):
    nz = got.shape[0]
    z = lax.axis_index("gz")
    low_half = iota((CY, CZ), 1) % 16 < H
    up = jnp.minimum(z + 1, nz - 1)
    a = jnp.where(jnp.full((CY, CZ), z, jnp.int32) < nz - 1, got[up], 0.0)
    b = jnp.where(jnp.full((CY, CZ), z, jnp.int32) > 0, got[jnp.maximum(z - 1, 0)], 0.0)
    lane = iota((8, CZ), 1)
    info = jnp.zeros((8, CZ), F32)
    for i in range(nz):
        v = got[i, 0:8]
        info = jnp.where(lane == i, roll(v, i, 1), info)
    info = jnp.where(lane == z + 1, pltpu.roll(a[0:8], z + 2, 1), info)
    info = jnp.where(lane < nz, info, 0.0)
    line[...] = jnp.broadcast_to((info[0:1] + roll(info[1:2], SLOT, 1))[None], line.shape)
    zk = jnp.where(low_half, a, b)
    zr = jnp.where(low_half, roll(a, H, 1), roll(b, -H, 1))
    zh[0] = zk
    zh[1] = zr
    to_low[0 : 2 * CX] = own[:, 0:H, :]
    to_low[2 * CX] = zk[0:H]
    to_low[2 * CX + 1] = zr[0:H]
    to_high[0 : 2 * CX] = own[:, CY - H : CY, :]
    to_high[2 * CX] = zk[CY - H : CY]
    to_high[2 * CX + 1] = zr[CY - H : CY]


def slab_kernel(own, zh, from_high, from_low, after, slab):
    slab[0 : 2 * CX, 0:CY] = own[...]
    slab[2 * CX : 2 * CX + 2, 0:CY] = zh[...]
    slab[:, CY : CY + H] = from_high[...]
    slab[:, CY + H : EY] = from_low[...]


def sum_kernel(part, line):
    line[...] = jnp.broadcast_to(jnp.sum(part[...], axis=0, keepdims=True), line.shape)


def table(rows, i, nx, ny, nz):
    out = []
    for x in range(nx):
        v = rows[x * ny : (x + 1) * ny].reshape(ny, CZ)
        v = jnp.where(iota((ny, CZ), 1) < nz, roll(v, -SLOT * i, 1), 0.0)
        v = pltpu.roll(v, 0, 1, stride=nz, stride_axis=0)
        out.append(jnp.sum(v, axis=0, keepdims=True))
    return out


def dot(a, b):
    return jnp.dot(a, b, precision=lax.Precision.HIGHEST, preferred_element_type=F32)


def diagonal_kernel(factor, out):
    n = factor.shape[0]
    bs = CZ
    nb = n // bs
    i = iota((bs, bs), 0)
    j = iota((bs, bs), 1)
    eye = i == j
    low = [factor[b * bs : (b + 1) * bs, b * bs : (b + 1) * bs].astype(F32) for b in range(nb)]
    inv = []
    for lb in low:
        diag = jnp.where(eye, lb, 0.0)
        col = 1.0 / jnp.sum(diag, axis=1, keepdims=True)
        row = 1.0 / jnp.sum(diag, axis=0, keepdims=True)
        pair = (i // 2 == j // 2) & (i > j)
        inv.append(jnp.where(eye, col, 0.0) - jnp.where(pair, col * lb * row, 0.0))
    s = 2
    while s < bs:
        mask = (i // (2 * s) == j // (2 * s)) & (i // s > j // s)
        mid = [dot(jnp.where(mask, lb, 0.0), x) for lb, x in zip(low, inv)]
        inv = [x - dot(x, m) for x, m in zip(inv, mid)]
        s *= 2
    for b in range(nb):
        out[b] = inv[b]


def inverse_of(factor, diagonal, out):
    n = factor.shape[0]
    bs = CZ
    for b in range(n // bs):
        out[b * bs : (b + 1) * bs, b * bs : (b + 1) * bs] = diagonal[b]
    s = bs
    while s < n:
        for at in range(0, n, 2 * s):
            for lo in range(s, 2 * s, bs):
                for hi in range(lo - s + bs, s, bs):
                    out[at + lo - s : at + lo - s + bs, at + hi : at + hi + bs] = jnp.zeros((bs, bs), F32)
            if s > bs:
                for lo in range(s, 2 * s, bs):
                    for hi in range(lo + bs, 2 * s, bs):
                        out[at + lo : at + lo + bs, at + hi : at + hi + bs] = jnp.zeros((bs, bs), F32)
            mid = dot(factor[at + s : at + 2 * s, at : at + s].astype(F32), out[at : at + s, at : at + s])
            out[at + s : at + 2 * s, at : at + s] = -dot(out[at + s : at + 2 * s, at + s : at + 2 * s], mid)
        s *= 2


def coarse_solve(inv, means):
    nb = len(means)
    bs = CZ
    rows = [jnp.zeros((1, bs), F32) for _ in range(nb)]
    for a in range(nb):
        acc = inv[a * bs : (a + 1) * bs, 0:bs] * means[0]
        for c in range(1, a + 1):
            acc = acc + inv[a * bs : (a + 1) * bs, c * bs : (c + 1) * bs] * means[c]
        u = jnp.sum(acc, axis=1, keepdims=True)
        for c in range(a + 1):
            rows[c] = rows[c] + jnp.sum(inv[a * bs : (a + 1) * bs, c * bs : (c + 1) * bs] * u, axis=0, keepdims=True)
    return rows


def neighbours(rows, nz, ny):
    nx = len(rows)
    x = lax.axis_index("gx")
    y = lax.axis_index("gy")
    z = lax.axis_index("gz")
    zero = jnp.zeros((1, CZ), F32)
    picked = []
    for dx in (-1, 0, 1):
        v = zero
        for r in range(nx):
            v = v + jnp.where(jnp.full((1, CZ), x + dx, jnp.int32) == r, rows[r], 0.0)
        picked.append(v)
    row = iota((8, CZ), 0)
    stack = jnp.where(row == 0, picked[0], jnp.where(row == 1, picked[1], jnp.where(row == 2, picked[2], 0.0)))
    lane = iota((8, CZ), 1)
    out = {}
    for dy in (-1, 0, 1):
        for dz in (-1, 0, 1):
            ok = (y + dy >= 0) & (y + dy < ny) & (z + dz >= 0) & (z + dz < nz)
            target = jnp.where(ok, (y + dy) * nz + z + dz, -1)
            out[dy, dz] = jnp.sum(jnp.where(lane == target, stack, 0.0), axis=1, keepdims=True)
    return out


def planes(low, high, body):
    count = high - low
    unroll = max(u for u in range(1, count // 2 + 1) if count % u == 0)

    def step(i, carry):
        for u in range(unroll):
            body(low + i * unroll + u)
        return carry

    lax.fori_loop(0, (high - low) // unroll, step, 0)


ROW_PARTS = ((0, 0), (8, 0), (16, 1), (24, -1))


def coarse_kernel(nx, ny, nz, factor, diagonal, gathered, after, inv, ff, f1, fy):
    inverse_of(factor, diagonal, inv)
    lane8 = iota((8, CZ), 1)
    lane8f = lane8.astype(F32)
    even8f = (lane8 - lane8 % 2).astype(F32)
    valid = (lane8 < H) | (lane8 >= CZ - H)
    ext = neighbours(table(gathered, 1, nx, ny, nz), nz, ny)
    y0 = neighbours(coarse_solve(inv, table(gathered, 0, nx, ny, nz)), nz, ny)
    for bx in range(3):
        for r, dy in ROW_PARTS:
            e = {dz: jnp.broadcast_to(ext[dy, dz][bx : bx + 1], (8, CZ)) for dz in (-1, 0, 1)}
            v = {dz: jnp.broadcast_to(y0[dy, dz][bx : bx + 1], (8, CZ)) for dz in (-1, 0, 1)}
            far = jnp.where(lane8 < CZ // 2, e[1], e[-1])
            m0 = jnp.where(lane8f < e[0], 1.0, 0.0)
            m1 = jnp.where(valid & (lane8f < far), 1.0, 0.0)
            ff[bx, r : r + 8, 0:CZ] = m0
            ff[bx, r : r + 8, CZ:EZ] = m1
            f1[bx, r : r + 8, 0:CZ] = jnp.where(even8f < e[0], 1.0, 0.0)
            f1[bx, r : r + 8, CZ:EZ] = jnp.where(valid & (even8f < far), 1.0, 0.0)
            fy[bx, r : r + 8, 0:CZ] = m0 * v[0]
            fy[bx, r : r + 8, CZ:EZ] = m1 * jnp.where(lane8 < CZ // 2, v[1], v[-1])


def main_kernel(
    left, own, right, ff, f1, fy,
    d_out, t_out, n_out, an_out, r_out, e0_out, ey_out, ez_out, ex_out, f_out, msg,
    kap, rr, cx, cy, cz, i0, k1, i1, u1, u2, dd, tt,
):
    for bx, src in enumerate((left, own, right)):
        for x in range(CX):
            at = bx * CX + x
            kap[at, :, 0:CZ] = src[x]
            kap[at, :, CZ:EZ] = roll(src[2 * CX], -16 * x, 1)
            rr[at, :, 0:CZ] = src[CX + x] * ff[bx, :, 0:CZ]
            rr[at, :, CZ:EZ] = roll(src[2 * CX + 1], -16 * x, 1) * ff[bx, :, CZ:EZ]
    row_even = iota((EY, EZ), 0) % 2 == 0
    lane_even = iota((EY, EZ), 1) % 2 == 0

    def pooled(s):
        s = s + jnp.where(row_even, roll(s, -1, 0), roll(s, 1, 0))
        return s + jnp.where(lane_even, roll(s, -1, 1), roll(s, 1, 1))

    def coefs(x):
        k = kap[x]
        cx[x] = 0.5 * (k + kap[jnp.minimum(x + 1, EX - 1)])
        cy[x] = 0.5 * (k + roll(k, -1, 0))
        cz[x] = 0.5 * (k + roll(k, -1, 1))

    planes(0, EX, coefs)

    def inverses(x):
        f = ff[x >> 3]
        b, c = cy[x], cz[x]
        s = cx[x] + cx[x - 1] + b + roll(b, 1, 0) + c + roll(c, 1, 1)
        i0[x] = OMEGA * f / (s + 1.0 - f)

    planes(1, EX - 1, inverses)

    def coarse_cond(i):
        k1[i] = pooled(kap[2 * i] + kap[2 * i + 1]) * 0.125

    planes(0, EX // 2, coarse_cond)

    def coarse_inv(i):
        k = k1[i]
        f = f1[i >> 2]
        s = k1[i - 1] + k1[i + 1] + roll(k, 2, 0) + roll(k, -2, 0) + roll(k, 2, 1) + roll(k, -2, 1)
        s = 3.0 * k + 0.5 * s
        i1[i] = OMEGA * f / (4.0 * s + 1.0 - f)

    planes(1, EX // 2 - 1, coarse_inv)

    def image(u, x):
        c = u[x]
        gx = cx[x] * (c - u[x + 1]) - cx[x - 1] * (u[x - 1] - c)
        gy = cy[x] * (c - roll(c, -1, 0))
        gz = cz[x] * (c - roll(c, -1, 1))
        return ff[x >> 3] * (gx + (gy - roll(gy, 1, 0)) + (gz - roll(gz, 1, 1)))

    def smooth(src, first_range, pair_range, out_range, put):
        def first(x):
            u1[x] = i0[x] * src[x]

        planes(*first_range, first)

        def pair(i):
            x = 2 * i
            s = (src[x] - image(u1, x)) + (src[x + 1] - image(u1, x + 1))
            below = ff[x >> 3] * (i1[i] * pooled(s))
            u2[x] = u1[x] + below
            u2[x + 1] = u1[x + 1] + below

        planes(*pair_range, pair)

        def last(x):
            put(x, u2[x] + i0[x] * (src[x] - image(u2, x)))

        planes(*out_range, last)

    def put_d(x, v):
        dd[x] = v + fy[x >> 3]

    smooth(rr, (1, EX - 1), (1, EX // 2 - 1), (3, EX - 3), put_d)

    def put_t(x):
        tt[x] = image(dd, x)

    planes(4, EX - 4, put_t)
    for x in range(CX):
        d_out[x] = dd[H + x, 0:CY, 0:CZ]

    def put_n(x, v):
        dd[x] = v

    zero = jnp.zeros((CY, CZ), F32)
    s_rz, s_dad = zero, zero
    for x in range(CX):
        s_rz = s_rz + rr[H + x, 0:CY, 0:CZ] * d_out[x]
        s_dad = s_dad + tt[H + x, 0:CY, 0:CZ] * d_out[x]
    smooth(tt, (4, EX - 4), (3, EX // 2 - 3), (7, EX - 7), put_n)
    s_x, s_y, s_tau, s_om, s_d, s_cy, s_cz = (zero,) * 7
    f = ff[1]
    row = iota((EY, EZ), 0)
    lane = iota((EY, EZ), 1)
    mine = jnp.where((row < CY) & (lane < CZ), f, 0.0)
    own_f = f[0:CY, 0:CZ]
    row_o = iota((CY, CZ), 0)
    lane_o = iota((CY, CZ), 1)
    f_out[...] = own_f
    f_up_y = roll(f, -1, 0)
    f_up_z = roll(f, -1, 1)
    dif_y = mine - roll(mine, -1, 0)
    dif_z = mine - roll(mine, -1, 1)
    for x in range(CX):
        at = H + x
        an = image(dd, at)[0:CY, 0:CZ]
        n = dd[at, 0:CY, 0:CZ]
        t = tt[at, 0:CY, 0:CZ]
        an_out[x] = an
        n_out[x] = n
        t_out[x] = t
        r_out[x] = rr[at, 0:CY, 0:CZ]
        b, c = cy[at], cz[at]
        gy = b * dif_y
        gz = c * dif_z
        e = ((gy - roll(gy, 1, 0)) + (gz - roll(gz, 1, 1)))[0:CY, 0:CZ]
        if x == 0:
            e = e + cx[H - 1, 0:CY, 0:CZ] * own_f
        if x == CX - 1:
            e = e + cx[at, 0:CY, 0:CZ] * own_f
        e = e * own_f
        e0_out[x] = e
        cut_y = jnp.where(
            row_o == CY - 1, (b * f_up_y)[0:CY, 0:CZ], jnp.where(row_o == 0, roll(b * f, 1, 0)[0:CY, 0:CZ], 0.0)
        ) * own_f
        cut_z = jnp.where(
            lane_o == CZ - 1, (c * f_up_z)[0:CY, 0:CZ], jnp.where(lane_o == 0, roll(c * f, 1, 1)[0:CY, 0:CZ], 0.0)
        ) * own_f
        ey_out[x] = cut_y
        ez_out[x] = cut_z
        s_x = s_x + t * n
        s_y = s_y + n * an
        s_tau = s_tau + t
        s_om = s_om + an
        s_d = s_d + e * own_f
        s_cy = s_cy + cut_y
        s_cz = s_cz + cut_z
    ex0 = cx[H - 1, 0:CY, 0:CZ] * own_f * ff[0, 0:CY, 0:CZ]
    ex1 = cx[H + CX - 1, 0:CY, 0:CZ] * own_f * ff[2, 0:CY, 0:CZ]
    ex_out[0] = ex0
    ex_out[1] = ex1
    at = iota((1, CZ), 1)
    z = lax.axis_index("gz")
    vectors = (
        s_tau, s_om, s_d, ex1,
        jnp.where(row_o == CY - 1, s_cy, 0.0), jnp.where(lane_o == CZ - 1, s_cz, 0.0),
    )
    line = jnp.zeros((1, CZ), F32)
    for i, v in enumerate(vectors):
        line = line + jnp.where(at == SLOT * i + z, total(v), 0.0)
    for i, v in enumerate((s_rz, s_dad, s_x, s_y)):
        line = line + jnp.where(at == 6 * SLOT + i, total(v), 0.0)
    msg[...] = jnp.broadcast_to(line[None], msg.shape)


def final_kernel(nx, ny, nz, gathered, inv, d_in, t_in, n_in, an_in, r_in, e0, ey, ez, ex, f_in, sol, res):
    vectors = [table(gathered, i, nx, ny, nz) for i in range(6)]
    tables = list(zip(*vectors))
    sums = jnp.sum(gathered[...], axis=0)
    at = iota((1, CZ), 1)

    def scalar(i):
        return jnp.sum(jnp.where(at == 6 * SLOT + i, sums, 0.0), axis=1, keepdims=True)

    rz, dad, xx, yy = (scalar(i) for i in range(4))
    tau = vectors[0]
    yt = coarse_solve(inv, [v * (1.0 / CELLS) for v in tau])
    add_x = jnp.zeros((1, CZ), F32)
    add_y = jnp.zeros((1, CZ), F32)
    for x in range(nx):
        y = yt[x]
        t = tables[x]
        add_x = add_x + t[0] * y
        cross = t[4] * roll(y, -nz, 1) + t[5] * roll(y, -1, 1)
        if x + 1 < nx:
            cross = cross + t[3] * yt[x + 1]
        add_y = add_y + y * (2.0 * t[1] + t[2] * y - 2.0 * cross)
    xx = xx + jnp.sum(add_x, axis=1, keepdims=True)
    yy = yy + jnp.sum(add_y, axis=1, keepdims=True)
    a0 = rz / dad
    new = a0 * a0 * xx - rz
    beta = new / rz
    zaz = dad - 2.0 * a0 * xx + a0 * a0 * yy
    a1 = new / (zaz - beta * beta * dad)
    near = neighbours(yt, nz, ny)
    shape = (CY, CZ)

    def wide(v, bx=1):
        return jnp.broadcast_to(v[bx : bx + 1], shape)

    y_own = wide(near[0, 0])
    y_y = jnp.where(iota(shape, 0) < CY // 2, wide(near[-1, 0]), wide(near[1, 0]))
    y_z = jnp.where(iota(shape, 1) < CZ // 2, wide(near[0, -1]), wide(near[0, 1]))
    f = f_in[...]
    c_d = jnp.broadcast_to(a0 + a1 * (1.0 + beta), shape)
    c_n = jnp.broadcast_to(a0 * a1, shape)
    for x in range(CX):
        n = n_in[x] + f * y_own
        an = an_in[x] + e0[x] * y_own - ey[x] * y_y - ez[x] * y_z
        if x == 0:
            an = an - ex[0] * wide(near[0, 0], 0)
        if x == CX - 1:
            an = an - ex[1] * wide(near[0, 0], 2)
        sol[x] = c_d * d_in[x] - c_n * n
        res[x] = r_in[x] - c_d * t_in[x] + c_n * an


def exchange(axis, to_low, to_high):
    size = lax.axis_size(axis)
    up = [(i, i + 1) for i in range(size - 1)]
    down = [(b, a) for a, b in up]
    return lax.ppermute(to_low, axis, down), lax.ppermute(to_high, axis, up)


def on_device(right_side, conductance, extents, coarse_factor):
    nx, ny, nz = (lax.axis_size(a) for a in ("gx", "gy", "gz"))
    sizes = (nx, ny, nz)
    any_space = pl.BlockSpec(memory_space=pl.ANY)
    own, msg = pl.pallas_call(
        pack_kernel,
        out_shape=[jax.ShapeDtypeStruct(s, F32) for s in ((2 * CX, CY, CZ), (nz, CY, CZ))],
        in_specs=[SMEM, pl.BlockSpec(memory_space=pltpu.HBM), pl.BlockSpec(memory_space=pltpu.HBM)],
        out_specs=[VMEM, VMEM],
        scratch_shapes=[pltpu.SemaphoreType.DMA((2,))],
        compiler_params=pltpu.CompilerParams(vmem_limit_bytes=8 * 1024 * 1024),
        name="pack",
    )(extents, right_side, conductance)
    got = lax.all_to_all(msg, "gz", 0, 0, tiled=True)
    depth = 2 * CX + 2
    zh, to_low, to_high, line = call(
        rows_kernel, [(2, CY, CZ), (depth, H, CZ), (depth, H, CZ), (nx * ny, 1, CZ)], 2, name="rows"
    )(own, got)
    first = lax.all_to_all(line, ("gx", "gy"), 0, 0, tiled=True)
    y_high, y_low = exchange("gy", to_low, to_high)
    slab = call(
        slab_kernel, [(depth, EY, CZ)], 5, in_specs=[VMEM] * 4 + [any_space], name="slab"
    )(own, zh, y_high, y_low, first)[0]
    slab, factor = lax.optimization_barrier((slab, coarse_factor))
    nb = factor.shape[0] // CZ
    diagonal = call(diagonal_kernel, [(nb, CZ, CZ)], 1, name="diagonal")(factor)[0]
    x_high, x_low = exchange("gx", slab, slab)
    block = (CX, CY, CZ)
    wide = (EX, EY, EZ)
    half = (EX // 2, EY, EZ)
    third = (3, EY, EZ)
    inv, ff, f1, fy = call(
        functools.partial(coarse_kernel, *sizes), [factor.shape] + [third] * 3, 4,
        in_specs=[VMEM] * 3 + [any_space], name="coarse",
    )(factor, diagonal, first, slab)
    outs = call(
        main_kernel,
        [block] * 8 + [(2, CY, CZ), (CY, CZ), (nz, 1, CZ)],
        6,
        scratch=[wide] * 6 + [half] * 2 + [wide] * 4,
        name="fields",
    )(x_low, slab, x_high, ff, f1, fy)
    part = lax.all_to_all(outs[-1], "gz", 0, 0, tiled=True)
    line = call(sum_kernel, [(nx * ny, 1, CZ)], 1, name="sum")(part)[0]
    second = lax.all_to_all(line, ("gx", "gy"), 0, 0, tiled=True)
    sol, res = call(functools.partial(final_kernel, *sizes), [block] * 2, 12, name="final")(
        second, inv, *outs[:-1]
    )
    return sol, res


def solution(mesh):
    spec = P("gx", "gy", "gz")
    return jax.shard_map(
        on_device, mesh=mesh, in_specs=(spec, spec, spec, P()), out_specs=(spec, spec), check_vma=False
    )
```

```python
import functools

import jax
import jax.numpy as jnp
from jax import lax
from jax.experimental import pallas as pl
from jax.experimental.pallas import tpu as pltpu
from jax.sharding import PartitionSpec as P

F32 = jnp.float32
PACK_MIB = 60
OMEGA = 0.8
CX, CY, CZ = 8, 16, 128
CELLS = CX * CY * CZ
H = 8
EX, EY, EZ = CX + 2 * H, CY + 2 * H, 2 * CZ
SLOT = 16
VMEM = pl.BlockSpec(memory_space=pltpu.VMEM)
SMEM = pl.BlockSpec(memory_space=pltpu.SMEM)


def call(kernel, out_shapes, n_in, scratch=(), in_specs=None, name=None, aliases=None, mib=24):
    outs = [jax.ShapeDtypeStruct(s, F32) for s in out_shapes]
    return pl.pallas_call(
        kernel,
        out_shape=outs,
        in_specs=in_specs or [VMEM] * n_in,
        out_specs=[VMEM] * len(outs),
        scratch_shapes=[pltpu.VMEM(s, F32) for s in scratch],
        input_output_aliases=aliases or {},
        compiler_params=pltpu.CompilerParams(vmem_limit_bytes=mib * 1024 * 1024),
        name=name,
    )


def roll(x, shift, axis):
    return pltpu.roll(x, shift % x.shape[axis], axis)


def iota(shape, dim):
    return lax.broadcasted_iota(jnp.int32, shape, dim)


def total(x):
    return jnp.sum(jnp.sum(x, axis=0, keepdims=True), axis=1, keepdims=True)


def pack_kernel(ext, rhs, cond, msg):
    nz = msg.shape[0]
    lane = iota((CY, CZ), 1)
    row = iota((CY, CZ), 0)
    a = jnp.zeros((CY, CZ), F32)
    b = jnp.zeros((CY, CZ), F32)
    acc = jnp.zeros((CY, CZ), F32)
    count = jnp.broadcast_to(ext[0], (CY, CZ))
    inside = lane < count
    z = lax.axis_index("gz")
    for x in range(CX):
        k = cond[x]
        r = rhs[x]
        acc = acc + jnp.where(inside, r, 0.0)
        hi = (lane >= 16 * x) & (lane < 16 * x + H)
        start = (16 * x - H) % CZ
        lo = (lane >= start) & (lane < start + H)
        a = jnp.where(hi, roll(k, 16 * x, 1), jnp.where(lo, roll(r, 16 * x - H, 1), a))
        b = jnp.where(lo, roll(k, 16 * x, 1), jnp.where(hi, roll(r, 16 * x + H, 1), b))
    info = jnp.where(row == 0, total(acc) / CELLS, count.astype(F32))
    a = jnp.where((lane == CZ - 1) & (row < 2), info, a)
    b = jnp.where((lane == 0) & (row < 2), info, b)
    for i in range(nz):
        msg[i] = b

    @pl.when(z > 0)
    def _():
        msg[z - 1] = a


def rows_kernel(rhs, cond, got, zh, to_low, to_high, line):
    nz = got.shape[0]
    z = lax.axis_index("gz")
    low_half = iota((CY, CZ), 1) % 16 < H
    up = jnp.minimum(z + 1, nz - 1)
    a = jnp.where(jnp.full((CY, CZ), z, jnp.int32) < nz - 1, got[up], 0.0)
    b = jnp.where(jnp.full((CY, CZ), z, jnp.int32) > 0, got[jnp.maximum(z - 1, 0)], 0.0)
    lane = iota((8, CZ), 1)
    info = jnp.zeros((8, CZ), F32)
    for i in range(nz):
        v = got[i, 0:8]
        info = jnp.where(lane == i, roll(v, i, 1), info)
    info = jnp.where(lane == z + 1, pltpu.roll(a[0:8], z + 2, 1), info)
    info = jnp.where(lane < nz, info, 0.0)
    line[...] = jnp.broadcast_to((info[0:1] + roll(info[1:2], SLOT, 1))[None], line.shape)
    zk = jnp.where(low_half, a, b)
    zr = jnp.where(low_half, roll(a, H, 1), roll(b, -H, 1))
    zh[0] = zk
    zh[1] = zr
    to_low[0:CX] = cond[:, 0:H, :]
    to_low[CX : 2 * CX] = rhs[:, 0:H, :]
    to_low[2 * CX] = zk[0:H]
    to_low[2 * CX + 1] = zr[0:H]
    to_high[0:CX] = cond[:, CY - H : CY, :]
    to_high[CX : 2 * CX] = rhs[:, CY - H : CY, :]
    to_high[2 * CX] = zk[CY - H : CY]
    to_high[2 * CX + 1] = zr[CY - H : CY]


def slab_kernel(rhs, cond, zh, from_high, from_low, after, slab):
    slab[0:CX, 0:CY] = cond[...]
    slab[CX : 2 * CX, 0:CY] = rhs[...]
    slab[2 * CX : 2 * CX + 2, 0:CY] = zh[...]
    slab[:, CY : CY + H] = from_high[...]
    slab[:, CY + H : EY] = from_low[...]


def sum_kernel(part, line):
    line[...] = jnp.broadcast_to(jnp.sum(part[...], axis=0, keepdims=True), line.shape)


def table(rows, i, nx, ny, nz):
    out = []
    for x in range(nx):
        v = rows[x * ny : (x + 1) * ny].reshape(ny, CZ)
        v = jnp.where(iota((ny, CZ), 1) < nz, roll(v, -SLOT * i, 1), 0.0)
        v = pltpu.roll(v, 0, 1, stride=nz, stride_axis=0)
        out.append(jnp.sum(v, axis=0, keepdims=True))
    return out


def dot(a, b):
    return jnp.dot(a, b, precision=lax.Precision.HIGHEST, preferred_element_type=F32)


def diagonal_kernel(factor, out):
    n = factor.shape[0]
    bs = CZ
    nb = n // bs
    i = iota((bs, bs), 0)
    j = iota((bs, bs), 1)
    eye = i == j
    low = [factor[b * bs : (b + 1) * bs, b * bs : (b + 1) * bs].astype(F32) for b in range(nb)]
    inv = []
    for lb in low:
        diag = jnp.where(eye, lb, 0.0)
        col = 1.0 / jnp.sum(diag, axis=1, keepdims=True)
        row = 1.0 / jnp.sum(diag, axis=0, keepdims=True)
        pair = (i // 2 == j // 2) & (i > j)
        inv.append(jnp.where(eye, col, 0.0) - jnp.where(pair, col * lb * row, 0.0))
    s = 2
    while s < bs:
        mask = (i // (2 * s) == j // (2 * s)) & (i // s > j // s)
        mid = [dot(jnp.where(mask, lb, 0.0), x) for lb, x in zip(low, inv)]
        inv = [x - dot(x, m) for x, m in zip(inv, mid)]
        s *= 2
    for b in range(nb):
        out[b] = inv[b]


def inverse_of(factor, diagonal, out):
    n = factor.shape[0]
    bs = CZ
    for b in range(n // bs):
        out[b * bs : (b + 1) * bs, b * bs : (b + 1) * bs] = diagonal[b]
    s = bs
    while s < n:
        for at in range(0, n, 2 * s):
            for lo in range(s, 2 * s, bs):
                for hi in range(lo - s + bs, s, bs):
                    out[at + lo - s : at + lo - s + bs, at + hi : at + hi + bs] = jnp.zeros((bs, bs), F32)
            if s > bs:
                for lo in range(s, 2 * s, bs):
                    for hi in range(lo + bs, 2 * s, bs):
                        out[at + lo : at + lo + bs, at + hi : at + hi + bs] = jnp.zeros((bs, bs), F32)
            mid = dot(factor[at + s : at + 2 * s, at : at + s].astype(F32), out[at : at + s, at : at + s])
            out[at + s : at + 2 * s, at : at + s] = -dot(out[at + s : at + 2 * s, at + s : at + 2 * s], mid)
        s *= 2


def coarse_solve(inv, means):
    nb = len(means)
    bs = CZ
    rows = [jnp.zeros((1, bs), F32) for _ in range(nb)]
    for a in range(nb):
        acc = inv[a * bs : (a + 1) * bs, 0:bs] * means[0]
        for c in range(1, a + 1):
            acc = acc + inv[a * bs : (a + 1) * bs, c * bs : (c + 1) * bs] * means[c]
        u = jnp.sum(acc, axis=1, keepdims=True)
        for c in range(a + 1):
            rows[c] = rows[c] + jnp.sum(inv[a * bs : (a + 1) * bs, c * bs : (c + 1) * bs] * u, axis=0, keepdims=True)
    return rows


def neighbours(rows, nz, ny):
    nx = len(rows)
    x = lax.axis_index("gx")
    y = lax.axis_index("gy")
    z = lax.axis_index("gz")
    zero = jnp.zeros((1, CZ), F32)
    picked = []
    for dx in (-1, 0, 1):
        v = zero
        for r in range(nx):
            v = v + jnp.where(jnp.full((1, CZ), x + dx, jnp.int32) == r, rows[r], 0.0)
        picked.append(v)
    row = iota((8, CZ), 0)
    stack = jnp.where(row == 0, picked[0], jnp.where(row == 1, picked[1], jnp.where(row == 2, picked[2], 0.0)))
    lane = iota((8, CZ), 1)
    out = {}
    for dy in (-1, 0, 1):
        for dz in (-1, 0, 1):
            ok = (y + dy >= 0) & (y + dy < ny) & (z + dz >= 0) & (z + dz < nz)
            target = jnp.where(ok, (y + dy) * nz + z + dz, -1)
            out[dy, dz] = jnp.sum(jnp.where(lane == target, stack, 0.0), axis=1, keepdims=True)
    return out


def groups(low, high, body, step=1):
    count = high - low
    size = max(u for u in range(1, count // 2 + 1) if count % u == 0)

    def go(i, carry):
        body([low + i * size + u for u in range(size)])
        return carry

    lax.fori_loop(0, count // size, go, 0)


def unpack(src, bx, kap, rr, ff):
    for x in range(CX):
        at = bx * CX + x
        kap[at, :, 0:CZ] = src[x]
        kap[at, :, CZ:EZ] = roll(src[2 * CX], -16 * x, 1)
        rr[at, :, 0:CZ] = src[CX + x] * ff[bx, :, 0:CZ]
        rr[at, :, CZ:EZ] = roll(src[2 * CX + 1], -16 * x, 1) * ff[bx, :, CZ:EZ]


def pooled(s):
    even = iota(s.shape, 0) % 2 == 0
    s = s + jnp.where(even, roll(s, -1, 0), roll(s, 1, 0))
    even = iota(s.shape, 1) % 2 == 0
    return s + jnp.where(even, roll(s, -1, 1), roll(s, 1, 1))


def coef_x(x, kap, cx):
    cx[x] = 0.5 * (kap[x] + kap[x + 1])


def coef_yz(x, kap, cy, cz):
    k = kap[x]
    cy[x] = 0.5 * (k + roll(k, -1, 0))
    cz[x] = 0.5 * (k + roll(k, -1, 1))


def inverse_fine(x, cx, cy, cz, i0, rr, u1, ff):
    f = ff[x >> 3]
    b, c = cy[x], cz[x]
    s = cx[x] + cx[x - 1] + b + roll(b, 1, 0) + c + roll(c, 1, 1)
    v = OMEGA * f / (s + 1.0 - f)
    i0[x] = v
    u1[x] = v * rr[x]


def coarse_cond(i, kap, k1):
    k1[i] = pooled(kap[2 * i] + kap[2 * i + 1]) * 0.125


def inverse_coarse(i, k1, i1, f1):
    k = k1[i]
    f = f1[i >> 2]
    s = k1[i - 1] + k1[i + 1] + roll(k, 2, 0) + roll(k, -2, 0) + roll(k, 2, 1) + roll(k, -2, 1)
    s = 3.0 * k + 0.5 * s
    i1[i] = OMEGA * f / (4.0 * s + 1.0 - f)


ROW_PARTS = ((0, 0), (8, 0), (16, 1), (24, -1))


def coarse_kernel(
    nx, ny, nz, factor, diagonal, gathered, slab,
    inv, ff, f1, fy, kap, rr, cx, cy, cz, i0, k1, i1, u1,
):
    inverse_of(factor, diagonal, inv)
    lane8 = iota((8, CZ), 1)
    lane8f = lane8.astype(F32)
    even8f = (lane8 - lane8 % 2).astype(F32)
    valid = (lane8 < H) | (lane8 >= CZ - H)
    ext = neighbours(table(gathered, 1, nx, ny, nz), nz, ny)
    y0 = neighbours(coarse_solve(inv, table(gathered, 0, nx, ny, nz)), nz, ny)
    for bx in range(3):
        for r, dy in ROW_PARTS:
            e = {dz: jnp.broadcast_to(ext[dy, dz][bx : bx + 1], (8, CZ)) for dz in (-1, 0, 1)}
            v = {dz: jnp.broadcast_to(y0[dy, dz][bx : bx + 1], (8, CZ)) for dz in (-1, 0, 1)}
            far = jnp.where(lane8 < CZ // 2, e[1], e[-1])
            m0 = jnp.where(lane8f < e[0], 1.0, 0.0)
            m1 = jnp.where(valid & (lane8f < far), 1.0, 0.0)
            ff[bx, r : r + 8, 0:CZ] = m0
            ff[bx, r : r + 8, CZ:EZ] = m1
            f1[bx, r : r + 8, 0:CZ] = jnp.where(even8f < e[0], 1.0, 0.0)
            f1[bx, r : r + 8, CZ:EZ] = jnp.where(valid & (even8f < far), 1.0, 0.0)
            fy[bx, r : r + 8, 0:CZ] = m0 * v[0]
            fy[bx, r : r + 8, CZ:EZ] = m1 * jnp.where(lane8 < CZ // 2, v[1], v[-1])


    unpack(slab, 1, kap, rr, ff)
    for x in range(CX, 2 * CX):
        coef_yz(x, kap, cy, cz)
        if x < 2 * CX - 1:
            coef_x(x, kap, cx)
    for x in range(CX + 1, 2 * CX - 1):
        inverse_fine(x, cx, cy, cz, i0, rr, u1, ff)
    for i in range(CX // 2, CX):
        coarse_cond(i, kap, k1)
    for i in range(CX // 2 + 1, CX - 1):
        inverse_coarse(i, k1, i1, f1)


def main_kernel(
    left, right, ff, f1, fy, *refs
):
    (kap, rr, cx, cy, cz, i0, k1, i1, u1) = refs[9:18]
    (d_out, t_out, n_out, an_out, r_out, e0_out, ey_out, ez_out, ex_out, f_out, msg) = refs[18:29]
    u2, dd, tt = refs[29:]
    unpack(left, 0, kap, rr, ff)
    unpack(right, 2, kap, rr, ff)
    coef_x(2 * CX - 1, kap, cx)

    def coefs(us):
        for u in us:
            for x in (u, u + 2 * CX):
                coef_yz(x, kap, cy, cz)
            coef_x(u, kap, cx)
            coef_x(jnp.minimum(u + 2 * CX, EX - 2), kap, cx)

    groups(0, CX, coefs)

    def inverses(us):
        for u in us:
            for x in (u, u + 2 * CX - 2):
                inverse_fine(x, cx, cy, cz, i0, rr, u1, ff)

    groups(1, CX + 1, inverses)
    for i in range(CX // 2):
        for j in (i, i + CX):
            coarse_cond(j, kap, k1)
    for i in range(1, CX // 2 + 1):
        for j in (i, i + CX - 2):
            inverse_coarse(j, k1, i1, f1)

    def images(u, xs, masked=True):
        c = [u[xs[0] - 1]] + [u[x] for x in xs] + [u[xs[-1] + 1]]
        flux = [cx[x] * (c[i] - c[i + 1]) for i, x in enumerate([xs[0] - 1] + list(xs))]
        out = []
        for i, x in enumerate(xs):
            v = c[i + 1]
            gy = cy[x] * (v - roll(v, -1, 0))
            gz = cz[x] * (v - roll(v, -1, 1))
            w = (flux[i + 1] - flux[i]) + (gy - roll(gy, 1, 0)) + (gz - roll(gz, 1, 1))
            out.append(ff[x >> 3] * w if masked else w)
        return out

    def smooth(src, pair_range, out_range, put):
        def pairs(ps):
            xs = [2 * ps[0] + j for j in range(2 * len(ps))]
            im = images(u1, xs)
            for j, i in enumerate(ps):
                x, y = xs[2 * j], xs[2 * j + 1]
                s = (src[x] - im[2 * j]) + (src[y] - im[2 * j + 1])
                below = ff[x >> 3] * (i1[i] * pooled(s))
                u2[x] = u1[x] + below
                u2[y] = u1[y] + below

        groups(*pair_range, pairs)

        def last(xs):
            for x, w in zip(xs, images(u2, xs, False)):
                put(x, u2[x] + i0[x] * (src[x] - w))

        groups(*out_range, last)

    def put_d(x, v):
        dd[x] = v + fy[x >> 3]

    smooth(rr, (1, EX // 2 - 1), (3, EX - 3), put_d)

    def apply(xs):
        for x, w in zip(xs, images(dd, xs)):
            tt[x] = w
            u1[x] = i0[x] * w

    groups(4, EX - 4, apply)
    for x in range(CX):
        d_out[x] = dd[H + x, 0:CY, 0:CZ]

    def put_n(x, v):
        dd[x] = v

    zero = jnp.zeros((CY, CZ), F32)
    s_rz, s_dad = zero, zero
    for x in range(CX):
        s_rz = s_rz + rr[H + x, 0:CY, 0:CZ] * d_out[x]
        s_dad = s_dad + tt[H + x, 0:CY, 0:CZ] * d_out[x]
    smooth(tt, (3, EX // 2 - 3), (7, EX - 7), put_n)
    s_x, s_y, s_tau, s_om, s_d, s_cy, s_cz = (zero,) * 7
    f = ff[1]
    row = iota((EY, EZ), 0)
    lane = iota((EY, EZ), 1)
    mine = jnp.where((row < CY) & (lane < CZ), f, 0.0)
    own_f = f[0:CY, 0:CZ]
    row_o = iota((CY, CZ), 0)
    lane_o = iota((CY, CZ), 1)
    f_out[...] = own_f
    f_up_y = roll(f, -1, 0)
    f_up_z = roll(f, -1, 1)
    dif_y = mine - roll(mine, -1, 0)
    dif_z = mine - roll(mine, -1, 1)
    image_n = images(dd, list(range(H, H + CX)))
    for x in range(CX):
        at = H + x
        an = image_n[x][0:CY, 0:CZ]
        n = dd[at, 0:CY, 0:CZ]
        t = tt[at, 0:CY, 0:CZ]
        an_out[x] = an
        n_out[x] = n
        t_out[x] = t
        r_out[x] = rr[at, 0:CY, 0:CZ]
        b, c = cy[at], cz[at]
        gy = b * dif_y
        gz = c * dif_z
        e = ((gy - roll(gy, 1, 0)) + (gz - roll(gz, 1, 1)))[0:CY, 0:CZ]
        if x == 0:
            e = e + cx[H - 1, 0:CY, 0:CZ] * own_f
        if x == CX - 1:
            e = e + cx[at, 0:CY, 0:CZ] * own_f
        e = e * own_f
        e0_out[x] = e
        cut_y = jnp.where(
            row_o == CY - 1, (b * f_up_y)[0:CY, 0:CZ], jnp.where(row_o == 0, roll(b * f, 1, 0)[0:CY, 0:CZ], 0.0)
        ) * own_f
        cut_z = jnp.where(
            lane_o == CZ - 1, (c * f_up_z)[0:CY, 0:CZ], jnp.where(lane_o == 0, roll(c * f, 1, 1)[0:CY, 0:CZ], 0.0)
        ) * own_f
        ey_out[x] = cut_y
        ez_out[x] = cut_z
        s_x = s_x + t * n
        s_y = s_y + n * an
        s_tau = s_tau + t
        s_om = s_om + an
        s_d = s_d + e * own_f
        s_cy = s_cy + cut_y
        s_cz = s_cz + cut_z
    ex0 = cx[H - 1, 0:CY, 0:CZ] * own_f * ff[0, 0:CY, 0:CZ]
    ex1 = cx[H + CX - 1, 0:CY, 0:CZ] * own_f * ff[2, 0:CY, 0:CZ]
    ex_out[0] = ex0
    ex_out[1] = ex1
    at = iota((1, CZ), 1)
    z = lax.axis_index("gz")
    vectors = (
        s_tau, s_om, s_d, ex1,
        jnp.where(row_o == CY - 1, s_cy, 0.0), jnp.where(lane_o == CZ - 1, s_cz, 0.0),
    )
    line = jnp.zeros((1, CZ), F32)
    for i, v in enumerate(vectors):
        line = line + jnp.where(at == SLOT * i + z, total(v), 0.0)
    for i, v in enumerate((s_rz, s_dad, s_x, s_y)):
        line = line + jnp.where(at == 6 * SLOT + i, total(v), 0.0)
    msg[...] = jnp.broadcast_to(line[None], msg.shape)


def final_kernel(nx, ny, nz, gathered, inv, d_in, t_in, n_in, an_in, r_in, e0, ey, ez, ex, f_in, sol, res):
    vectors = [table(gathered, i, nx, ny, nz) for i in range(6)]
    tables = list(zip(*vectors))
    sums = jnp.sum(gathered[...], axis=0)
    at = iota((1, CZ), 1)

    def scalar(i):
        return jnp.sum(jnp.where(at == 6 * SLOT + i, sums, 0.0), axis=1, keepdims=True)

    rz, dad, xx, yy = (scalar(i) for i in range(4))
    tau = vectors[0]
    yt = coarse_solve(inv, [v * (1.0 / CELLS) for v in tau])
    add_x = jnp.zeros((1, CZ), F32)
    add_y = jnp.zeros((1, CZ), F32)
    for x in range(nx):
        y = yt[x]
        t = tables[x]
        add_x = add_x + t[0] * y
        cross = t[4] * roll(y, -nz, 1) + t[5] * roll(y, -1, 1)
        if x + 1 < nx:
            cross = cross + t[3] * yt[x + 1]
        add_y = add_y + y * (2.0 * t[1] + t[2] * y - 2.0 * cross)
    xx = xx + jnp.sum(add_x, axis=1, keepdims=True)
    yy = yy + jnp.sum(add_y, axis=1, keepdims=True)
    a0 = rz / dad
    new = a0 * a0 * xx - rz
    beta = new / rz
    zaz = dad - 2.0 * a0 * xx + a0 * a0 * yy
    a1 = new / (zaz - beta * beta * dad)
    near = neighbours(yt, nz, ny)
    shape = (CY, CZ)

    def wide(v, bx=1):
        return jnp.broadcast_to(v[bx : bx + 1], shape)

    y_own = wide(near[0, 0])
    y_y = jnp.where(iota(shape, 0) < CY // 2, wide(near[-1, 0]), wide(near[1, 0]))
    y_z = jnp.where(iota(shape, 1) < CZ // 2, wide(near[0, -1]), wide(near[0, 1]))
    f = f_in[...]
    c_d = jnp.broadcast_to(a0 + a1 * (1.0 + beta), shape)
    c_n = jnp.broadcast_to(a0 * a1, shape)
    for x in range(CX):
        n = n_in[x] + f * y_own
        an = an_in[x] + e0[x] * y_own - ey[x] * y_y - ez[x] * y_z
        if x == 0:
            an = an - ex[0] * wide(near[0, 0], 0)
        if x == CX - 1:
            an = an - ex[1] * wide(near[0, 0], 2)
        sol[x] = c_d * d_in[x] - c_n * n
        res[x] = r_in[x] - c_d * t_in[x] + c_n * an


def exchange(axis, to_low, to_high):
    size = lax.axis_size(axis)
    up = [(i, i + 1) for i in range(size - 1)]
    down = [(b, a) for a, b in up]
    return lax.ppermute(to_low, axis, down), lax.ppermute(to_high, axis, up)


def on_device(right_side, conductance, extents, coarse_factor):
    nx, ny, nz = (lax.axis_size(a) for a in ("gx", "gy", "gz"))
    sizes = (nx, ny, nz)
    any_space = pl.BlockSpec(memory_space=pl.ANY)
    msg = call(pack_kernel, [(nz, CY, CZ)], 3, name="pack", mib=PACK_MIB)(extents, right_side, conductance)[0]
    got = lax.all_to_all(msg, "gz", 0, 0, tiled=True)
    depth = 2 * CX + 2
    zh, to_low, to_high, line = call(
        rows_kernel, [(2, CY, CZ), (depth, H, CZ), (depth, H, CZ), (nx * ny, 1, CZ)], 3, name="rows"
    )(right_side, conductance, got)
    first = lax.all_to_all(line, ("gx", "gy"), 0, 0, tiled=True)
    y_high, y_low = exchange("gy", to_low, to_high)
    slab = call(
        slab_kernel, [(depth, EY, CZ)], 6, in_specs=[VMEM] * 5 + [any_space], name="slab"
    )(right_side, conductance, zh, y_high, y_low, first)[0]
    slab, factor = lax.optimization_barrier((slab, coarse_factor))
    nb = factor.shape[0] // CZ
    diagonal = call(diagonal_kernel, [(nb, CZ, CZ)], 1, name="diagonal")(factor)[0]
    x_high, x_low = exchange("gx", slab, slab)
    block = (CX, CY, CZ)
    wide = (EX, EY, EZ)
    half = (EX // 2, EY, EZ)
    third = (3, EY, EZ)
    arrays = [wide] * 6 + [half] * 2 + [wide]
    inv, ff, f1, fy, *fields = call(
        functools.partial(coarse_kernel, *sizes), [factor.shape] + [third] * 3 + arrays, 4, name="coarse"
    )(factor, diagonal, first, slab)
    outs = call(
        main_kernel,
        arrays + [block] * 8 + [(2, CY, CZ), (CY, CZ), (nz, 1, CZ)],
        14,
        scratch=[wide] * 3,
        aliases={5 + i: i for i in range(9)},
        name="fields",
    )(x_low, x_high, ff, f1, fy, *fields)[9:]
    part = lax.all_to_all(outs[-1], "gz", 0, 0, tiled=True)
    line = call(sum_kernel, [(nx * ny, 1, CZ)], 1, name="sum")(part)[0]
    second = lax.all_to_all(line, ("gx", "gy"), 0, 0, tiled=True)
    sol, res = call(functools.partial(final_kernel, *sizes), [block] * 2, 12, name="final")(
        second, inv, *outs[:-1]
    )
    return sol, res


def solution(mesh):
    spec = P("gx", "gy", "gz")
    return jax.shard_map(
        on_device, mesh=mesh, in_specs=(spec, spec, spec, P()), out_specs=(spec, spec), check_vma=False
    )
```

```python
import functools

import jax
import jax.numpy as jnp
from jax import lax
from jax.experimental import pallas as pl
from jax.experimental.pallas import tpu as pltpu
from jax.sharding import PartitionSpec as P

F32 = jnp.float32
PACK_MIB = 60
OMEGA = 0.8
CX, CY, CZ = 8, 16, 128
CELLS = CX * CY * CZ
H = 8
EX, EY, EZ = CX + 2 * H, CY + 2 * H, 2 * CZ
SLOT = 16
VMEM = pl.BlockSpec(memory_space=pltpu.VMEM)
SMEM = pl.BlockSpec(memory_space=pltpu.SMEM)


def call(kernel, out_shapes, n_in, scratch=(), in_specs=None, name=None, aliases=None, mib=24):
    outs = [jax.ShapeDtypeStruct(s, F32) for s in out_shapes]
    return pl.pallas_call(
        kernel,
        out_shape=outs,
        in_specs=in_specs or [VMEM] * n_in,
        out_specs=[VMEM] * len(outs),
        scratch_shapes=[pltpu.VMEM(s, F32) for s in scratch],
        input_output_aliases=aliases or {},
        compiler_params=pltpu.CompilerParams(vmem_limit_bytes=mib * 1024 * 1024),
        name=name,
    )


def roll(x, shift, axis):
    return pltpu.roll(x, shift % x.shape[axis], axis)


def iota(shape, dim):
    return lax.broadcasted_iota(jnp.int32, shape, dim)


def total(x):
    return jnp.sum(jnp.sum(x, axis=0, keepdims=True), axis=1, keepdims=True)


def pack_kernel(ext, rhs, cond, msg):
    nz = msg.shape[0]
    lane = iota((CY, CZ), 1)
    row = iota((CY, CZ), 0)
    a = jnp.zeros((CY, CZ), F32)
    b = jnp.zeros((CY, CZ), F32)
    acc = jnp.zeros((CY, CZ), F32)
    count = jnp.broadcast_to(ext[0], (CY, CZ))
    inside = lane < count
    z = lax.axis_index("gz")
    for x in range(CX):
        k = cond[x]
        r = rhs[x]
        acc = acc + jnp.where(inside, r, 0.0)
        hi = (lane >= 16 * x) & (lane < 16 * x + H)
        start = (16 * x - H) % CZ
        lo = (lane >= start) & (lane < start + H)
        a = jnp.where(hi, roll(k, 16 * x, 1), jnp.where(lo, roll(r, 16 * x - H, 1), a))
        b = jnp.where(lo, roll(k, 16 * x, 1), jnp.where(hi, roll(r, 16 * x + H, 1), b))
    info = jnp.where(row == 0, total(acc) / CELLS, count.astype(F32))
    a = jnp.where((lane == CZ - 1) & (row < 2), info, a)
    b = jnp.where((lane == 0) & (row < 2), info, b)
    for i in range(nz):
        msg[i] = b

    @pl.when(z > 0)
    def _():
        msg[z - 1] = a


def rows_kernel(rhs, cond, got, slab, line):
    nz = got.shape[0]
    z = lax.axis_index("gz")
    low_half = iota((CY, CZ), 1) % 16 < H
    up = jnp.minimum(z + 1, nz - 1)
    a = jnp.where(jnp.full((CY, CZ), z, jnp.int32) < nz - 1, got[up], 0.0)
    b = jnp.where(jnp.full((CY, CZ), z, jnp.int32) > 0, got[jnp.maximum(z - 1, 0)], 0.0)
    lane = iota((8, CZ), 1)
    info = jnp.zeros((8, CZ), F32)
    for i in range(nz):
        v = got[i, 0:8]
        info = jnp.where(lane == i, roll(v, i, 1), info)
    info = jnp.where(lane == z + 1, pltpu.roll(a[0:8], z + 2, 1), info)
    info = jnp.where(lane < nz, info, 0.0)
    line[...] = jnp.broadcast_to((info[0:1] + roll(info[1:2], SLOT, 1))[None], line.shape)
    slab[0:CX] = cond[...]
    slab[CX : 2 * CX] = rhs[...]
    slab[2 * CX] = jnp.where(low_half, a, b)
    slab[2 * CX + 1] = jnp.where(low_half, roll(a, H, 1), roll(b, -H, 1))


def y_kernel(left, own, right, after, to_low, to_high):
    n = own.shape[0]
    for i, src in enumerate((left, own, right)):
        to_low[i * n : (i + 1) * n] = src[:, 0:H]
        to_high[i * n : (i + 1) * n] = src[:, CY - H : CY]


def sum_kernel(part, line):
    line[...] = jnp.broadcast_to(jnp.sum(part[...], axis=0, keepdims=True), line.shape)


def table(rows, i, nx, ny, nz):
    out = []
    for x in range(nx):
        v = rows[x * ny : (x + 1) * ny].reshape(ny, CZ)
        v = jnp.where(iota((ny, CZ), 1) < nz, roll(v, -SLOT * i, 1), 0.0)
        v = pltpu.roll(v, 0, 1, stride=nz, stride_axis=0)
        out.append(jnp.sum(v, axis=0, keepdims=True))
    return out


def dot(a, b):
    return jnp.dot(a, b, precision=lax.Precision.HIGHEST, preferred_element_type=F32)


def diagonal_kernel(factor, out):
    n = factor.shape[0]
    bs = CZ
    nb = n // bs
    i = iota((bs, bs), 0)
    j = iota((bs, bs), 1)
    eye = i == j
    low = [factor[b * bs : (b + 1) * bs, b * bs : (b + 1) * bs].astype(F32) for b in range(nb)]
    inv = []
    for lb in low:
        diag = jnp.where(eye, lb, 0.0)
        col = 1.0 / jnp.sum(diag, axis=1, keepdims=True)
        row = 1.0 / jnp.sum(diag, axis=0, keepdims=True)
        pair = (i // 2 == j // 2) & (i > j)
        inv.append(jnp.where(eye, col, 0.0) - jnp.where(pair, col * lb * row, 0.0))
    s = 2
    while s < bs:
        mask = (i // (2 * s) == j // (2 * s)) & (i // s > j // s)
        mid = [dot(jnp.where(mask, lb, 0.0), x) for lb, x in zip(low, inv)]
        inv = [x - dot(x, m) for x, m in zip(inv, mid)]
        s *= 2
    for b in range(nb):
        out[b] = inv[b]


def inverse_of(factor, diagonal, out):
    n = factor.shape[0]
    bs = CZ
    for b in range(n // bs):
        out[b * bs : (b + 1) * bs, b * bs : (b + 1) * bs] = diagonal[b]
    s = bs
    while s < n:
        for at in range(0, n, 2 * s):
            for lo in range(s, 2 * s, bs):
                for hi in range(lo - s + bs, s, bs):
                    out[at + lo - s : at + lo - s + bs, at + hi : at + hi + bs] = jnp.zeros((bs, bs), F32)
            if s > bs:
                for lo in range(s, 2 * s, bs):
                    for hi in range(lo + bs, 2 * s, bs):
                        out[at + lo : at + lo + bs, at + hi : at + hi + bs] = jnp.zeros((bs, bs), F32)
            mid = dot(factor[at + s : at + 2 * s, at : at + s].astype(F32), out[at : at + s, at : at + s])
            out[at + s : at + 2 * s, at : at + s] = -dot(out[at + s : at + 2 * s, at + s : at + 2 * s], mid)
        s *= 2


def coarse_solve(inv, means):
    nb = len(means)
    bs = CZ
    rows = [jnp.zeros((1, bs), F32) for _ in range(nb)]
    for a in range(nb):
        acc = inv[a * bs : (a + 1) * bs, 0:bs] * means[0]
        for c in range(1, a + 1):
            acc = acc + inv[a * bs : (a + 1) * bs, c * bs : (c + 1) * bs] * means[c]
        u = jnp.sum(acc, axis=1, keepdims=True)
        for c in range(a + 1):
            rows[c] = rows[c] + jnp.sum(inv[a * bs : (a + 1) * bs, c * bs : (c + 1) * bs] * u, axis=0, keepdims=True)
    return rows


def neighbours(rows, nz, ny):
    nx = len(rows)
    x = lax.axis_index("gx")
    y = lax.axis_index("gy")
    z = lax.axis_index("gz")
    zero = jnp.zeros((1, CZ), F32)
    picked = []
    for dx in (-1, 0, 1):
        v = zero
        for r in range(nx):
            v = v + jnp.where(jnp.full((1, CZ), x + dx, jnp.int32) == r, rows[r], 0.0)
        picked.append(v)
    row = iota((8, CZ), 0)
    stack = jnp.where(row == 0, picked[0], jnp.where(row == 1, picked[1], jnp.where(row == 2, picked[2], 0.0)))
    lane = iota((8, CZ), 1)
    out = {}
    for dy in (-1, 0, 1):
        for dz in (-1, 0, 1):
            ok = (y + dy >= 0) & (y + dy < ny) & (z + dz >= 0) & (z + dz < nz)
            target = jnp.where(ok, (y + dy) * nz + z + dz, -1)
            out[dy, dz] = jnp.sum(jnp.where(lane == target, stack, 0.0), axis=1, keepdims=True)
    return out


def groups(low, high, body, step=1):
    count = high - low
    size = max(u for u in range(1, count // 2 + 1) if count % u == 0)

    def go(i, carry):
        body([low + i * size + u for u in range(size)])
        return carry

    lax.fori_loop(0, count // size, go, 0)


def unpack(src, high, low, bx, kap, rr, ff):
    n = src.shape[0]
    for rows, part, at in ((slice(0, CY), src, 0), (slice(CY, CY + H), high, bx * n), (slice(CY + H, EY), low, bx * n)):
        zk = part[at + 2 * CX]
        zr = part[at + 2 * CX + 1]
        f0 = ff[bx, rows, 0:CZ]
        f1 = ff[bx, rows, CZ:EZ]
        for x in range(CX):
            to = bx * CX + x
            kap[to, rows, 0:CZ] = part[at + x]
            kap[to, rows, CZ:EZ] = roll(zk, -16 * x, 1)
            rr[to, rows, 0:CZ] = part[at + CX + x] * f0
            rr[to, rows, CZ:EZ] = roll(zr, -16 * x, 1) * f1


def pooled(s):
    even = iota(s.shape, 0) % 2 == 0
    s = s + jnp.where(even, roll(s, -1, 0), roll(s, 1, 0))
    even = iota(s.shape, 1) % 2 == 0
    return s + jnp.where(even, roll(s, -1, 1), roll(s, 1, 1))


def coef_x(x, kap, cx):
    cx[x] = 0.5 * (kap[x] + kap[x + 1])


def coef_yz(x, kap, cy, cz):
    k = kap[x]
    cy[x] = 0.5 * (k + roll(k, -1, 0))
    cz[x] = 0.5 * (k + roll(k, -1, 1))


def inverse_fine(x, cx, cy, cz, i0, rr, u1, ff):
    f = ff[x >> 3]
    b, c = cy[x], cz[x]
    s = cx[x] + cx[x - 1] + b + roll(b, 1, 0) + c + roll(c, 1, 1)
    v = OMEGA * f / (s + 1.0 - f)
    i0[x] = v
    u1[x] = v * rr[x]


def coarse_cond(i, kap, k1):
    k1[i] = pooled(kap[2 * i] + kap[2 * i + 1]) * 0.125


def inverse_coarse(i, k1, i1, f1):
    k = k1[i]
    f = f1[i >> 2]
    s = k1[i - 1] + k1[i + 1] + roll(k, 2, 0) + roll(k, -2, 0) + roll(k, 2, 1) + roll(k, -2, 1)
    s = 3.0 * k + 0.5 * s
    i1[i] = OMEGA * f / (4.0 * s + 1.0 - f)


ROW_PARTS = ((0, 0), (8, 0), (16, 1), (24, -1))


def coarse_kernel(nx, ny, nz, factor, diagonal, gathered, inv, ff, f1, fy):
    inverse_of(factor, diagonal, inv)
    lane8 = iota((8, CZ), 1)
    lane8f = lane8.astype(F32)
    even8f = (lane8 - lane8 % 2).astype(F32)
    valid = (lane8 < H) | (lane8 >= CZ - H)
    ext = neighbours(table(gathered, 1, nx, ny, nz), nz, ny)
    y0 = neighbours(coarse_solve(inv, table(gathered, 0, nx, ny, nz)), nz, ny)
    for bx in range(3):
        for r, dy in ROW_PARTS:
            e = {dz: jnp.broadcast_to(ext[dy, dz][bx : bx + 1], (8, CZ)) for dz in (-1, 0, 1)}
            v = {dz: jnp.broadcast_to(y0[dy, dz][bx : bx + 1], (8, CZ)) for dz in (-1, 0, 1)}
            far = jnp.where(lane8 < CZ // 2, e[1], e[-1])
            m0 = jnp.where(lane8f < e[0], 1.0, 0.0)
            m1 = jnp.where(valid & (lane8f < far), 1.0, 0.0)
            ff[bx, r : r + 8, 0:CZ] = m0
            ff[bx, r : r + 8, CZ:EZ] = m1
            f1[bx, r : r + 8, 0:CZ] = jnp.where(even8f < e[0], 1.0, 0.0)
            f1[bx, r : r + 8, CZ:EZ] = jnp.where(valid & (even8f < far), 1.0, 0.0)
            fy[bx, r : r + 8, 0:CZ] = m0 * v[0]
            fy[bx, r : r + 8, CZ:EZ] = m1 * jnp.where(lane8 < CZ // 2, v[1], v[-1])


def main_kernel(left, own, right, high, low, ff, f1, fy, *refs):
    (d_out, t_out, n_out, an_out, r_out, e0_out, ey_out, ez_out, ex_out, f_out, msg) = refs[:11]
    kap, rr, cx, cy, cz, i0, u1, u2, dd, tt, k1, i1 = refs[11:]
    for bx, src in enumerate((left, own, right)):
        unpack(src, high, low, bx, kap, rr, ff)

    def coefs(xs):
        for x in xs:
            k = kap[x]
            cx[x] = 0.5 * (k + kap[jnp.minimum(x + 1, EX - 1)])
            coef_yz(x, kap, cy, cz)

    groups(0, EX, coefs)

    def inverses(xs):
        for x in xs:
            inverse_fine(x, cx, cy, cz, i0, rr, u1, ff)

    groups(1, EX - 1, inverses)

    def conds(xs):
        for i in xs:
            coarse_cond(i, kap, k1)

    groups(0, EX // 2, conds)

    def coarse_inverses(xs):
        for i in xs:
            inverse_coarse(i, k1, i1, f1)

    groups(1, EX // 2 - 1, coarse_inverses)

    def images(u, xs, masked=True):
        c = [u[xs[0] - 1]] + [u[x] for x in xs] + [u[xs[-1] + 1]]
        flux = [cx[x] * (c[i] - c[i + 1]) for i, x in enumerate([xs[0] - 1] + list(xs))]
        out = []
        for i, x in enumerate(xs):
            v = c[i + 1]
            gy = cy[x] * (v - roll(v, -1, 0))
            gz = cz[x] * (v - roll(v, -1, 1))
            w = (flux[i + 1] - flux[i]) + (gy - roll(gy, 1, 0)) + (gz - roll(gz, 1, 1))
            out.append(ff[x >> 3] * w if masked else w)
        return out

    def smooth(src, pair_range, out_range, put):
        def pairs(ps):
            xs = [2 * ps[0] + j for j in range(2 * len(ps))]
            im = images(u1, xs)
            for j, i in enumerate(ps):
                x, y = xs[2 * j], xs[2 * j + 1]
                s = (src[x] - im[2 * j]) + (src[y] - im[2 * j + 1])
                below = ff[x >> 3] * (i1[i] * pooled(s))
                u2[x] = u1[x] + below
                u2[y] = u1[y] + below

        groups(*pair_range, pairs)

        def last(xs):
            for x, w in zip(xs, images(u2, xs, False)):
                put(x, u2[x] + i0[x] * (src[x] - w))

        groups(*out_range, last)

    def put_d(x, v):
        dd[x] = v + fy[x >> 3]

    smooth(rr, (1, EX // 2 - 1), (3, EX - 3), put_d)

    def apply(xs):
        for x, w in zip(xs, images(dd, xs)):
            tt[x] = w
            u1[x] = i0[x] * w

    groups(4, EX - 4, apply)
    for x in range(CX):
        d_out[x] = dd[H + x, 0:CY, 0:CZ]

    def put_n(x, v):
        dd[x] = v

    zero = jnp.zeros((CY, CZ), F32)
    s_rz, s_dad = zero, zero
    for x in range(CX):
        s_rz = s_rz + rr[H + x, 0:CY, 0:CZ] * d_out[x]
        s_dad = s_dad + tt[H + x, 0:CY, 0:CZ] * d_out[x]
    smooth(tt, (3, EX // 2 - 3), (7, EX - 7), put_n)
    s_x, s_y, s_tau, s_om, s_d, s_cy, s_cz = (zero,) * 7
    f = ff[1]
    row = iota((EY, EZ), 0)
    lane = iota((EY, EZ), 1)
    mine = jnp.where((row < CY) & (lane < CZ), f, 0.0)
    own_f = f[0:CY, 0:CZ]
    row_o = iota((CY, CZ), 0)
    lane_o = iota((CY, CZ), 1)
    f_out[...] = own_f
    f_up_y = roll(f, -1, 0)
    f_up_z = roll(f, -1, 1)
    dif_y = mine - roll(mine, -1, 0)
    dif_z = mine - roll(mine, -1, 1)
    image_n = images(dd, list(range(H, H + CX)))
    for x in range(CX):
        at = H + x
        an = image_n[x][0:CY, 0:CZ]
        n = dd[at, 0:CY, 0:CZ]
        t = tt[at, 0:CY, 0:CZ]
        an_out[x] = an
        n_out[x] = n
        t_out[x] = t
        r_out[x] = rr[at, 0:CY, 0:CZ]
        b, c = cy[at], cz[at]
        gy = b * dif_y
        gz = c * dif_z
        e = ((gy - roll(gy, 1, 0)) + (gz - roll(gz, 1, 1)))[0:CY, 0:CZ]
        if x == 0:
            e = e + cx[H - 1, 0:CY, 0:CZ] * own_f
        if x == CX - 1:
            e = e + cx[at, 0:CY, 0:CZ] * own_f
        e = e * own_f
        e0_out[x] = e
        cut_y = jnp.where(
            row_o == CY - 1, (b * f_up_y)[0:CY, 0:CZ], jnp.where(row_o == 0, roll(b * f, 1, 0)[0:CY, 0:CZ], 0.0)
        ) * own_f
        cut_z = jnp.where(
            lane_o == CZ - 1, (c * f_up_z)[0:CY, 0:CZ], jnp.where(lane_o == 0, roll(c * f, 1, 1)[0:CY, 0:CZ], 0.0)
        ) * own_f
        ey_out[x] = cut_y
        ez_out[x] = cut_z
        s_x = s_x + t * n
        s_y = s_y + n * an
        s_tau = s_tau + t
        s_om = s_om + an
        s_d = s_d + e * own_f
        s_cy = s_cy + cut_y
        s_cz = s_cz + cut_z
    ex0 = cx[H - 1, 0:CY, 0:CZ] * own_f * ff[0, 0:CY, 0:CZ]
    ex1 = cx[H + CX - 1, 0:CY, 0:CZ] * own_f * ff[2, 0:CY, 0:CZ]
    ex_out[0] = ex0
    ex_out[1] = ex1
    at = iota((1, CZ), 1)
    z = lax.axis_index("gz")
    vectors = (
        s_tau, s_om, s_d, ex1,
        jnp.where(row_o == CY - 1, s_cy, 0.0), jnp.where(lane_o == CZ - 1, s_cz, 0.0),
    )
    line = jnp.zeros((1, CZ), F32)
    for i, v in enumerate(vectors):
        line = line + jnp.where(at == SLOT * i + z, total(v), 0.0)
    for i, v in enumerate((s_rz, s_dad, s_x, s_y)):
        line = line + jnp.where(at == 6 * SLOT + i, total(v), 0.0)
    msg[...] = jnp.broadcast_to(line[None], msg.shape)


def final_kernel(nx, ny, nz, gathered, inv, d_in, t_in, n_in, an_in, r_in, e0, ey, ez, ex, f_in, sol, res):
    vectors = [table(gathered, i, nx, ny, nz) for i in range(6)]
    tables = list(zip(*vectors))
    sums = jnp.sum(gathered[...], axis=0)
    at = iota((1, CZ), 1)

    def scalar(i):
        return jnp.sum(jnp.where(at == 6 * SLOT + i, sums, 0.0), axis=1, keepdims=True)

    rz, dad, xx, yy = (scalar(i) for i in range(4))
    tau = vectors[0]
    yt = coarse_solve(inv, [v * (1.0 / CELLS) for v in tau])
    add_x = jnp.zeros((1, CZ), F32)
    add_y = jnp.zeros((1, CZ), F32)
    for x in range(nx):
        y = yt[x]
        t = tables[x]
        add_x = add_x + t[0] * y
        cross = t[4] * roll(y, -nz, 1) + t[5] * roll(y, -1, 1)
        if x + 1 < nx:
            cross = cross + t[3] * yt[x + 1]
        add_y = add_y + y * (2.0 * t[1] + t[2] * y - 2.0 * cross)
    xx = xx + jnp.sum(add_x, axis=1, keepdims=True)
    yy = yy + jnp.sum(add_y, axis=1, keepdims=True)
    a0 = rz / dad
    new = a0 * a0 * xx - rz
    beta = new / rz
    zaz = dad - 2.0 * a0 * xx + a0 * a0 * yy
    a1 = new / (zaz - beta * beta * dad)
    near = neighbours(yt, nz, ny)
    shape = (CY, CZ)

    def wide(v, bx=1):
        return jnp.broadcast_to(v[bx : bx + 1], shape)

    y_own = wide(near[0, 0])
    y_y = jnp.where(iota(shape, 0) < CY // 2, wide(near[-1, 0]), wide(near[1, 0]))
    y_z = jnp.where(iota(shape, 1) < CZ // 2, wide(near[0, -1]), wide(near[0, 1]))
    f = f_in[...]
    c_d = jnp.broadcast_to(a0 + a1 * (1.0 + beta), shape)
    c_n = jnp.broadcast_to(a0 * a1, shape)
    for x in range(CX):
        n = n_in[x] + f * y_own
        an = an_in[x] + e0[x] * y_own - ey[x] * y_y - ez[x] * y_z
        if x == 0:
            an = an - ex[0] * wide(near[0, 0], 0)
        if x == CX - 1:
            an = an - ex[1] * wide(near[0, 0], 2)
        sol[x] = c_d * d_in[x] - c_n * n
        res[x] = r_in[x] - c_d * t_in[x] + c_n * an


def exchange(axis, to_low, to_high):
    size = lax.axis_size(axis)
    up = [(i, i + 1) for i in range(size - 1)]
    down = [(b, a) for a, b in up]
    return lax.ppermute(to_low, axis, down), lax.ppermute(to_high, axis, up)


def on_device(right_side, conductance, extents, coarse_factor):
    nx, ny, nz = (lax.axis_size(a) for a in ("gx", "gy", "gz"))
    sizes = (nx, ny, nz)
    any_space = pl.BlockSpec(memory_space=pl.ANY)
    msg = call(pack_kernel, [(nz, CY, CZ)], 3, name="pack", mib=PACK_MIB)(extents, right_side, conductance)[0]
    got = lax.all_to_all(msg, "gz", 0, 0, tiled=True)
    depth = 2 * CX + 2
    depth = 2 * CX + 2
    slab, line = call(rows_kernel, [(depth, CY, CZ), (nx * ny, 1, CZ)], 3, name="rows")(right_side, conductance, got)
    x_high, x_low = exchange("gx", slab, slab)
    first = lax.all_to_all(line, ("gx", "gy"), 0, 0, tiled=True)
    to_low, to_high = call(
        y_kernel, [(3 * depth, H, CZ)] * 2, 4, in_specs=[VMEM] * 3 + [any_space], name="faces"
    )(x_low, slab, x_high, first)
    to_low, to_high, factor = lax.optimization_barrier((to_low, to_high, coarse_factor))
    y_high, y_low = exchange("gy", to_low, to_high)
    nb = factor.shape[0] // CZ
    diagonal = call(diagonal_kernel, [(nb, CZ, CZ)], 1, name="diagonal")(factor)[0]
    block = (CX, CY, CZ)
    wide = (EX, EY, EZ)
    half = (EX // 2, EY, EZ)
    third = (3, EY, EZ)
    inv, ff, f1, fy = call(
        functools.partial(coarse_kernel, *sizes), [factor.shape] + [third] * 3, 3, name="coarse"
    )(factor, diagonal, first)
    outs = call(
        main_kernel,
        [block] * 8 + [(2, CY, CZ), (CY, CZ), (nz, 1, CZ)],
        8,
        scratch=[wide] * 10 + [half] * 2,
        name="fields",
    )(x_low, slab, x_high, y_high, y_low, ff, f1, fy)
    part = lax.all_to_all(outs[-1], "gz", 0, 0, tiled=True)
    line = call(sum_kernel, [(nx * ny, 1, CZ)], 1, name="sum")(part)[0]
    second = lax.all_to_all(line, ("gx", "gy"), 0, 0, tiled=True)
    sol, res = call(functools.partial(final_kernel, *sizes), [block] * 2, 12, name="final")(
        second, inv, *outs[:-1]
    )
    return sol, res


def solution(mesh):
    spec = P("gx", "gy", "gz")
    return jax.shard_map(
        on_device, mesh=mesh, in_specs=(spec, spec, spec, P()), out_specs=(spec, spec), check_vma=False
    )
```

```python
import functools

import jax
import jax.numpy as jnp
from jax import lax
from jax.experimental import pallas as pl
from jax.experimental.pallas import tpu as pltpu
from jax.sharding import PartitionSpec as P

F32 = jnp.float32
PACK_MIB = 48
OMEGA = 0.8
CX, CY, CZ = 8, 16, 128
CELLS = CX * CY * CZ
H = 8
EX, EY, EZ = CX + 2 * H, CY + 2 * H, 2 * CZ
SLOT = 16
VMEM = pl.BlockSpec(memory_space=pltpu.VMEM)
SMEM = pl.BlockSpec(memory_space=pltpu.SMEM)


def call(kernel, out_shapes, n_in, scratch=(), in_specs=None, name=None, aliases=None, mib=24):
    outs = [jax.ShapeDtypeStruct(s, F32) for s in out_shapes]
    return pl.pallas_call(
        kernel,
        out_shape=outs,
        in_specs=in_specs or [VMEM] * n_in,
        out_specs=[VMEM] * len(outs),
        scratch_shapes=[pltpu.VMEM(s, F32) for s in scratch],
        input_output_aliases=aliases or {},
        compiler_params=pltpu.CompilerParams(vmem_limit_bytes=mib * 1024 * 1024),
        name=name,
    )


def roll(x, shift, axis):
    return pltpu.roll(x, shift % x.shape[axis], axis)


def iota(shape, dim):
    return lax.broadcasted_iota(jnp.int32, shape, dim)


def total(x):
    return jnp.sum(jnp.sum(x, axis=0, keepdims=True), axis=1, keepdims=True)


def pack_kernel(ext, rhs, cond, msg):
    nz = msg.shape[0]
    lane = iota((CY, CZ), 1)
    row = iota((CY, CZ), 0)
    a = jnp.zeros((CY, CZ), F32)
    b = jnp.zeros((CY, CZ), F32)
    acc = jnp.zeros((CY, CZ), F32)
    count = jnp.broadcast_to(ext[0], (CY, CZ))
    inside = lane < count
    z = lax.axis_index("gz")
    for x in range(CX):
        k = cond[x]
        r = rhs[x]
        acc = acc + jnp.where(inside, r, 0.0)
        hi = (lane >= 16 * x) & (lane < 16 * x + H)
        start = (16 * x - H) % CZ
        lo = (lane >= start) & (lane < start + H)
        a = jnp.where(hi, roll(k, 16 * x, 1), jnp.where(lo, roll(r, 16 * x - H, 1), a))
        b = jnp.where(lo, roll(k, 16 * x, 1), jnp.where(hi, roll(r, 16 * x + H, 1), b))
    info = jnp.where(row == 0, total(acc) / CELLS, count.astype(F32))
    a = jnp.where((lane == CZ - 1) & (row < 2), info, a)
    b = jnp.where((lane == 0) & (row < 2), info, b)
    for i in range(nz):
        msg[i] = b

    @pl.when(z > 0)
    def _():
        msg[z - 1] = a


def rows_kernel(rhs, cond, got, zh, to_low, to_high, line):
    nz = got.shape[0]
    z = lax.axis_index("gz")
    low_half = iota((CY, CZ), 1) % 16 < H
    up = jnp.minimum(z + 1, nz - 1)
    a = jnp.where(jnp.full((CY, CZ), z, jnp.int32) < nz - 1, got[up], 0.0)
    b = jnp.where(jnp.full((CY, CZ), z, jnp.int32) > 0, got[jnp.maximum(z - 1, 0)], 0.0)
    lane = iota((8, CZ), 1)
    info = jnp.zeros((8, CZ), F32)
    for i in range(nz):
        v = got[i, 0:8]
        info = jnp.where(lane == i, roll(v, i, 1), info)
    info = jnp.where(lane == z + 1, pltpu.roll(a[0:8], z + 2, 1), info)
    info = jnp.where(lane < nz, info, 0.0)
    line[...] = jnp.broadcast_to((info[0:1] + roll(info[1:2], SLOT, 1))[None], line.shape)
    zk = jnp.where(low_half, a, b)
    zr = jnp.where(low_half, roll(a, H, 1), roll(b, -H, 1))
    zh[0] = zk
    zh[1] = zr
    to_low[0:CX] = cond[:, 0:H, :]
    to_low[CX : 2 * CX] = rhs[:, 0:H, :]
    to_low[2 * CX] = zk[0:H]
    to_low[2 * CX + 1] = zr[0:H]
    to_high[0:CX] = cond[:, CY - H : CY, :]
    to_high[CX : 2 * CX] = rhs[:, CY - H : CY, :]
    to_high[2 * CX] = zk[CY - H : CY]
    to_high[2 * CX + 1] = zr[CY - H : CY]


def x_tiles():
    at = 0
    cond, rhs = {}, {}
    for layer in range(1, H + 1):
        for part, whole, none in ((cond, 5, 9), (rhs, 4, 8)):
            n = 4 if layer <= whole else 3 if layer < none else 0
            part[layer] = (at, n)
            at += n
    return cond, rhs, at


X_TILES = x_tiles()[2] + 8


def slab_kernel(rhs, cond, zh, from_high, from_low, after, slab, to_low, to_high):
    slab[0:CX, 0:CY] = cond[...]
    slab[CX : 2 * CX, 0:CY] = rhs[...]
    slab[2 * CX : 2 * CX + 2, 0:CY] = zh[...]
    slab[:, CY : CY + H] = from_high[...]
    slab[:, CY + H : EY] = from_low[...]
    in_cond, in_rhs, z_at = x_tiles()
    near = iota((8, CZ), 0) < 4
    for msg, flip in ((to_low, False), (to_high, True)):
        for x in range(CX):
            layer = H - x if flip else x + 1
            for part, base, src in ((in_cond, 0, cond), (in_rhs, CX, rhs)):
                at, n = part[layer]
                if n == 0:
                    continue
                msg[at] = src[x, 0:8]
                msg[at + 1] = src[x, 8:16]
                high, low = from_high[base + x], from_low[base + x]
                if n == 4:
                    msg[at + 2] = high
                    msg[at + 3] = low
                else:
                    msg[at + 2] = jnp.where(near, high, low)
        for i in range(2):
            at = z_at + 4 * i
            msg[at] = zh[i, 0:8]
            msg[at + 1] = zh[i, 8:16]
            msg[at + 2] = from_high[2 * CX + i]
            msg[at + 3] = from_low[2 * CX + i]


def sum_kernel(part, line):
    line[...] = jnp.broadcast_to(jnp.sum(part[...], axis=0, keepdims=True), line.shape)


def table(rows, i, nx, ny, nz):
    out = []
    for x in range(nx):
        v = rows[x * ny : (x + 1) * ny].reshape(ny, CZ)
        v = jnp.where(iota((ny, CZ), 1) < nz, roll(v, -SLOT * i, 1), 0.0)
        v = pltpu.roll(v, 0, 1, stride=nz, stride_axis=0)
        out.append(jnp.sum(v, axis=0, keepdims=True))
    return out


def dot(a, b):
    return jnp.dot(a, b, precision=lax.Precision.HIGHEST, preferred_element_type=F32)


def diagonal_kernel(factor, out):
    n = factor.shape[0]
    bs = CZ
    nb = n // bs
    i = iota((bs, bs), 0)
    j = iota((bs, bs), 1)
    eye = i == j
    low = [factor[b * bs : (b + 1) * bs, b * bs : (b + 1) * bs].astype(F32) for b in range(nb)]
    inv = []
    for lb in low:
        diag = jnp.where(eye, lb, 0.0)
        col = 1.0 / jnp.sum(diag, axis=1, keepdims=True)
        row = 1.0 / jnp.sum(diag, axis=0, keepdims=True)
        pair = (i // 2 == j // 2) & (i > j)
        inv.append(jnp.where(eye, col, 0.0) - jnp.where(pair, col * lb * row, 0.0))
    s = 2
    while s < bs:
        mask = (i // (2 * s) == j // (2 * s)) & (i // s > j // s)
        mid = [dot(jnp.where(mask, lb, 0.0), x) for lb, x in zip(low, inv)]
        inv = [x - dot(x, m) for x, m in zip(inv, mid)]
        s *= 2
    for b in range(nb):
        out[b] = inv[b]


def inverse_of(factor, diagonal, out):
    n = factor.shape[0]
    bs = CZ
    for b in range(n // bs):
        out[b * bs : (b + 1) * bs, b * bs : (b + 1) * bs] = diagonal[b]
    s = bs
    while s < n:
        for at in range(0, n, 2 * s):
            for lo in range(s, 2 * s, bs):
                for hi in range(lo - s + bs, s, bs):
                    out[at + lo - s : at + lo - s + bs, at + hi : at + hi + bs] = jnp.zeros((bs, bs), F32)
            if s > bs:
                for lo in range(s, 2 * s, bs):
                    for hi in range(lo + bs, 2 * s, bs):
                        out[at + lo : at + lo + bs, at + hi : at + hi + bs] = jnp.zeros((bs, bs), F32)
            mid = dot(factor[at + s : at + 2 * s, at : at + s].astype(F32), out[at : at + s, at : at + s])
            out[at + s : at + 2 * s, at : at + s] = -dot(out[at + s : at + 2 * s, at + s : at + 2 * s], mid)
        s *= 2


def coarse_solve(inv, means):
    nb = len(means)
    bs = CZ
    rows = [jnp.zeros((1, bs), F32) for _ in range(nb)]
    for a in range(nb):
        acc = inv[a * bs : (a + 1) * bs, 0:bs] * means[0]
        for c in range(1, a + 1):
            acc = acc + inv[a * bs : (a + 1) * bs, c * bs : (c + 1) * bs] * means[c]
        u = jnp.sum(acc, axis=1, keepdims=True)
        for c in range(a + 1):
            rows[c] = rows[c] + jnp.sum(inv[a * bs : (a + 1) * bs, c * bs : (c + 1) * bs] * u, axis=0, keepdims=True)
    return rows


def neighbours(rows, nz, ny):
    nx = len(rows)
    x = lax.axis_index("gx")
    y = lax.axis_index("gy")
    z = lax.axis_index("gz")
    zero = jnp.zeros((1, CZ), F32)
    picked = []
    for dx in (-1, 0, 1):
        v = zero
        for r in range(nx):
            v = v + jnp.where(jnp.full((1, CZ), x + dx, jnp.int32) == r, rows[r], 0.0)
        picked.append(v)
    row = iota((8, CZ), 0)
    stack = jnp.where(row == 0, picked[0], jnp.where(row == 1, picked[1], jnp.where(row == 2, picked[2], 0.0)))
    lane = iota((8, CZ), 1)
    out = {}
    for dy in (-1, 0, 1):
        for dz in (-1, 0, 1):
            ok = (y + dy >= 0) & (y + dy < ny) & (z + dz >= 0) & (z + dz < nz)
            target = jnp.where(ok, (y + dy) * nz + z + dz, -1)
            out[dy, dz] = jnp.sum(jnp.where(lane == target, stack, 0.0), axis=1, keepdims=True)
    return out


def groups(low, high, body, step=1):
    count = high - low
    size = max(u for u in range(1, count // 2 + 1) if count % u == 0)

    def go(i, carry):
        body([low + i * size + u for u in range(size)])
        return carry

    lax.fori_loop(0, count // size, go, 0)


def unpack(src, bx, kap, rr, ff):
    for x in range(CX):
        at = bx * CX + x
        kap[at, :, 0:CZ] = src[x]
        kap[at, :, CZ:EZ] = roll(src[2 * CX], -16 * x, 1)
        rr[at, :, 0:CZ] = src[CX + x] * ff[bx, :, 0:CZ]
        rr[at, :, CZ:EZ] = roll(src[2 * CX + 1], -16 * x, 1) * ff[bx, :, CZ:EZ]


def unpack_message(msg, flip, bx, kap, rr, ff):
    in_cond, in_rhs, z_at = x_tiles()
    for tile in range(4):
        rows = slice(8 * tile, 8 * tile + 8)
        for part, to, i in ((in_cond, kap, 0), (in_rhs, rr, 1)):
            packed = msg[z_at + 4 * i + tile]
            for x in range(CX):
                at, n = part[H - x if flip else x + 1]
                if n == 0:
                    continue
                v = msg[at + min(tile, n - 1)]
                q = roll(packed, -16 * x, 1)
                if i:
                    v = v * ff[bx, rows, 0:CZ]
                    q = q * ff[bx, rows, CZ:EZ]
                to[bx * CX + x, rows, 0:CZ] = v
                to[bx * CX + x, rows, CZ:EZ] = q


def pooled(s):
    even = iota(s.shape, 0) % 2 == 0
    s = s + jnp.where(even, roll(s, -1, 0), roll(s, 1, 0))
    even = iota(s.shape, 1) % 2 == 0
    return s + jnp.where(even, roll(s, -1, 1), roll(s, 1, 1))


def coef_x(x, kap, cx):
    cx[x] = 0.5 * (kap[x] + kap[x + 1])


def coef_yz(x, kap, cy, cz):
    k = kap[x]
    cy[x] = 0.5 * (k + roll(k, -1, 0))
    cz[x] = 0.5 * (k + roll(k, -1, 1))


def inverse_fine(x, cx, cy, cz, i0, rr, u1, ff):
    f = ff[x >> 3]
    b, c = cy[x], cz[x]
    s = cx[x] + cx[x - 1] + b + roll(b, 1, 0) + c + roll(c, 1, 1)
    v = OMEGA * f / (s + 1.0 - f)
    i0[x] = v
    u1[x] = v * rr[x]


def coarse_cond(i, kap, k1):
    k1[i] = pooled(kap[2 * i] + kap[2 * i + 1]) * 0.125


def inverse_coarse(i, k1, i1, f1):
    k = k1[i]
    f = f1[i >> 2]
    s = k1[i - 1] + k1[i + 1] + roll(k, 2, 0) + roll(k, -2, 0) + roll(k, 2, 1) + roll(k, -2, 1)
    s = 3.0 * k + 0.5 * s
    i1[i] = OMEGA * f / (4.0 * s + 1.0 - f)


ROW_PARTS = ((0, 0), (8, 0), (16, 1), (24, -1))


def coarse_kernel(
    nx, ny, nz, factor, diagonal, gathered, slab,
    inv, ff, f1, fy, kap, rr, cx, cy, cz, i0, k1, i1, u1,
):
    inverse_of(factor, diagonal, inv)
    lane8 = iota((8, CZ), 1)
    lane8f = lane8.astype(F32)
    even8f = (lane8 - lane8 % 2).astype(F32)
    valid = (lane8 < H) | (lane8 >= CZ - H)
    ext = neighbours(table(gathered, 1, nx, ny, nz), nz, ny)
    y0 = neighbours(coarse_solve(inv, table(gathered, 0, nx, ny, nz)), nz, ny)
    for bx in range(3):
        for r, dy in ROW_PARTS:
            e = {dz: jnp.broadcast_to(ext[dy, dz][bx : bx + 1], (8, CZ)) for dz in (-1, 0, 1)}
            v = {dz: jnp.broadcast_to(y0[dy, dz][bx : bx + 1], (8, CZ)) for dz in (-1, 0, 1)}
            far = jnp.where(lane8 < CZ // 2, e[1], e[-1])
            m0 = jnp.where(lane8f < e[0], 1.0, 0.0)
            m1 = jnp.where(valid & (lane8f < far), 1.0, 0.0)
            ff[bx, r : r + 8, 0:CZ] = m0
            ff[bx, r : r + 8, CZ:EZ] = m1
            f1[bx, r : r + 8, 0:CZ] = jnp.where(even8f < e[0], 1.0, 0.0)
            f1[bx, r : r + 8, CZ:EZ] = jnp.where(valid & (even8f < far), 1.0, 0.0)
            fy[bx, r : r + 8, 0:CZ] = m0 * v[0]
            fy[bx, r : r + 8, CZ:EZ] = m1 * jnp.where(lane8 < CZ // 2, v[1], v[-1])


    unpack(slab, 1, kap, rr, ff)
    for x in range(CX, 2 * CX):
        coef_yz(x, kap, cy, cz)
        if x < 2 * CX - 1:
            coef_x(x, kap, cx)
    for x in range(CX + 1, 2 * CX - 1):
        inverse_fine(x, cx, cy, cz, i0, rr, u1, ff)
    for i in range(CX // 2, CX):
        coarse_cond(i, kap, k1)
    for i in range(CX // 2 + 1, CX - 1):
        inverse_coarse(i, k1, i1, f1)


def main_kernel(
    left, right, ff, f1, fy, *refs
):
    (kap, rr, cx, cy, cz, i0, k1, i1, u1) = refs[9:18]
    (d_out, t_out, n_out, an_out, r_out, e0_out, ey_out, ez_out, ex_out, f_out, msg) = refs[18:29]
    u2, dd, tt = refs[29:]
    unpack_message(left, True, 0, kap, rr, ff)
    unpack_message(right, False, 2, kap, rr, ff)
    coef_x(2 * CX - 1, kap, cx)

    def coefs(us):
        for u in us:
            for x in (u, u + 2 * CX):
                coef_yz(x, kap, cy, cz)
            coef_x(u, kap, cx)
            coef_x(jnp.minimum(u + 2 * CX, EX - 2), kap, cx)

    groups(0, CX, coefs)

    def inverses(us):
        for u in us:
            for x in (u, u + 2 * CX - 2):
                inverse_fine(x, cx, cy, cz, i0, rr, u1, ff)

    groups(1, CX + 1, inverses)
    for i in range(CX // 2):
        for j in (i, i + CX):
            coarse_cond(j, kap, k1)
    for i in range(1, CX // 2 + 1):
        for j in (i, i + CX - 2):
            inverse_coarse(j, k1, i1, f1)

    def images(u, xs, masked=True):
        c = [u[xs[0] - 1]] + [u[x] for x in xs] + [u[xs[-1] + 1]]
        flux = [cx[x] * (c[i] - c[i + 1]) for i, x in enumerate([xs[0] - 1] + list(xs))]
        out = []
        for i, x in enumerate(xs):
            v = c[i + 1]
            gy = cy[x] * (v - roll(v, -1, 0))
            gz = cz[x] * (v - roll(v, -1, 1))
            w = (flux[i + 1] - flux[i]) + (gy - roll(gy, 1, 0)) + (gz - roll(gz, 1, 1))
            out.append(ff[x >> 3] * w if masked else w)
        return out

    def smooth(src, pair_range, out_range, put):
        def pairs(ps):
            xs = [2 * ps[0] + j for j in range(2 * len(ps))]
            im = images(u1, xs)
            for j, i in enumerate(ps):
                x, y = xs[2 * j], xs[2 * j + 1]
                s = (src[x] - im[2 * j]) + (src[y] - im[2 * j + 1])
                below = ff[x >> 3] * (i1[i] * pooled(s))
                u2[x] = u1[x] + below
                u2[y] = u1[y] + below

        groups(*pair_range, pairs)

        def last(xs):
            for x, w in zip(xs, images(u2, xs, False)):
                put(x, u2[x] + i0[x] * (src[x] - w))

        groups(*out_range, last)

    def put_d(x, v):
        dd[x] = v + fy[x >> 3]

    smooth(rr, (1, EX // 2 - 1), (3, EX - 3), put_d)

    def apply(xs):
        for x, w in zip(xs, images(dd, xs)):
            tt[x] = w
            u1[x] = i0[x] * w

    groups(4, EX - 4, apply)
    for x in range(CX):
        d_out[x] = dd[H + x, 0:CY, 0:CZ]

    def put_n(x, v):
        dd[x] = v

    zero = jnp.zeros((CY, CZ), F32)
    s_rz, s_dad = zero, zero
    for x in range(CX):
        s_rz = s_rz + rr[H + x, 0:CY, 0:CZ] * d_out[x]
        s_dad = s_dad + tt[H + x, 0:CY, 0:CZ] * d_out[x]
    smooth(tt, (3, EX // 2 - 3), (7, EX - 7), put_n)
    s_x, s_y, s_tau, s_om, s_d, s_cy, s_cz = (zero,) * 7
    f = ff[1]
    row = iota((EY, EZ), 0)
    lane = iota((EY, EZ), 1)
    mine = jnp.where((row < CY) & (lane < CZ), f, 0.0)
    own_f = f[0:CY, 0:CZ]
    row_o = iota((CY, CZ), 0)
    lane_o = iota((CY, CZ), 1)
    f_out[...] = own_f
    f_up_y = roll(f, -1, 0)
    f_up_z = roll(f, -1, 1)
    dif_y = mine - roll(mine, -1, 0)
    dif_z = mine - roll(mine, -1, 1)
    image_n = images(dd, list(range(H, H + CX)))
    for x in range(CX):
        at = H + x
        an = image_n[x][0:CY, 0:CZ]
        n = dd[at, 0:CY, 0:CZ]
        t = tt[at, 0:CY, 0:CZ]
        an_out[x] = an
        n_out[x] = n
        t_out[x] = t
        r_out[x] = rr[at, 0:CY, 0:CZ]
        b, c = cy[at], cz[at]
        gy = b * dif_y
        gz = c * dif_z
        e = ((gy - roll(gy, 1, 0)) + (gz - roll(gz, 1, 1)))[0:CY, 0:CZ]
        if x == 0:
            e = e + cx[H - 1, 0:CY, 0:CZ] * own_f
        if x == CX - 1:
            e = e + cx[at, 0:CY, 0:CZ] * own_f
        e = e * own_f
        e0_out[x] = e
        cut_y = jnp.where(
            row_o == CY - 1, (b * f_up_y)[0:CY, 0:CZ], jnp.where(row_o == 0, roll(b * f, 1, 0)[0:CY, 0:CZ], 0.0)
        ) * own_f
        cut_z = jnp.where(
            lane_o == CZ - 1, (c * f_up_z)[0:CY, 0:CZ], jnp.where(lane_o == 0, roll(c * f, 1, 1)[0:CY, 0:CZ], 0.0)
        ) * own_f
        ey_out[x] = cut_y
        ez_out[x] = cut_z
        s_x = s_x + t * n
        s_y = s_y + n * an
        s_tau = s_tau + t
        s_om = s_om + an
        s_d = s_d + e * own_f
        s_cy = s_cy + cut_y
        s_cz = s_cz + cut_z
    ex0 = cx[H - 1, 0:CY, 0:CZ] * own_f * ff[0, 0:CY, 0:CZ]
    ex1 = cx[H + CX - 1, 0:CY, 0:CZ] * own_f * ff[2, 0:CY, 0:CZ]
    ex_out[0] = ex0
    ex_out[1] = ex1
    at = iota((1, CZ), 1)
    z = lax.axis_index("gz")
    vectors = (
        s_tau, s_om, s_d, ex1,
        jnp.where(row_o == CY - 1, s_cy, 0.0), jnp.where(lane_o == CZ - 1, s_cz, 0.0),
    )
    line = jnp.zeros((1, CZ), F32)
    for i, v in enumerate(vectors):
        line = line + jnp.where(at == SLOT * i + z, total(v), 0.0)
    for i, v in enumerate((s_rz, s_dad, s_x, s_y)):
        line = line + jnp.where(at == 6 * SLOT + i, total(v), 0.0)
    msg[...] = jnp.broadcast_to(line[None], msg.shape)


def final_kernel(nx, ny, nz, gathered, inv, d_in, t_in, n_in, an_in, r_in, e0, ey, ez, ex, f_in, sol, res):
    vectors = [table(gathered, i, nx, ny, nz) for i in range(6)]
    tables = list(zip(*vectors))
    sums = jnp.sum(gathered[...], axis=0)
    at = iota((1, CZ), 1)

    def scalar(i):
        return jnp.sum(jnp.where(at == 6 * SLOT + i, sums, 0.0), axis=1, keepdims=True)

    rz, dad, xx, yy = (scalar(i) for i in range(4))
    tau = vectors[0]
    yt = coarse_solve(inv, [v * (1.0 / CELLS) for v in tau])
    add_x = jnp.zeros((1, CZ), F32)
    add_y = jnp.zeros((1, CZ), F32)
    for x in range(nx):
        y = yt[x]
        t = tables[x]
        add_x = add_x + t[0] * y
        cross = t[4] * roll(y, -nz, 1) + t[5] * roll(y, -1, 1)
        if x + 1 < nx:
            cross = cross + t[3] * yt[x + 1]
        add_y = add_y + y * (2.0 * t[1] + t[2] * y - 2.0 * cross)
    xx = xx + jnp.sum(add_x, axis=1, keepdims=True)
    yy = yy + jnp.sum(add_y, axis=1, keepdims=True)
    a0 = rz / dad
    new = a0 * a0 * xx - rz
    beta = new / rz
    zaz = dad - 2.0 * a0 * xx + a0 * a0 * yy
    a1 = new / (zaz - beta * beta * dad)
    near = neighbours(yt, nz, ny)
    shape = (CY, CZ)

    def wide(v, bx=1):
        return jnp.broadcast_to(v[bx : bx + 1], shape)

    y_own = wide(near[0, 0])
    y_y = jnp.where(iota(shape, 0) < CY // 2, wide(near[-1, 0]), wide(near[1, 0]))
    y_z = jnp.where(iota(shape, 1) < CZ // 2, wide(near[0, -1]), wide(near[0, 1]))
    f = f_in[...]
    c_d = jnp.broadcast_to(a0 + a1 * (1.0 + beta), shape)
    c_n = jnp.broadcast_to(a0 * a1, shape)
    for x in range(CX):
        n = n_in[x] + f * y_own
        an = an_in[x] + e0[x] * y_own - ey[x] * y_y - ez[x] * y_z
        if x == 0:
            an = an - ex[0] * wide(near[0, 0], 0)
        if x == CX - 1:
            an = an - ex[1] * wide(near[0, 0], 2)
        sol[x] = c_d * d_in[x] - c_n * n
        res[x] = r_in[x] - c_d * t_in[x] + c_n * an


def exchange(axis, to_low, to_high):
    size = lax.axis_size(axis)
    up = [(i, i + 1) for i in range(size - 1)]
    down = [(b, a) for a, b in up]
    return lax.ppermute(to_low, axis, down), lax.ppermute(to_high, axis, up)


def on_device(right_side, conductance, extents, coarse_factor):
    nx, ny, nz = (lax.axis_size(a) for a in ("gx", "gy", "gz"))
    sizes = (nx, ny, nz)
    any_space = pl.BlockSpec(memory_space=pl.ANY)
    msg = call(pack_kernel, [(nz, CY, CZ)], 3, name="pack", mib=PACK_MIB)(extents, right_side, conductance)[0]
    got = lax.all_to_all(msg, "gz", 0, 0, tiled=True)
    depth = 2 * CX + 2
    zh, to_low, to_high, line = call(
        rows_kernel, [(2, CY, CZ), (depth, H, CZ), (depth, H, CZ), (nx * ny, 1, CZ)], 3, name="rows"
    )(right_side, conductance, got)
    first = lax.all_to_all(line, ("gx", "gy"), 0, 0, tiled=True)
    y_high, y_low = exchange("gy", to_low, to_high)
    slab, to_low, to_high = call(
        slab_kernel, [(depth, EY, CZ)] + [(X_TILES, 8, CZ)] * 2, 6, in_specs=[VMEM] * 5 + [any_space], name="slab"
    )(right_side, conductance, zh, y_high, y_low, first)
    to_low, to_high, factor = lax.optimization_barrier((to_low, to_high, coarse_factor))
    nb = factor.shape[0] // CZ
    diagonal = call(diagonal_kernel, [(nb, CZ, CZ)], 1, name="diagonal")(factor)[0]
    x_high, x_low = exchange("gx", to_low, to_high)
    block = (CX, CY, CZ)
    wide = (EX, EY, EZ)
    half = (EX // 2, EY, EZ)
    third = (3, EY, EZ)
    arrays = [wide] * 6 + [half] * 2 + [wide]
    inv, ff, f1, fy, *fields = call(
        functools.partial(coarse_kernel, *sizes), [factor.shape] + [third] * 3 + arrays, 4, name="coarse"
    )(factor, diagonal, first, slab)
    outs = call(
        main_kernel,
        arrays + [block] * 8 + [(2, CY, CZ), (CY, CZ), (nz, 1, CZ)],
        14,
        scratch=[wide] * 3,
        aliases={5 + i: i for i in range(9)},
        name="fields",
    )(x_low, x_high, ff, f1, fy, *fields)[9:]
    part = lax.all_to_all(outs[-1], "gz", 0, 0, tiled=True)
    line = call(sum_kernel, [(nx * ny, 1, CZ)], 1, name="sum")(part)[0]
    second = lax.all_to_all(line, ("gx", "gy"), 0, 0, tiled=True)
    sol, res = call(functools.partial(final_kernel, *sizes), [block] * 2, 12, name="final")(
        second, inv, *outs[:-1]
    )
    return sol, res


def solution(mesh):
    spec = P("gx", "gy", "gz")
    return jax.shard_map(
        on_device, mesh=mesh, in_specs=(spec, spec, spec, P()), out_specs=(spec, spec), check_vma=False
    )
```

```python
import functools

import jax
import jax.numpy as jnp
from jax import lax
from jax.experimental import pallas as pl
from jax.experimental.pallas import tpu as pltpu
from jax.sharding import PartitionSpec as P

F32 = jnp.float32
PACK_MIB = 48
OMEGA = 0.8
CX, CY, CZ = 8, 16, 128
CELLS = CX * CY * CZ
H = 8
EX, EY, EZ = CX + 2 * H, CY + 2 * H, 2 * CZ
SLOT = 16
VMEM = pl.BlockSpec(memory_space=pltpu.VMEM)
SMEM = pl.BlockSpec(memory_space=pltpu.SMEM)


def call(kernel, out_shapes, n_in, scratch=(), in_specs=None, name=None, aliases=None, mib=24):
    outs = [jax.ShapeDtypeStruct(s, F32) for s in out_shapes]
    return pl.pallas_call(
        kernel,
        out_shape=outs,
        in_specs=in_specs or [VMEM] * n_in,
        out_specs=[VMEM] * len(outs),
        scratch_shapes=[pltpu.VMEM(s, F32) for s in scratch],
        input_output_aliases=aliases or {},
        compiler_params=pltpu.CompilerParams(vmem_limit_bytes=mib * 1024 * 1024),
        name=name,
    )


def roll(x, shift, axis):
    return pltpu.roll(x, shift % x.shape[axis], axis)


def iota(shape, dim):
    return lax.broadcasted_iota(jnp.int32, shape, dim)


def total(x):
    return jnp.sum(jnp.sum(x, axis=0, keepdims=True), axis=1, keepdims=True)


def pack_kernel(ext, rhs, cond, msg):
    nz = msg.shape[0]
    lane = iota((CY, CZ), 1)
    row = iota((CY, CZ), 0)
    a = jnp.zeros((CY, CZ), F32)
    b = jnp.zeros((CY, CZ), F32)
    acc = jnp.zeros((CY, CZ), F32)
    count = jnp.broadcast_to(ext[0], (CY, CZ))
    inside = lane < count
    z = lax.axis_index("gz")
    for x in range(CX):
        k = cond[x]
        r = rhs[x]
        acc = acc + jnp.where(inside, r, 0.0)
        hi = (lane >= 16 * x) & (lane < 16 * x + H)
        start = (16 * x - H) % CZ
        lo = (lane >= start) & (lane < start + H)
        a = jnp.where(hi, roll(k, 16 * x, 1), jnp.where(lo, roll(r, 16 * x - H, 1), a))
        b = jnp.where(lo, roll(k, 16 * x, 1), jnp.where(hi, roll(r, 16 * x + H, 1), b))
    info = jnp.where(row == 0, total(acc) / CELLS, count.astype(F32))
    a = jnp.where((lane == CZ - 1) & (row < 2), info, a)
    b = jnp.where((lane == 0) & (row < 2), info, b)
    for i in range(nz):
        msg[i] = b

    @pl.when(z > 0)
    def _():
        msg[z - 1] = a


def rows_kernel(rhs, cond, got, zh, to_low, to_high, line):
    nz = got.shape[0]
    z = lax.axis_index("gz")
    low_half = iota((CY, CZ), 1) % 16 < H
    up = jnp.minimum(z + 1, nz - 1)
    a = jnp.where(jnp.full((CY, CZ), z, jnp.int32) < nz - 1, got[up], 0.0)
    b = jnp.where(jnp.full((CY, CZ), z, jnp.int32) > 0, got[jnp.maximum(z - 1, 0)], 0.0)
    lane = iota((8, CZ), 1)
    info = jnp.zeros((8, CZ), F32)
    for i in range(nz):
        v = got[i, 0:8]
        info = jnp.where(lane == i, roll(v, i, 1), info)
    info = jnp.where(lane == z + 1, pltpu.roll(a[0:8], z + 2, 1), info)
    info = jnp.where(lane < nz, info, 0.0)
    line[...] = jnp.broadcast_to((info[0:1] + roll(info[1:2], SLOT, 1))[None], line.shape)
    zk = jnp.where(low_half, a, b)
    zr = jnp.where(low_half, roll(a, H, 1), roll(b, -H, 1))
    zh[0] = zk
    zh[1] = zr
    to_low[0:CX] = cond[:, 0:H, :]
    to_low[CX : 2 * CX] = rhs[:, 0:H, :]
    to_low[2 * CX] = zk[0:H]
    to_low[2 * CX + 1] = zr[0:H]
    to_high[0:CX] = cond[:, CY - H : CY, :]
    to_high[CX : 2 * CX] = rhs[:, CY - H : CY, :]
    to_high[2 * CX] = zk[CY - H : CY]
    to_high[2 * CX + 1] = zr[CY - H : CY]


def x_tiles():
    at = 0
    cond, rhs = {}, {}
    for layer in range(1, H + 1):
        for part, whole, none in ((cond, 5, 9), (rhs, 4, 8)):
            n = 4 if layer <= whole else 3 if layer < none else 0
            part[layer] = (at, n)
            at += n
    return cond, rhs, at


X_TILES = x_tiles()[2] + 8


def slab_kernel(rhs, cond, zh, from_high, from_low, after, slab, to_low, to_high):
    slab[0:CX, 0:CY] = cond[...]
    slab[CX : 2 * CX, 0:CY] = rhs[...]
    slab[2 * CX : 2 * CX + 2, 0:CY] = zh[...]
    slab[:, CY : CY + H] = from_high[...]
    slab[:, CY + H : EY] = from_low[...]
    in_cond, in_rhs, z_at = x_tiles()
    near = iota((8, CZ), 0) < 4
    for msg, flip in ((to_low, False), (to_high, True)):
        for x in range(CX):
            layer = H - x if flip else x + 1
            for part, base, src in ((in_cond, 0, cond), (in_rhs, CX, rhs)):
                at, n = part[layer]
                if n == 0:
                    continue
                msg[at] = src[x, 0:8]
                msg[at + 1] = src[x, 8:16]
                high, low = from_high[base + x], from_low[base + x]
                if n == 4:
                    msg[at + 2] = high
                    msg[at + 3] = low
                else:
                    msg[at + 2] = jnp.where(near, high, low)
        for i in range(2):
            at = z_at + 4 * i
            msg[at] = zh[i, 0:8]
            msg[at + 1] = zh[i, 8:16]
            msg[at + 2] = from_high[2 * CX + i]
            msg[at + 3] = from_low[2 * CX + i]


def sum_kernel(part, line):
    line[...] = jnp.broadcast_to(jnp.sum(part[...], axis=0, keepdims=True), line.shape)


def table(rows, i, nx, ny, nz):
    out = []
    for x in range(nx):
        v = rows[x * ny : (x + 1) * ny].reshape(ny, CZ)
        v = jnp.where(iota((ny, CZ), 1) < nz, roll(v, -SLOT * i, 1), 0.0)
        v = pltpu.roll(v, 0, 1, stride=nz, stride_axis=0)
        out.append(jnp.sum(v, axis=0, keepdims=True))
    return out


def dot(a, b):
    return jnp.dot(a, b, precision=lax.Precision.HIGHEST, preferred_element_type=F32)


def diagonal_kernel(factor, out):
    n = factor.shape[0]
    bs = CZ
    nb = n // bs
    i = iota((bs, bs), 0)
    j = iota((bs, bs), 1)
    eye = i == j
    low = [factor[b * bs : (b + 1) * bs, b * bs : (b + 1) * bs].astype(F32) for b in range(nb)]
    inv = []
    for lb in low:
        diag = jnp.where(eye, lb, 0.0)
        col = 1.0 / jnp.sum(diag, axis=1, keepdims=True)
        row = 1.0 / jnp.sum(diag, axis=0, keepdims=True)
        pair = (i // 2 == j // 2) & (i > j)
        inv.append(jnp.where(eye, col, 0.0) - jnp.where(pair, col * lb * row, 0.0))
    s = 2
    while s < bs:
        mask = (i // (2 * s) == j // (2 * s)) & (i // s > j // s)
        mid = [dot(jnp.where(mask, lb, 0.0), x) for lb, x in zip(low, inv)]
        inv = [x - dot(x, m) for x, m in zip(inv, mid)]
        s *= 2
    for b in range(nb):
        out[b] = inv[b]


def inverse_of(factor, diagonal, out):
    n = factor.shape[0]
    bs = CZ
    for b in range(n // bs):
        out[b * bs : (b + 1) * bs, b * bs : (b + 1) * bs] = diagonal[b]
    s = bs
    while s < n:
        for at in range(0, n, 2 * s):
            for lo in range(s, 2 * s, bs):
                for hi in range(lo - s + bs, s, bs):
                    out[at + lo - s : at + lo - s + bs, at + hi : at + hi + bs] = jnp.zeros((bs, bs), F32)
            if s > bs:
                for lo in range(s, 2 * s, bs):
                    for hi in range(lo + bs, 2 * s, bs):
                        out[at + lo : at + lo + bs, at + hi : at + hi + bs] = jnp.zeros((bs, bs), F32)
            mid = dot(factor[at + s : at + 2 * s, at : at + s].astype(F32), out[at : at + s, at : at + s])
            out[at + s : at + 2 * s, at : at + s] = -dot(out[at + s : at + 2 * s, at + s : at + 2 * s], mid)
        s *= 2


def coarse_solve(inv, means):
    nb = len(means)
    bs = CZ
    rows = [jnp.zeros((1, bs), F32) for _ in range(nb)]
    for a in range(nb):
        acc = inv[a * bs : (a + 1) * bs, 0:bs] * means[0]
        for c in range(1, a + 1):
            acc = acc + inv[a * bs : (a + 1) * bs, c * bs : (c + 1) * bs] * means[c]
        u = jnp.sum(acc, axis=1, keepdims=True)
        for c in range(a + 1):
            rows[c] = rows[c] + jnp.sum(inv[a * bs : (a + 1) * bs, c * bs : (c + 1) * bs] * u, axis=0, keepdims=True)
    return rows


def neighbours(rows, nz, ny):
    nx = len(rows)
    x = lax.axis_index("gx")
    y = lax.axis_index("gy")
    z = lax.axis_index("gz")
    zero = jnp.zeros((1, CZ), F32)
    picked = []
    for dx in (-1, 0, 1):
        v = zero
        for r in range(nx):
            v = v + jnp.where(jnp.full((1, CZ), x + dx, jnp.int32) == r, rows[r], 0.0)
        picked.append(v)
    row = iota((8, CZ), 0)
    stack = jnp.where(row == 0, picked[0], jnp.where(row == 1, picked[1], jnp.where(row == 2, picked[2], 0.0)))
    lane = iota((8, CZ), 1)
    out = {}
    for dy in (-1, 0, 1):
        for dz in (-1, 0, 1):
            ok = (y + dy >= 0) & (y + dy < ny) & (z + dz >= 0) & (z + dz < nz)
            target = jnp.where(ok, (y + dy) * nz + z + dz, -1)
            out[dy, dz] = jnp.sum(jnp.where(lane == target, stack, 0.0), axis=1, keepdims=True)
    return out


def groups(low, high, body, step=1):
    count = high - low
    size = max(u for u in range(1, count // 2 + 1) if count % u == 0)

    def go(i, carry):
        body([low + i * size + u for u in range(size)])
        return carry

    lax.fori_loop(0, count // size, go, 0)


def unpack(src, bx, kap, rr, ff):
    for x in range(CX):
        at = bx * CX + x
        kap[at, :, 0:CZ] = src[x]
        kap[at, :, CZ:EZ] = roll(src[2 * CX], -16 * x, 1)
        rr[at, :, 0:CZ] = src[CX + x] * ff[bx, :, 0:CZ]
        rr[at, :, CZ:EZ] = roll(src[2 * CX + 1], -16 * x, 1) * ff[bx, :, CZ:EZ]


def unpack_message(msg, flip, bx, kap, rr, ff):
    in_cond, in_rhs, z_at = x_tiles()
    for tile in range(4):
        rows = slice(8 * tile, 8 * tile + 8)
        for part, to, i in ((in_cond, kap, 0), (in_rhs, rr, 1)):
            packed = msg[z_at + 4 * i + tile]
            for x in range(CX):
                at, n = part[H - x if flip else x + 1]
                if n == 0:
                    continue
                v = msg[at + min(tile, n - 1)]
                q = roll(packed, -16 * x, 1)
                if i:
                    v = v * ff[bx, rows, 0:CZ]
                    q = q * ff[bx, rows, CZ:EZ]
                to[bx * CX + x, rows, 0:CZ] = v
                to[bx * CX + x, rows, CZ:EZ] = q


def pooled(s):
    even = iota(s.shape, 0) % 2 == 0
    s = s + jnp.where(even, roll(s, -1, 0), roll(s, 1, 0))
    even = iota(s.shape, 1) % 2 == 0
    return s + jnp.where(even, roll(s, -1, 1), roll(s, 1, 1))


def coef_x(x, kap, cx):
    cx[x] = 0.5 * (kap[x] + kap[x + 1])


def coef_yz(x, kap, cy, cz):
    k = kap[x]
    cy[x] = 0.5 * (k + roll(k, -1, 0))
    cz[x] = 0.5 * (k + roll(k, -1, 1))


def inverse_fine(x, cx, cy, cz, i0, rr, u1, ff):
    f = ff[x >> 3]
    b, c = cy[x], cz[x]
    s = cx[x] + cx[x - 1] + b + roll(b, 1, 0) + c + roll(c, 1, 1)
    v = OMEGA * f / (s + 1.0 - f)
    i0[x] = v
    u1[x] = v * rr[x]


def coarse_cond(i, kap, k1):
    k1[i] = pooled(kap[2 * i] + kap[2 * i + 1]) * 0.125


def inverse_coarse(i, k1, i1, f1):
    k = k1[i]
    f = f1[i >> 2]
    s = k1[i - 1] + k1[i + 1] + roll(k, 2, 0) + roll(k, -2, 0) + roll(k, 2, 1) + roll(k, -2, 1)
    s = 3.0 * k + 0.5 * s
    i1[i] = OMEGA * f / (4.0 * s + 1.0 - f)


ROW_PARTS = ((0, 0), (8, 0), (16, 1), (24, -1))


def coarse_kernel(
    nx, ny, nz, factor, diagonal, gathered, slab,
    inv, ff, f1, fy, ey_out, ez_out, f_out, sums, e0, kap, rr, cx, cy, cz, i0, k1, i1, u1,
):
    inverse_of(factor, diagonal, inv)
    lane8 = iota((8, CZ), 1)
    lane8f = lane8.astype(F32)
    even8f = (lane8 - lane8 % 2).astype(F32)
    valid = (lane8 < H) | (lane8 >= CZ - H)
    ext = neighbours(table(gathered, 1, nx, ny, nz), nz, ny)
    y0 = neighbours(coarse_solve(inv, table(gathered, 0, nx, ny, nz)), nz, ny)
    for bx in range(3):
        for r, dy in ROW_PARTS:
            e = {dz: jnp.broadcast_to(ext[dy, dz][bx : bx + 1], (8, CZ)) for dz in (-1, 0, 1)}
            v = {dz: jnp.broadcast_to(y0[dy, dz][bx : bx + 1], (8, CZ)) for dz in (-1, 0, 1)}
            far = jnp.where(lane8 < CZ // 2, e[1], e[-1])
            m0 = jnp.where(lane8f < e[0], 1.0, 0.0)
            m1 = jnp.where(valid & (lane8f < far), 1.0, 0.0)
            ff[bx, r : r + 8, 0:CZ] = m0
            ff[bx, r : r + 8, CZ:EZ] = m1
            f1[bx, r : r + 8, 0:CZ] = jnp.where(even8f < e[0], 1.0, 0.0)
            f1[bx, r : r + 8, CZ:EZ] = jnp.where(valid & (even8f < far), 1.0, 0.0)
            fy[bx, r : r + 8, 0:CZ] = m0 * v[0]
            fy[bx, r : r + 8, CZ:EZ] = m1 * jnp.where(lane8 < CZ // 2, v[1], v[-1])


    unpack(slab, 1, kap, rr, ff)
    for x in range(CX, 2 * CX):
        coef_yz(x, kap, cy, cz)
        if x < 2 * CX - 1:
            coef_x(x, kap, cx)
    for x in range(CX + 1, 2 * CX - 1):
        inverse_fine(x, cx, cy, cz, i0, rr, u1, ff)
    for i in range(CX // 2, CX):
        coarse_cond(i, kap, k1)
    for i in range(CX // 2 + 1, CX - 1):
        inverse_coarse(i, k1, i1, f1)
    f_y = ff[1, :, 0:CZ]
    f_z = ff[1, 0:CY]
    own_f = f_z[:, 0:CZ]
    f_out[...] = own_f
    mine_y = jnp.where(iota((EY, CZ), 0) < CY, f_y, 0.0)
    mine_z = jnp.where(iota((CY, EZ), 1) < CZ, f_z, 0.0)
    dif_y = mine_y - roll(mine_y, -1, 0)
    dif_z = mine_z - roll(mine_z, -1, 1)
    up_y = roll(f_y, -1, 0)[0:CY]
    up_z = roll(f_z, -1, 1)[:, 0:CZ]
    row_o = iota((CY, CZ), 0)
    lane_o = iota((CY, CZ), 1)
    s_d = s_y = s_z = jnp.zeros((CY, CZ), F32)
    for x in range(CX):
        b = cy[H + x, :, 0:CZ]
        c = cz[H + x, 0:CY]
        gy = b * dif_y
        gz = c * dif_z
        e = ((gy - roll(gy, 1, 0))[0:CY] + (gz - roll(gz, 1, 1))[:, 0:CZ]) * own_f
        low_y = roll(b * f_y, 1, 0)[0:CY]
        low_z = roll(c * f_z, 1, 1)[:, 0:CZ]
        cut_y = jnp.where(row_o == CY - 1, b[0:CY] * up_y, jnp.where(row_o == 0, low_y, 0.0)) * own_f
        cut_z = jnp.where(lane_o == CZ - 1, c[:, 0:CZ] * up_z, jnp.where(lane_o == 0, low_z, 0.0)) * own_f
        e0[x] = e
        ey_out[x] = cut_y
        ez_out[x] = cut_z
        s_d = s_d + e
        s_y = s_y + cut_y
        s_z = s_z + cut_z
    sums[0] = s_d
    sums[1] = jnp.where(row_o == CY - 1, s_y, 0.0)
    sums[2] = jnp.where(lane_o == CZ - 1, s_z, 0.0)


def main_kernel(
    left, right, ff, f1, fy, sums, *refs
):
    (e0, kap, rr, cx, cy, cz, i0, k1, i1, u1) = refs[10:20]
    (d_out, t_out, n_out, an_out, r_out, ex_out, msg) = refs[20:27]
    u2, dd, tt = refs[27:]
    unpack_message(left, True, 0, kap, rr, ff)
    unpack_message(right, False, 2, kap, rr, ff)
    coef_x(2 * CX - 1, kap, cx)

    def coefs(us):
        for u in us:
            for x in (u, u + 2 * CX):
                coef_yz(x, kap, cy, cz)
            coef_x(u, kap, cx)
            coef_x(jnp.minimum(u + 2 * CX, EX - 2), kap, cx)

    groups(0, CX, coefs)

    def inverses(us):
        for u in us:
            for x in (u, u + 2 * CX - 2):
                inverse_fine(x, cx, cy, cz, i0, rr, u1, ff)

    groups(1, CX + 1, inverses)
    for i in range(CX // 2):
        for j in (i, i + CX):
            coarse_cond(j, kap, k1)
    for i in range(1, CX // 2 + 1):
        for j in (i, i + CX - 2):
            inverse_coarse(j, k1, i1, f1)

    def images(u, xs, masked=True):
        c = [u[xs[0] - 1]] + [u[x] for x in xs] + [u[xs[-1] + 1]]
        flux = [cx[x] * (c[i] - c[i + 1]) for i, x in enumerate([xs[0] - 1] + list(xs))]
        out = []
        for i, x in enumerate(xs):
            v = c[i + 1]
            gy = cy[x] * (v - roll(v, -1, 0))
            gz = cz[x] * (v - roll(v, -1, 1))
            w = (flux[i + 1] - flux[i]) + (gy - roll(gy, 1, 0)) + (gz - roll(gz, 1, 1))
            out.append(ff[x >> 3] * w if masked else w)
        return out

    def smooth(src, pair_range, out_range, put):
        def pairs(ps):
            xs = [2 * ps[0] + j for j in range(2 * len(ps))]
            im = images(u1, xs)
            for j, i in enumerate(ps):
                x, y = xs[2 * j], xs[2 * j + 1]
                s = (src[x] - im[2 * j]) + (src[y] - im[2 * j + 1])
                below = ff[x >> 3] * (i1[i] * pooled(s))
                u2[x] = u1[x] + below
                u2[y] = u1[y] + below

        groups(*pair_range, pairs)

        def last(xs):
            for x, w in zip(xs, images(u2, xs, False)):
                put(x, u2[x] + i0[x] * (src[x] - w))

        groups(*out_range, last)

    def put_d(x, v):
        dd[x] = v + fy[x >> 3]

    smooth(rr, (1, EX // 2 - 1), (3, EX - 3), put_d)

    def apply(xs):
        for x, w in zip(xs, images(dd, xs)):
            tt[x] = w
            u1[x] = i0[x] * w

    groups(4, EX - 4, apply)
    for x in range(CX):
        d_out[x] = dd[H + x, 0:CY, 0:CZ]

    def put_n(x, v):
        dd[x] = v

    zero = jnp.zeros((CY, CZ), F32)
    s_rz, s_dad = zero, zero
    for x in range(CX):
        s_rz = s_rz + rr[H + x, 0:CY, 0:CZ] * d_out[x]
        s_dad = s_dad + tt[H + x, 0:CY, 0:CZ] * d_out[x]
    smooth(tt, (3, EX // 2 - 3), (7, EX - 7), put_n)
    s_x, s_y, s_tau, s_om = (zero,) * 4
    own_f = ff[1, 0:CY, 0:CZ]
    image_n = images(dd, list(range(H, H + CX)))
    for x in range(CX):
        at = H + x
        an = image_n[x][0:CY, 0:CZ]
        n = dd[at, 0:CY, 0:CZ]
        t = tt[at, 0:CY, 0:CZ]
        an_out[x] = an
        n_out[x] = n
        t_out[x] = t
        r_out[x] = rr[at, 0:CY, 0:CZ]
        s_x = s_x + t * n
        s_y = s_y + n * an
        s_tau = s_tau + t
        s_om = s_om + an
    side0 = cx[H - 1, 0:CY, 0:CZ] * own_f
    side1 = cx[H + CX - 1, 0:CY, 0:CZ] * own_f
    e0[0] = e0[0] + side0
    e0[CX - 1] = e0[CX - 1] + side1
    ex0 = side0 * ff[0, 0:CY, 0:CZ]
    ex1 = side1 * ff[2, 0:CY, 0:CZ]
    ex_out[0] = ex0
    ex_out[1] = ex1
    at = iota((1, CZ), 1)
    z = lax.axis_index("gz")
    vectors = (s_tau, s_om, sums[0] + side0 + side1, ex1, sums[1], sums[2])
    line = jnp.zeros((1, CZ), F32)
    for i, v in enumerate(vectors):
        line = line + jnp.where(at == SLOT * i + z, total(v), 0.0)
    for i, v in enumerate((s_rz, s_dad, s_x, s_y)):
        line = line + jnp.where(at == 6 * SLOT + i, total(v), 0.0)
    msg[...] = jnp.broadcast_to(line[None], msg.shape)


def final_kernel(nx, ny, nz, gathered, inv, d_in, t_in, n_in, an_in, r_in, e0, ey, ez, ex, f_in, sol, res):
    vectors = [table(gathered, i, nx, ny, nz) for i in range(6)]
    tables = list(zip(*vectors))
    sums = jnp.sum(gathered[...], axis=0)
    at = iota((1, CZ), 1)

    def scalar(i):
        return jnp.sum(jnp.where(at == 6 * SLOT + i, sums, 0.0), axis=1, keepdims=True)

    rz, dad, xx, yy = (scalar(i) for i in range(4))
    tau = vectors[0]
    yt = coarse_solve(inv, [v * (1.0 / CELLS) for v in tau])
    add_x = jnp.zeros((1, CZ), F32)
    add_y = jnp.zeros((1, CZ), F32)
    for x in range(nx):
        y = yt[x]
        t = tables[x]
        add_x = add_x + t[0] * y
        cross = t[4] * roll(y, -nz, 1) + t[5] * roll(y, -1, 1)
        if x + 1 < nx:
            cross = cross + t[3] * yt[x + 1]
        add_y = add_y + y * (2.0 * t[1] + t[2] * y - 2.0 * cross)
    xx = xx + jnp.sum(add_x, axis=1, keepdims=True)
    yy = yy + jnp.sum(add_y, axis=1, keepdims=True)
    a0 = rz / dad
    new = a0 * a0 * xx - rz
    beta = new / rz
    zaz = dad - 2.0 * a0 * xx + a0 * a0 * yy
    a1 = new / (zaz - beta * beta * dad)
    near = neighbours(yt, nz, ny)
    shape = (CY, CZ)

    def wide(v, bx=1):
        return jnp.broadcast_to(v[bx : bx + 1], shape)

    y_own = wide(near[0, 0])
    y_y = jnp.where(iota(shape, 0) < CY // 2, wide(near[-1, 0]), wide(near[1, 0]))
    y_z = jnp.where(iota(shape, 1) < CZ // 2, wide(near[0, -1]), wide(near[0, 1]))
    f = f_in[...]
    c_d = jnp.broadcast_to(a0 + a1 * (1.0 + beta), shape)
    c_n = jnp.broadcast_to(a0 * a1, shape)
    for x in range(CX):
        n = n_in[x] + f * y_own
        an = an_in[x] + e0[x] * y_own - ey[x] * y_y - ez[x] * y_z
        if x == 0:
            an = an - ex[0] * wide(near[0, 0], 0)
        if x == CX - 1:
            an = an - ex[1] * wide(near[0, 0], 2)
        sol[x] = c_d * d_in[x] - c_n * n
        res[x] = r_in[x] - c_d * t_in[x] + c_n * an


def exchange(axis, to_low, to_high):
    size = lax.axis_size(axis)
    up = [(i, i + 1) for i in range(size - 1)]
    down = [(b, a) for a, b in up]
    return lax.ppermute(to_low, axis, down), lax.ppermute(to_high, axis, up)


def on_device(right_side, conductance, extents, coarse_factor):
    nx, ny, nz = (lax.axis_size(a) for a in ("gx", "gy", "gz"))
    sizes = (nx, ny, nz)
    any_space = pl.BlockSpec(memory_space=pl.ANY)
    msg = call(pack_kernel, [(nz, CY, CZ)], 3, name="pack", mib=PACK_MIB)(extents, right_side, conductance)[0]
    got = lax.all_to_all(msg, "gz", 0, 0, tiled=True)
    depth = 2 * CX + 2
    zh, to_low, to_high, line = call(
        rows_kernel, [(2, CY, CZ), (depth, H, CZ), (depth, H, CZ), (nx * ny, 1, CZ)], 3, name="rows"
    )(right_side, conductance, got)
    first = lax.all_to_all(line, ("gx", "gy"), 0, 0, tiled=True)
    y_high, y_low = exchange("gy", to_low, to_high)
    slab, to_low, to_high = call(
        slab_kernel, [(depth, EY, CZ)] + [(X_TILES, 8, CZ)] * 2, 6, in_specs=[VMEM] * 5 + [any_space], name="slab"
    )(right_side, conductance, zh, y_high, y_low, first)
    to_low, to_high, factor = lax.optimization_barrier((to_low, to_high, coarse_factor))
    nb = factor.shape[0] // CZ
    diagonal = call(diagonal_kernel, [(nb, CZ, CZ)], 1, name="diagonal")(factor)[0]
    x_high, x_low = exchange("gx", to_low, to_high)
    block = (CX, CY, CZ)
    wide = (EX, EY, EZ)
    half = (EX // 2, EY, EZ)
    third = (3, EY, EZ)
    arrays = [block] + [wide] * 6 + [half] * 2 + [wide]
    inv, ff, f1, fy, ey, ez, fluid, sums, *fields = call(
        functools.partial(coarse_kernel, *sizes),
        [factor.shape] + [third] * 3 + [block] * 2 + [(CY, CZ), (3, CY, CZ)] + arrays, 4, name="coarse",
    )(factor, diagonal, first, slab)
    e0, *outs = call(
        main_kernel,
        arrays + [block] * 5 + [(2, CY, CZ), (nz, 1, CZ)],
        16,
        scratch=[wide] * 3,
        aliases={6 + i: i for i in range(10)},
        name="fields",
    )(x_low, x_high, ff, f1, fy, sums, *fields)
    d0, t0, n0, an0, r0, ex, msg = outs[9:]
    part = lax.all_to_all(msg, "gz", 0, 0, tiled=True)
    line = call(sum_kernel, [(nx * ny, 1, CZ)], 1, name="sum")(part)[0]
    second = lax.all_to_all(line, ("gx", "gy"), 0, 0, tiled=True)
    sol, res = call(functools.partial(final_kernel, *sizes), [block] * 2, 12, name="final")(
        second, inv, d0, t0, n0, an0, r0, e0, ey, ez, ex, fluid
    )
    return sol, res


def solution(mesh):
    spec = P("gx", "gy", "gz")
    return jax.shard_map(
        on_device, mesh=mesh, in_specs=(spec, spec, spec, P()), out_specs=(spec, spec), check_vma=False
    )
```

```python
import functools

import jax
import jax.numpy as jnp
from jax import lax
from jax.experimental import pallas as pl
from jax.experimental.pallas import tpu as pltpu
from jax.sharding import PartitionSpec as P

F32 = jnp.float32
PACK_MIB = 48
OMEGA = 0.8
CX, CY, CZ = 8, 16, 128
CELLS = CX * CY * CZ
H = 8
EX, EY, EZ = CX + 2 * H, CY + 2 * H, 2 * CZ
SLOT = 16
VMEM = pl.BlockSpec(memory_space=pltpu.VMEM)
SMEM = pl.BlockSpec(memory_space=pltpu.SMEM)


def call(kernel, out_shapes, n_in, scratch=(), in_specs=None, name=None, aliases=None, mib=24):
    outs = [jax.ShapeDtypeStruct(s, F32) for s in out_shapes]
    return pl.pallas_call(
        kernel,
        out_shape=outs,
        in_specs=in_specs or [VMEM] * n_in,
        out_specs=[VMEM] * len(outs),
        scratch_shapes=[pltpu.VMEM(s, F32) for s in scratch],
        input_output_aliases=aliases or {},
        compiler_params=pltpu.CompilerParams(vmem_limit_bytes=mib * 1024 * 1024),
        name=name,
    )


def roll(x, shift, axis):
    return pltpu.roll(x, shift % x.shape[axis], axis)


def iota(shape, dim):
    return lax.broadcasted_iota(jnp.int32, shape, dim)


def total(x):
    return jnp.sum(jnp.sum(x, axis=0, keepdims=True), axis=1, keepdims=True)


def pack_kernel(ext, rhs, cond, msg):
    nz = msg.shape[0]
    lane = iota((CY, CZ), 1)
    row = iota((CY, CZ), 0)
    a = jnp.zeros((CY, CZ), F32)
    b = jnp.zeros((CY, CZ), F32)
    acc = jnp.zeros((CY, CZ), F32)
    count = jnp.broadcast_to(ext[0], (CY, CZ))
    inside = lane < count
    z = lax.axis_index("gz")
    for x in range(CX):
        k = cond[x]
        r = rhs[x]
        acc = acc + jnp.where(inside, r, 0.0)
        hi = (lane >= 16 * x) & (lane < 16 * x + H)
        start = (16 * x - H) % CZ
        lo = (lane >= start) & (lane < start + H)
        a = jnp.where(hi, roll(k, 16 * x, 1), jnp.where(lo, roll(r, 16 * x - H, 1), a))
        b = jnp.where(lo, roll(k, 16 * x, 1), jnp.where(hi, roll(r, 16 * x + H, 1), b))
    info = jnp.where(row == 0, total(acc) / CELLS, count.astype(F32))
    a = jnp.where((lane == CZ - 1) & (row < 2), info, a)
    b = jnp.where((lane == 0) & (row < 2), info, b)
    for i in range(nz):
        msg[i] = b

    @pl.when(z > 0)
    def _():
        msg[z - 1] = a


def rows_kernel(rhs, cond, got, zh, to_low, to_high, line):
    nz = got.shape[0]
    z = lax.axis_index("gz")
    low_half = iota((CY, CZ), 1) % 16 < H
    up = jnp.minimum(z + 1, nz - 1)
    a = jnp.where(jnp.full((CY, CZ), z, jnp.int32) < nz - 1, got[up], 0.0)
    b = jnp.where(jnp.full((CY, CZ), z, jnp.int32) > 0, got[jnp.maximum(z - 1, 0)], 0.0)
    lane = iota((8, CZ), 1)
    info = jnp.zeros((8, CZ), F32)
    for i in range(nz):
        v = got[i, 0:8]
        info = jnp.where(lane == i, roll(v, i, 1), info)
    info = jnp.where(lane == z + 1, pltpu.roll(a[0:8], z + 2, 1), info)
    info = jnp.where(lane < nz, info, 0.0)
    line[...] = jnp.broadcast_to((info[0:1] + roll(info[1:2], SLOT, 1))[None], line.shape)
    zk = jnp.where(low_half, a, b)
    zr = jnp.where(low_half, roll(a, H, 1), roll(b, -H, 1))
    zh[0] = zk
    zh[1] = zr
    to_low[0:CX] = cond[:, 0:H, :]
    to_low[CX : 2 * CX] = rhs[:, 0:H, :]
    to_low[2 * CX] = zk[0:H]
    to_low[2 * CX + 1] = zr[0:H]
    to_high[0:CX] = cond[:, CY - H : CY, :]
    to_high[CX : 2 * CX] = rhs[:, CY - H : CY, :]
    to_high[2 * CX] = zk[CY - H : CY]
    to_high[2 * CX + 1] = zr[CY - H : CY]


def x_tiles():
    at = 0
    cond, rhs = {}, {}
    for layer in range(1, H + 1):
        for part, whole, none in ((cond, 5, 9), (rhs, 4, 8)):
            n = 4 if layer <= whole else 3 if layer < none else 0
            part[layer] = (at, n)
            at += n
    return cond, rhs, at


X_TILES = x_tiles()[2] + 8


def slab_kernel(rhs, cond, zh, from_high, from_low, after, slab, to_low, to_high):
    slab[0:CX, 0:CY] = cond[...]
    slab[CX : 2 * CX, 0:CY] = rhs[...]
    slab[2 * CX : 2 * CX + 2, 0:CY] = zh[...]
    slab[:, CY : CY + H] = from_high[...]
    slab[:, CY + H : EY] = from_low[...]
    in_cond, in_rhs, z_at = x_tiles()
    near = iota((8, CZ), 0) < 4
    for msg, flip in ((to_low, False), (to_high, True)):
        for x in range(CX):
            layer = H - x if flip else x + 1
            for part, base, src in ((in_cond, 0, cond), (in_rhs, CX, rhs)):
                at, n = part[layer]
                if n == 0:
                    continue
                msg[at] = src[x, 0:8]
                msg[at + 1] = src[x, 8:16]
                high, low = from_high[base + x], from_low[base + x]
                if n == 4:
                    msg[at + 2] = high
                    msg[at + 3] = low
                else:
                    msg[at + 2] = jnp.where(near, high, low)
        for i in range(2):
            at = z_at + 4 * i
            msg[at] = zh[i, 0:8]
            msg[at + 1] = zh[i, 8:16]
            msg[at + 2] = from_high[2 * CX + i]
            msg[at + 3] = from_low[2 * CX + i]


def sum_kernel(part, line):
    line[...] = jnp.broadcast_to(jnp.sum(part[...], axis=0, keepdims=True), line.shape)


def table(rows, i, nx, ny, nz):
    out = []
    for x in range(nx):
        v = rows[x * ny : (x + 1) * ny].reshape(ny, CZ)
        v = jnp.where(iota((ny, CZ), 1) < nz, roll(v, -SLOT * i, 1), 0.0)
        v = pltpu.roll(v, 0, 1, stride=nz, stride_axis=0)
        out.append(jnp.sum(v, axis=0, keepdims=True))
    return out


def dot(a, b):
    return jnp.dot(a, b, precision=lax.Precision.HIGHEST, preferred_element_type=F32)


def diagonal_kernel(factor, out):
    n = factor.shape[0]
    bs = CZ
    nb = n // bs
    i = iota((bs, bs), 0)
    j = iota((bs, bs), 1)
    eye = i == j
    low = [factor[b * bs : (b + 1) * bs, b * bs : (b + 1) * bs].astype(F32) for b in range(nb)]
    inv = []
    for lb in low:
        diag = jnp.where(eye, lb, 0.0)
        col = 1.0 / jnp.sum(diag, axis=1, keepdims=True)
        row = 1.0 / jnp.sum(diag, axis=0, keepdims=True)
        pair = (i // 2 == j // 2) & (i > j)
        inv.append(jnp.where(eye, col, 0.0) - jnp.where(pair, col * lb * row, 0.0))
    s = 2
    while s < bs:
        mask = (i // (2 * s) == j // (2 * s)) & (i // s > j // s)
        mid = [dot(jnp.where(mask, lb, 0.0), x) for lb, x in zip(low, inv)]
        inv = [x - dot(x, m) for x, m in zip(inv, mid)]
        s *= 2
    for b in range(nb):
        out[b] = inv[b]


def inverse_of(factor, diagonal, out):
    n = factor.shape[0]
    bs = CZ
    for b in range(n // bs):
        out[b * bs : (b + 1) * bs, b * bs : (b + 1) * bs] = diagonal[b]
    s = bs
    while s < n:
        for at in range(0, n, 2 * s):
            for lo in range(s, 2 * s, bs):
                for hi in range(lo - s + bs, s, bs):
                    out[at + lo - s : at + lo - s + bs, at + hi : at + hi + bs] = jnp.zeros((bs, bs), F32)
            if s > bs:
                for lo in range(s, 2 * s, bs):
                    for hi in range(lo + bs, 2 * s, bs):
                        out[at + lo : at + lo + bs, at + hi : at + hi + bs] = jnp.zeros((bs, bs), F32)
            mid = dot(factor[at + s : at + 2 * s, at : at + s].astype(F32), out[at : at + s, at : at + s])
            out[at + s : at + 2 * s, at : at + s] = -dot(out[at + s : at + 2 * s, at + s : at + 2 * s], mid)
        s *= 2


def coarse_solve(inv, means):
    nb = len(means)
    bs = CZ
    rows = [jnp.zeros((1, bs), F32) for _ in range(nb)]
    for a in range(nb):
        acc = inv[a * bs : (a + 1) * bs, 0:bs] * means[0]
        for c in range(1, a + 1):
            acc = acc + inv[a * bs : (a + 1) * bs, c * bs : (c + 1) * bs] * means[c]
        u = jnp.sum(acc, axis=1, keepdims=True)
        for c in range(a + 1):
            rows[c] = rows[c] + jnp.sum(inv[a * bs : (a + 1) * bs, c * bs : (c + 1) * bs] * u, axis=0, keepdims=True)
    return rows


def neighbours(rows, nz, ny):
    nx = len(rows)
    x = lax.axis_index("gx")
    y = lax.axis_index("gy")
    z = lax.axis_index("gz")
    zero = jnp.zeros((1, CZ), F32)
    picked = []
    for dx in (-1, 0, 1):
        v = zero
        for r in range(nx):
            v = v + jnp.where(jnp.full((1, CZ), x + dx, jnp.int32) == r, rows[r], 0.0)
        picked.append(v)
    row = iota((8, CZ), 0)
    stack = jnp.where(row == 0, picked[0], jnp.where(row == 1, picked[1], jnp.where(row == 2, picked[2], 0.0)))
    lane = iota((8, CZ), 1)
    out = {}
    for dy in (-1, 0, 1):
        for dz in (-1, 0, 1):
            ok = (y + dy >= 0) & (y + dy < ny) & (z + dz >= 0) & (z + dz < nz)
            target = jnp.where(ok, (y + dy) * nz + z + dz, -1)
            out[dy, dz] = jnp.sum(jnp.where(lane == target, stack, 0.0), axis=1, keepdims=True)
    return out


def groups(low, high, body, step=1):
    count = high - low
    size = max(u for u in range(1, count // 2 + 1) if count % u == 0)

    def go(i, carry):
        body([low + i * size + u for u in range(size)])
        return carry

    lax.fori_loop(0, count // size, go, 0)


def unpack(src, bx, kap, rr, ff):
    for x in range(CX):
        at = bx * CX + x
        kap[at, :, 0:CZ] = src[x]
        kap[at, :, CZ:EZ] = roll(src[2 * CX], -16 * x, 1)
        rr[at, :, 0:CZ] = src[CX + x] * ff[bx, :, 0:CZ]
        rr[at, :, CZ:EZ] = roll(src[2 * CX + 1], -16 * x, 1) * ff[bx, :, CZ:EZ]


def unpack_message(msg, flip, bx, kap, rr, ff):
    in_cond, in_rhs, z_at = x_tiles()
    for tile in range(4):
        rows = slice(8 * tile, 8 * tile + 8)
        for part, to, i in ((in_cond, kap, 0), (in_rhs, rr, 1)):
            packed = msg[z_at + 4 * i + tile]
            for x in range(CX):
                at, n = part[H - x if flip else x + 1]
                if n == 0:
                    continue
                v = msg[at + min(tile, n - 1)]
                q = roll(packed, -16 * x, 1)
                if i:
                    v = v * ff[bx, rows, 0:CZ]
                    q = q * ff[bx, rows, CZ:EZ]
                to[bx * CX + x, rows, 0:CZ] = v
                to[bx * CX + x, rows, CZ:EZ] = q


def pooled(s):
    even = iota(s.shape, 0) % 2 == 0
    s = s + jnp.where(even, roll(s, -1, 0), roll(s, 1, 0))
    even = iota(s.shape, 1) % 2 == 0
    return s + jnp.where(even, roll(s, -1, 1), roll(s, 1, 1))


def coef_x(x, kap, cx):
    cx[x] = 0.5 * (kap[x] + kap[x + 1])


def coef_yz(x, kap, cy, cz):
    k = kap[x]
    cy[x] = 0.5 * (k + roll(k, -1, 0))
    cz[x] = 0.5 * (k + roll(k, -1, 1))


def inverse_fine(x, cx, cy, cz, i0, rr, u1, ff):
    f = ff[x >> 3]
    b, c = cy[x], cz[x]
    s = cx[x] + cx[x - 1] + b + roll(b, 1, 0) + c + roll(c, 1, 1)
    v = OMEGA * f / (s + 1.0 - f)
    i0[x] = v
    u1[x] = v * rr[x]


def coarse_cond(i, kap, k1):
    k1[i] = pooled(kap[2 * i] + kap[2 * i + 1]) * 0.125


def inverse_coarse(i, k1, i1, f1):
    k = k1[i]
    f = f1[i >> 2]
    s = k1[i - 1] + k1[i + 1] + roll(k, 2, 0) + roll(k, -2, 0) + roll(k, 2, 1) + roll(k, -2, 1)
    s = 3.0 * k + 0.5 * s
    i1[i] = OMEGA * f / (4.0 * s + 1.0 - f)


ROW_PARTS = ((0, 0), (8, 0), (16, 1), (24, -1))


def coarse_kernel(
    nx, ny, nz, factor, diagonal, gathered, slab,
    inv, ff, f1, fy, ey_out, ez_out, f_out, sums, e0, kap, rr, cx, cy, cz, i0, k1, i1, u1,
):
    inverse_of(factor, diagonal, inv)
    lane8 = iota((8, CZ), 1)
    lane8f = lane8.astype(F32)
    even8f = (lane8 - lane8 % 2).astype(F32)
    valid = (lane8 < H) | (lane8 >= CZ - H)
    ext = neighbours(table(gathered, 1, nx, ny, nz), nz, ny)
    y0 = neighbours(coarse_solve(inv, table(gathered, 0, nx, ny, nz)), nz, ny)
    for bx in range(3):
        for r, dy in ROW_PARTS:
            e = {dz: jnp.broadcast_to(ext[dy, dz][bx : bx + 1], (8, CZ)) for dz in (-1, 0, 1)}
            v = {dz: jnp.broadcast_to(y0[dy, dz][bx : bx + 1], (8, CZ)) for dz in (-1, 0, 1)}
            far = jnp.where(lane8 < CZ // 2, e[1], e[-1])
            m0 = jnp.where(lane8f < e[0], 1.0, 0.0)
            m1 = jnp.where(valid & (lane8f < far), 1.0, 0.0)
            ff[bx, r : r + 8, 0:CZ] = m0
            ff[bx, r : r + 8, CZ:EZ] = m1
            f1[bx, r : r + 8, 0:CZ] = jnp.where(even8f < e[0], 1.0, 0.0)
            f1[bx, r : r + 8, CZ:EZ] = jnp.where(valid & (even8f < far), 1.0, 0.0)
            fy[bx, r : r + 8, 0:CZ] = m0 * v[0]
            fy[bx, r : r + 8, CZ:EZ] = m1 * jnp.where(lane8 < CZ // 2, v[1], v[-1])


    unpack(slab, 1, kap, rr, ff)
    for x in range(CX, 2 * CX):
        coef_yz(x, kap, cy, cz)
        if x < 2 * CX - 1:
            coef_x(x, kap, cx)
    for x in range(CX + 1, 2 * CX - 1):
        inverse_fine(x, cx, cy, cz, i0, rr, u1, ff)
    for i in range(CX // 2, CX):
        coarse_cond(i, kap, k1)
    for i in range(CX // 2 + 1, CX - 1):
        inverse_coarse(i, k1, i1, f1)
    f_y = ff[1, :, 0:CZ]
    f_z = ff[1, 0:CY]
    own_f = f_z[:, 0:CZ]
    f_out[...] = own_f
    mine_y = jnp.where(iota((EY, CZ), 0) < CY, f_y, 0.0)
    mine_z = jnp.where(iota((CY, EZ), 1) < CZ, f_z, 0.0)
    dif_y = mine_y - roll(mine_y, -1, 0)
    dif_z = mine_z - roll(mine_z, -1, 1)
    up_y = roll(f_y, -1, 0)[0:CY]
    up_z = roll(f_z, -1, 1)[:, 0:CZ]
    row_o = iota((CY, CZ), 0)
    lane_o = iota((CY, CZ), 1)
    s_d = s_y = s_z = jnp.zeros((CY, CZ), F32)
    for x in range(CX):
        b = cy[H + x, :, 0:CZ]
        c = cz[H + x, 0:CY]
        gy = b * dif_y
        gz = c * dif_z
        e = ((gy - roll(gy, 1, 0))[0:CY] + (gz - roll(gz, 1, 1))[:, 0:CZ]) * own_f
        low_y = roll(b * f_y, 1, 0)[0:CY]
        low_z = roll(c * f_z, 1, 1)[:, 0:CZ]
        cut_y = jnp.where(row_o == CY - 1, b[0:CY] * up_y, jnp.where(row_o == 0, low_y, 0.0)) * own_f
        cut_z = jnp.where(lane_o == CZ - 1, c[:, 0:CZ] * up_z, jnp.where(lane_o == 0, low_z, 0.0)) * own_f
        e0[x] = e
        ey_out[x] = cut_y
        ez_out[x] = cut_z
        s_d = s_d + e
        s_y = s_y + cut_y
        s_z = s_z + cut_z
    sums[0] = s_d
    sums[1] = jnp.where(row_o == CY - 1, s_y, 0.0)
    sums[2] = jnp.where(lane_o == CZ - 1, s_z, 0.0)


def main_kernel(
    left, right, ff, f1, fy, sums, *refs
):
    (e0, kap, rr, cx, cy, cz, i0, k1, i1, u1) = refs[10:20]
    (d_out, t_out, n_out, an_out, r_out, ex_out, msg) = refs[20:27]
    u2, dd, tt = refs[27:]
    unpack_message(left, True, 0, kap, rr, ff)
    unpack_message(right, False, 2, kap, rr, ff)
    coef_x(2 * CX - 1, kap, cx)

    def coefs(us):
        for u in us:
            for x in (u, u + 2 * CX):
                coef_yz(x, kap, cy, cz)
            coef_x(u, kap, cx)
            coef_x(jnp.minimum(u + 2 * CX, EX - 2), kap, cx)

    groups(0, CX, coefs)

    def inverses(us):
        for u in us:
            for x in (u, u + 2 * CX - 2):
                inverse_fine(x, cx, cy, cz, i0, rr, u1, ff)

    groups(1, CX + 1, inverses)
    for i in range(CX // 2):
        for j in (i, i + CX):
            coarse_cond(j, kap, k1)
    for i in range(1, CX // 2 + 1):
        for j in (i, i + CX - 2):
            inverse_coarse(j, k1, i1, f1)

    def images(u, xs, masked=True):
        c = [u[xs[0] - 1]] + [u[x] for x in xs] + [u[xs[-1] + 1]]
        flux = [cx[x] * (c[i] - c[i + 1]) for i, x in enumerate([xs[0] - 1] + list(xs))]
        out = []
        for i, x in enumerate(xs):
            v = c[i + 1]
            gy = cy[x] * (v - roll(v, -1, 0))
            gz = cz[x] * (v - roll(v, -1, 1))
            w = (flux[i + 1] - flux[i]) + (gy - roll(gy, 1, 0)) + (gz - roll(gz, 1, 1))
            out.append(ff[x >> 3] * w if masked else w)
        return out

    def smooth(src, pair_range, out_range, put):
        def pairs(ps):
            faces = [2 * i - 1 for i in ps] + [2 * ps[-1] + 1]
            flux = [cx[x] * (u1[x] - u1[x + 1]) for x in faces]
            for j, i in enumerate(ps):
                x, y = 2 * i, 2 * i + 1
                v, w = u1[x], u1[y]
                gy = cy[x] * (v - roll(v, -1, 0)) + cy[y] * (w - roll(w, -1, 0))
                gz = cz[x] * (v - roll(v, -1, 1)) + cz[y] * (w - roll(w, -1, 1))
                both = (flux[j + 1] - flux[j]) + (gy - roll(gy, 1, 0)) + (gz - roll(gz, 1, 1))
                s = (src[x] + src[y]) - ff[x >> 3] * both
                below = ff[x >> 3] * (i1[i] * pooled(s))
                u2[x] = u1[x] + below
                u2[y] = u1[y] + below

        groups(*pair_range, pairs)

        def last(xs):
            for x, w in zip(xs, images(u2, xs, False)):
                put(x, u2[x] + i0[x] * (src[x] - w))

        groups(*out_range, last)

    def put_d(x, v):
        dd[x] = v + fy[x >> 3]

    smooth(rr, (1, EX // 2 - 1), (3, EX - 3), put_d)

    def apply(xs):
        for x, w in zip(xs, images(dd, xs)):
            tt[x] = w
            u1[x] = i0[x] * w

    groups(4, EX - 4, apply)
    for x in range(CX):
        d_out[x] = dd[H + x, 0:CY, 0:CZ]

    def put_n(x, v):
        dd[x] = v

    zero = jnp.zeros((CY, CZ), F32)
    s_rz, s_dad = zero, zero
    for x in range(CX):
        s_rz = s_rz + rr[H + x, 0:CY, 0:CZ] * d_out[x]
        s_dad = s_dad + tt[H + x, 0:CY, 0:CZ] * d_out[x]
    smooth(tt, (3, EX // 2 - 3), (7, EX - 7), put_n)
    s_x, s_y, s_tau, s_om = (zero,) * 4
    own_f = ff[1, 0:CY, 0:CZ]
    image_n = images(dd, list(range(H, H + CX)))
    for x in range(CX):
        at = H + x
        an = image_n[x][0:CY, 0:CZ]
        n = dd[at, 0:CY, 0:CZ]
        t = tt[at, 0:CY, 0:CZ]
        an_out[x] = an
        n_out[x] = n
        t_out[x] = t
        r_out[x] = rr[at, 0:CY, 0:CZ]
        s_x = s_x + t * n
        s_y = s_y + n * an
        s_tau = s_tau + t
        s_om = s_om + an
    side0 = cx[H - 1, 0:CY, 0:CZ] * own_f
    side1 = cx[H + CX - 1, 0:CY, 0:CZ] * own_f
    e0[0] = e0[0] + side0
    e0[CX - 1] = e0[CX - 1] + side1
    ex0 = side0 * ff[0, 0:CY, 0:CZ]
    ex1 = side1 * ff[2, 0:CY, 0:CZ]
    ex_out[0] = ex0
    ex_out[1] = ex1
    at = iota((1, CZ), 1)
    z = lax.axis_index("gz")
    vectors = (s_tau, s_om, sums[0] + side0 + side1, ex1, sums[1], sums[2])
    line = jnp.zeros((1, CZ), F32)
    for i, v in enumerate(vectors):
        line = line + jnp.where(at == SLOT * i + z, total(v), 0.0)
    for i, v in enumerate((s_rz, s_dad, s_x, s_y)):
        line = line + jnp.where(at == 6 * SLOT + i, total(v), 0.0)
    msg[...] = jnp.broadcast_to(line[None], msg.shape)


def final_kernel(nx, ny, nz, gathered, inv, d_in, t_in, n_in, an_in, r_in, e0, ey, ez, ex, f_in, sol, res):
    vectors = [table(gathered, i, nx, ny, nz) for i in range(6)]
    tables = list(zip(*vectors))
    sums = jnp.sum(gathered[...], axis=0)
    at = iota((1, CZ), 1)

    def scalar(i):
        return jnp.sum(jnp.where(at == 6 * SLOT + i, sums, 0.0), axis=1, keepdims=True)

    rz, dad, xx, yy = (scalar(i) for i in range(4))
    tau = vectors[0]
    yt = coarse_solve(inv, [v * (1.0 / CELLS) for v in tau])
    add_x = jnp.zeros((1, CZ), F32)
    add_y = jnp.zeros((1, CZ), F32)
    for x in range(nx):
        y = yt[x]
        t = tables[x]
        add_x = add_x + t[0] * y
        cross = t[4] * roll(y, -nz, 1) + t[5] * roll(y, -1, 1)
        if x + 1 < nx:
            cross = cross + t[3] * yt[x + 1]
        add_y = add_y + y * (2.0 * t[1] + t[2] * y - 2.0 * cross)
    xx = xx + jnp.sum(add_x, axis=1, keepdims=True)
    yy = yy + jnp.sum(add_y, axis=1, keepdims=True)
    a0 = rz / dad
    new = a0 * a0 * xx - rz
    beta = new / rz
    zaz = dad - 2.0 * a0 * xx + a0 * a0 * yy
    a1 = new / (zaz - beta * beta * dad)
    near = neighbours(yt, nz, ny)
    shape = (CY, CZ)

    def wide(v, bx=1):
        return jnp.broadcast_to(v[bx : bx + 1], shape)

    y_own = wide(near[0, 0])
    y_y = jnp.where(iota(shape, 0) < CY // 2, wide(near[-1, 0]), wide(near[1, 0]))
    y_z = jnp.where(iota(shape, 1) < CZ // 2, wide(near[0, -1]), wide(near[0, 1]))
    f = f_in[...]
    c_d = jnp.broadcast_to(a0 + a1 * (1.0 + beta), shape)
    c_n = jnp.broadcast_to(a0 * a1, shape)
    for x in range(CX):
        n = n_in[x] + f * y_own
        an = an_in[x] + e0[x] * y_own - ey[x] * y_y - ez[x] * y_z
        if x == 0:
            an = an - ex[0] * wide(near[0, 0], 0)
        if x == CX - 1:
            an = an - ex[1] * wide(near[0, 0], 2)
        sol[x] = c_d * d_in[x] - c_n * n
        res[x] = r_in[x] - c_d * t_in[x] + c_n * an


def exchange(axis, to_low, to_high):
    size = lax.axis_size(axis)
    up = [(i, i + 1) for i in range(size - 1)]
    down = [(b, a) for a, b in up]
    return lax.ppermute(to_low, axis, down), lax.ppermute(to_high, axis, up)


def on_device(right_side, conductance, extents, coarse_factor):
    nx, ny, nz = (lax.axis_size(a) for a in ("gx", "gy", "gz"))
    sizes = (nx, ny, nz)
    any_space = pl.BlockSpec(memory_space=pl.ANY)
    msg = call(pack_kernel, [(nz, CY, CZ)], 3, name="pack", mib=PACK_MIB)(extents, right_side, conductance)[0]
    got = lax.all_to_all(msg, "gz", 0, 0, tiled=True)
    depth = 2 * CX + 2
    zh, to_low, to_high, line = call(
        rows_kernel, [(2, CY, CZ), (depth, H, CZ), (depth, H, CZ), (nx * ny, 1, CZ)], 3, name="rows"
    )(right_side, conductance, got)
    first = lax.all_to_all(line, ("gx", "gy"), 0, 0, tiled=True)
    y_high, y_low = exchange("gy", to_low, to_high)
    slab, to_low, to_high = call(
        slab_kernel, [(depth, EY, CZ)] + [(X_TILES, 8, CZ)] * 2, 6, in_specs=[VMEM] * 5 + [any_space], name="slab"
    )(right_side, conductance, zh, y_high, y_low, first)
    to_low, to_high, factor = lax.optimization_barrier((to_low, to_high, coarse_factor))
    nb = factor.shape[0] // CZ
    diagonal = call(diagonal_kernel, [(nb, CZ, CZ)], 1, name="diagonal")(factor)[0]
    x_high, x_low = exchange("gx", to_low, to_high)
    block = (CX, CY, CZ)
    wide = (EX, EY, EZ)
    half = (EX // 2, EY, EZ)
    third = (3, EY, EZ)
    arrays = [block] + [wide] * 6 + [half] * 2 + [wide]
    inv, ff, f1, fy, ey, ez, fluid, sums, *fields = call(
        functools.partial(coarse_kernel, *sizes),
        [factor.shape] + [third] * 3 + [block] * 2 + [(CY, CZ), (3, CY, CZ)] + arrays, 4, name="coarse",
    )(factor, diagonal, first, slab)
    e0, *outs = call(
        main_kernel,
        arrays + [block] * 5 + [(2, CY, CZ), (nz, 1, CZ)],
        16,
        scratch=[wide] * 3,
        aliases={6 + i: i for i in range(10)},
        name="fields",
    )(x_low, x_high, ff, f1, fy, sums, *fields)
    d0, t0, n0, an0, r0, ex, msg = outs[9:]
    part = lax.all_to_all(msg, "gz", 0, 0, tiled=True)
    line = call(sum_kernel, [(nx * ny, 1, CZ)], 1, name="sum")(part)[0]
    second = lax.all_to_all(line, ("gx", "gy"), 0, 0, tiled=True)
    sol, res = call(functools.partial(final_kernel, *sizes), [block] * 2, 12, name="final")(
        second, inv, d0, t0, n0, an0, r0, e0, ey, ez, ex, fluid
    )
    return sol, res


def solution(mesh):
    spec = P("gx", "gy", "gz")
    return jax.shard_map(
        on_device, mesh=mesh, in_specs=(spec, spec, spec, P()), out_specs=(spec, spec), check_vma=False
    )
```

```python
import functools

import jax
import jax.numpy as jnp
from jax import lax
from jax.experimental import pallas as pl
from jax.experimental.pallas import tpu as pltpu
from jax.sharding import PartitionSpec as P

F32 = jnp.float32
PACK_MIB = 48
OMEGA = 0.8
CX, CY, CZ = 8, 16, 128
CELLS = CX * CY * CZ
H = 8
EX, EY, EZ = CX + 2 * H, CY + 2 * H, 2 * CZ
SLOT = 16
VMEM = pl.BlockSpec(memory_space=pltpu.VMEM)
SMEM = pl.BlockSpec(memory_space=pltpu.SMEM)


def call(kernel, out_shapes, n_in, scratch=(), in_specs=None, name=None, aliases=None, mib=24):
    outs = [jax.ShapeDtypeStruct(s, F32) for s in out_shapes]
    return pl.pallas_call(
        kernel,
        out_shape=outs,
        in_specs=in_specs or [VMEM] * n_in,
        out_specs=[VMEM] * len(outs),
        scratch_shapes=[pltpu.VMEM(s, F32) for s in scratch],
        input_output_aliases=aliases or {},
        compiler_params=pltpu.CompilerParams(vmem_limit_bytes=mib * 1024 * 1024),
        name=name,
    )


def roll(x, shift, axis):
    return pltpu.roll(x, shift % x.shape[axis], axis)


def iota(shape, dim):
    return lax.broadcasted_iota(jnp.int32, shape, dim)


def total(x):
    return jnp.sum(jnp.sum(x, axis=0, keepdims=True), axis=1, keepdims=True)


def pack_kernel(ext, rhs, cond, msg):
    nz = msg.shape[0]
    lane = iota((CY, CZ), 1)
    row = iota((CY, CZ), 0)
    a = jnp.zeros((CY, CZ), F32)
    b = jnp.zeros((CY, CZ), F32)
    acc = jnp.zeros((CY, CZ), F32)
    count = jnp.broadcast_to(ext[0], (CY, CZ))
    inside = lane < count
    z = lax.axis_index("gz")
    for x in range(CX):
        k = cond[x]
        r = rhs[x]
        acc = acc + jnp.where(inside, r, 0.0)
        hi = (lane >= 16 * x) & (lane < 16 * x + H)
        start = (16 * x - H) % CZ
        lo = (lane >= start) & (lane < start + H)
        a = jnp.where(hi, roll(k, 16 * x, 1), jnp.where(lo, roll(r, 16 * x - H, 1), a))
        b = jnp.where(lo, roll(k, 16 * x, 1), jnp.where(hi, roll(r, 16 * x + H, 1), b))
    info = jnp.where(row == 0, total(acc) / CELLS, count.astype(F32))
    a = jnp.where((lane == CZ - 1) & (row < 2), info, a)
    b = jnp.where((lane == 0) & (row < 2), info, b)
    for i in range(nz):
        msg[i] = b

    @pl.when(z > 0)
    def _():
        msg[z - 1] = a


def rows_kernel(rhs, cond, got, zh, to_low, to_high, line):
    nz = got.shape[0]
    z = lax.axis_index("gz")
    low_half = iota((CY, CZ), 1) % 16 < H
    up = jnp.minimum(z + 1, nz - 1)
    a = jnp.where(jnp.full((CY, CZ), z, jnp.int32) < nz - 1, got[up], 0.0)
    b = jnp.where(jnp.full((CY, CZ), z, jnp.int32) > 0, got[jnp.maximum(z - 1, 0)], 0.0)
    lane = iota((8, CZ), 1)
    info = jnp.zeros((8, CZ), F32)
    for i in range(nz):
        v = got[i, 0:8]
        info = jnp.where(lane == i, roll(v, i, 1), info)
    info = jnp.where(lane == z + 1, pltpu.roll(a[0:8], z + 2, 1), info)
    info = jnp.where(lane < nz, info, 0.0)
    line[...] = jnp.broadcast_to((info[0:1] + roll(info[1:2], SLOT, 1))[None], line.shape)
    zk = jnp.where(low_half, a, b)
    zr = jnp.where(low_half, roll(a, H, 1), roll(b, -H, 1))
    zh[0] = zk
    zh[1] = zr
    to_low[0:CX] = cond[:, 0:H, :]
    to_low[CX : 2 * CX] = rhs[:, 0:H, :]
    to_low[2 * CX] = zk[0:H]
    to_low[2 * CX + 1] = zr[0:H]
    to_high[0:CX] = cond[:, CY - H : CY, :]
    to_high[CX : 2 * CX] = rhs[:, CY - H : CY, :]
    to_high[2 * CX] = zk[CY - H : CY]
    to_high[2 * CX + 1] = zr[CY - H : CY]


def x_tiles():
    at = 0
    cond, rhs = {}, {}
    for layer in range(1, H + 1):
        for part, whole, none in ((cond, 5, 9), (rhs, 4, 8)):
            n = 4 if layer <= whole else 3 if layer < none else 0
            part[layer] = (at, n)
            at += n
    return cond, rhs, at


X_TILES = x_tiles()[2] + 8


def slab_kernel(rhs, cond, zh, from_high, from_low, after, slab, to_low, to_high):
    slab[0:CX, 0:CY] = cond[...]
    slab[CX : 2 * CX, 0:CY] = rhs[...]
    slab[2 * CX : 2 * CX + 2, 0:CY] = zh[...]
    slab[:, CY : CY + H] = from_high[...]
    slab[:, CY + H : EY] = from_low[...]
    in_cond, in_rhs, z_at = x_tiles()
    near = iota((8, CZ), 0) < 4
    for msg, flip in ((to_low, False), (to_high, True)):
        for x in range(CX):
            layer = H - x if flip else x + 1
            for part, base, src in ((in_cond, 0, cond), (in_rhs, CX, rhs)):
                at, n = part[layer]
                if n == 0:
                    continue
                msg[at] = src[x, 0:8]
                msg[at + 1] = src[x, 8:16]
                high, low = from_high[base + x], from_low[base + x]
                if n == 4:
                    msg[at + 2] = high
                    msg[at + 3] = low
                else:
                    msg[at + 2] = jnp.where(near, high, low)
        for i in range(2):
            at = z_at + 4 * i
            msg[at] = zh[i, 0:8]
            msg[at + 1] = zh[i, 8:16]
            msg[at + 2] = from_high[2 * CX + i]
            msg[at + 3] = from_low[2 * CX + i]


def sum_kernel(part, line):
    line[...] = jnp.broadcast_to(jnp.sum(part[...], axis=0, keepdims=True), line.shape)


def table(rows, i, nx, ny, nz):
    out = []
    for x in range(nx):
        v = rows[x * ny : (x + 1) * ny].reshape(ny, CZ)
        v = jnp.where(iota((ny, CZ), 1) < nz, roll(v, -SLOT * i, 1), 0.0)
        v = pltpu.roll(v, 0, 1, stride=nz, stride_axis=0)
        out.append(jnp.sum(v, axis=0, keepdims=True))
    return out


def dot(a, b):
    return jnp.dot(a, b, precision=lax.Precision.HIGHEST, preferred_element_type=F32)


def diagonal_kernel(factor, out):
    n = factor.shape[0]
    bs = CZ
    nb = n // bs
    i = iota((bs, bs), 0)
    j = iota((bs, bs), 1)
    eye = i == j
    low = [factor[b * bs : (b + 1) * bs, b * bs : (b + 1) * bs].astype(F32) for b in range(nb)]
    inv = []
    for lb in low:
        diag = jnp.where(eye, lb, 0.0)
        col = 1.0 / jnp.sum(diag, axis=1, keepdims=True)
        row = 1.0 / jnp.sum(diag, axis=0, keepdims=True)
        pair = (i // 2 == j // 2) & (i > j)
        inv.append(jnp.where(eye, col, 0.0) - jnp.where(pair, col * lb * row, 0.0))
    s = 2
    while s < bs:
        mask = (i // (2 * s) == j // (2 * s)) & (i // s > j // s)
        mid = [dot(jnp.where(mask, lb, 0.0), x) for lb, x in zip(low, inv)]
        inv = [x - dot(x, m) for x, m in zip(inv, mid)]
        s *= 2
    for b in range(nb):
        out[b] = inv[b]


def inverse_of(factor, diagonal, out):
    n = factor.shape[0]
    bs = CZ
    for b in range(n // bs):
        out[b * bs : (b + 1) * bs, b * bs : (b + 1) * bs] = diagonal[b]
    s = bs
    while s < n:
        for at in range(0, n, 2 * s):
            for lo in range(s, 2 * s, bs):
                for hi in range(lo - s + bs, s, bs):
                    out[at + lo - s : at + lo - s + bs, at + hi : at + hi + bs] = jnp.zeros((bs, bs), F32)
            if s > bs:
                for lo in range(s, 2 * s, bs):
                    for hi in range(lo + bs, 2 * s, bs):
                        out[at + lo : at + lo + bs, at + hi : at + hi + bs] = jnp.zeros((bs, bs), F32)
            mid = dot(factor[at + s : at + 2 * s, at : at + s].astype(F32), out[at : at + s, at : at + s])
            out[at + s : at + 2 * s, at : at + s] = -dot(out[at + s : at + 2 * s, at + s : at + 2 * s], mid)
        s *= 2


def coarse_solve(inv, means):
    nb = len(means)
    bs = CZ
    rows = [jnp.zeros((1, bs), F32) for _ in range(nb)]
    for a in range(nb):
        acc = inv[a * bs : (a + 1) * bs, 0:bs] * means[0]
        for c in range(1, a + 1):
            acc = acc + inv[a * bs : (a + 1) * bs, c * bs : (c + 1) * bs] * means[c]
        u = jnp.sum(acc, axis=1, keepdims=True)
        for c in range(a + 1):
            rows[c] = rows[c] + jnp.sum(inv[a * bs : (a + 1) * bs, c * bs : (c + 1) * bs] * u, axis=0, keepdims=True)
    return rows


def neighbours(rows, nz, ny):
    nx = len(rows)
    x = lax.axis_index("gx")
    y = lax.axis_index("gy")
    z = lax.axis_index("gz")
    zero = jnp.zeros((1, CZ), F32)
    picked = []
    for dx in (-1, 0, 1):
        v = zero
        for r in range(nx):
            v = v + jnp.where(jnp.full((1, CZ), x + dx, jnp.int32) == r, rows[r], 0.0)
        picked.append(v)
    row = iota((8, CZ), 0)
    stack = jnp.where(row == 0, picked[0], jnp.where(row == 1, picked[1], jnp.where(row == 2, picked[2], 0.0)))
    lane = iota((8, CZ), 1)
    out = {}
    for dy in (-1, 0, 1):
        for dz in (-1, 0, 1):
            ok = (y + dy >= 0) & (y + dy < ny) & (z + dz >= 0) & (z + dz < nz)
            target = jnp.where(ok, (y + dy) * nz + z + dz, -1)
            out[dy, dz] = jnp.sum(jnp.where(lane == target, stack, 0.0), axis=1, keepdims=True)
    return out


def groups(low, high, body, step=1):
    count = high - low
    size = max(u for u in range(1, count // 2 + 1) if count % u == 0)

    def go(i, carry):
        body([low + i * size + u for u in range(size)])
        return carry

    lax.fori_loop(0, count // size, go, 0)


def unpack(src, bx, kap, rr, ff):
    for x in range(CX):
        at = bx * CX + x
        kap[at, :, 0:CZ] = src[x]
        kap[at, :, CZ:EZ] = roll(src[2 * CX], -16 * x, 1)
        rr[at, :, 0:CZ] = src[CX + x] * ff[bx, :, 0:CZ]
        rr[at, :, CZ:EZ] = roll(src[2 * CX + 1], -16 * x, 1) * ff[bx, :, CZ:EZ]


def unpack_message(msg, flip, bx, kap, rr, ff):
    in_cond, in_rhs, z_at = x_tiles()
    for tile in range(4):
        rows = slice(8 * tile, 8 * tile + 8)
        for part, to, i in ((in_cond, kap, 0), (in_rhs, rr, 1)):
            packed = msg[z_at + 4 * i + tile]
            for x in range(CX):
                at, n = part[H - x if flip else x + 1]
                if n == 0:
                    continue
                v = msg[at + min(tile, n - 1)]
                q = roll(packed, -16 * x, 1)
                if i:
                    v = v * ff[bx, rows, 0:CZ]
                    q = q * ff[bx, rows, CZ:EZ]
                to[bx * CX + x, rows, 0:CZ] = v
                to[bx * CX + x, rows, CZ:EZ] = q


def pooled(s):
    even = iota(s.shape, 0) % 2 == 0
    s = s + jnp.where(even, roll(s, -1, 0), roll(s, 1, 0))
    even = iota(s.shape, 1) % 2 == 0
    return s + jnp.where(even, roll(s, -1, 1), roll(s, 1, 1))


def coef_x(x, kap, cx):
    cx[x] = 0.5 * (kap[x] + kap[x + 1])


def coef_yz(x, kap, cy, cz):
    k = kap[x]
    cy[x] = 0.5 * (k + roll(k, -1, 0))
    cz[x] = 0.5 * (k + roll(k, -1, 1))


def inverse_fine(x, cx, cy, cz, i0, rr, u1, ff):
    f = ff[x >> 3]
    b, c = cy[x], cz[x]
    s = cx[x] + cx[x - 1] + b + roll(b, 1, 0) + c + roll(c, 1, 1)
    v = OMEGA * f / (s + 1.0 - f)
    i0[x] = v
    u1[x] = v * rr[x]


def coarse_cond(i, kap, k1):
    k1[i] = pooled(kap[2 * i] + kap[2 * i + 1]) * 0.125


def pair_step(ps, src, u1, u2, cx, cy, cz, ff, i1):
    faces = [2 * i - 1 for i in ps] + [2 * ps[-1] + 1]
    flux = [cx[x] * (u1[x] - u1[x + 1]) for x in faces]
    for j, i in enumerate(ps):
        x, y = 2 * i, 2 * i + 1
        v, w = u1[x], u1[y]
        gy = cy[x] * (v - roll(v, -1, 0)) + cy[y] * (w - roll(w, -1, 0))
        gz = cz[x] * (v - roll(v, -1, 1)) + cz[y] * (w - roll(w, -1, 1))
        both = (flux[j + 1] - flux[j]) + (gy - roll(gy, 1, 0)) + (gz - roll(gz, 1, 1))
        s = (src[x] + src[y]) - ff[x >> 3] * both
        below = i1[i] * pooled(s)
        u2[x] = u1[x] + below
        u2[y] = u1[y] + below


def inverse_coarse(i, k1, i1, f1, ff):
    k = k1[i]
    f = f1[i >> 2]
    s = k1[i - 1] + k1[i + 1] + roll(k, 2, 0) + roll(k, -2, 0) + roll(k, 2, 1) + roll(k, -2, 1)
    s = 3.0 * k + 0.5 * s
    i1[i] = OMEGA * f / (4.0 * s + 1.0 - f) * ff[i >> 2]


ROW_PARTS = ((0, 0), (8, 0), (16, 1), (24, -1))


def coarse_kernel(
    nx, ny, nz, factor, diagonal, gathered, slab,
    inv, ff, f1, fy, ey_out, ez_out, f_out, sums, e0, kap, rr, cx, cy, cz, i0, k1, i1, u1, u2,
):
    inverse_of(factor, diagonal, inv)
    lane8 = iota((8, CZ), 1)
    lane8f = lane8.astype(F32)
    even8f = (lane8 - lane8 % 2).astype(F32)
    valid = (lane8 < H) | (lane8 >= CZ - H)
    ext = neighbours(table(gathered, 1, nx, ny, nz), nz, ny)
    y0 = neighbours(coarse_solve(inv, table(gathered, 0, nx, ny, nz)), nz, ny)
    for bx in range(3):
        for r, dy in ROW_PARTS:
            e = {dz: jnp.broadcast_to(ext[dy, dz][bx : bx + 1], (8, CZ)) for dz in (-1, 0, 1)}
            v = {dz: jnp.broadcast_to(y0[dy, dz][bx : bx + 1], (8, CZ)) for dz in (-1, 0, 1)}
            far = jnp.where(lane8 < CZ // 2, e[1], e[-1])
            m0 = jnp.where(lane8f < e[0], 1.0, 0.0)
            m1 = jnp.where(valid & (lane8f < far), 1.0, 0.0)
            ff[bx, r : r + 8, 0:CZ] = m0
            ff[bx, r : r + 8, CZ:EZ] = m1
            f1[bx, r : r + 8, 0:CZ] = jnp.where(even8f < e[0], 1.0, 0.0)
            f1[bx, r : r + 8, CZ:EZ] = jnp.where(valid & (even8f < far), 1.0, 0.0)
            fy[bx, r : r + 8, 0:CZ] = m0 * v[0]
            fy[bx, r : r + 8, CZ:EZ] = m1 * jnp.where(lane8 < CZ // 2, v[1], v[-1])


    unpack(slab, 1, kap, rr, ff)
    for x in range(CX, 2 * CX):
        coef_yz(x, kap, cy, cz)
        if x < 2 * CX - 1:
            coef_x(x, kap, cx)
    for x in range(CX + 1, 2 * CX - 1):
        inverse_fine(x, cx, cy, cz, i0, rr, u1, ff)
    for i in range(CX // 2, CX):
        coarse_cond(i, kap, k1)
    for i in range(CX // 2 + 1, CX - 1):
        inverse_coarse(i, k1, i1, f1, ff)
    pair_step([CX // 2 + 1, CX // 2 + 2], rr, u1, u2, cx, cy, cz, ff, i1)
    f_y = ff[1, :, 0:CZ]
    f_z = ff[1, 0:CY]
    own_f = f_z[:, 0:CZ]
    f_out[...] = own_f
    mine_y = jnp.where(iota((EY, CZ), 0) < CY, f_y, 0.0)
    mine_z = jnp.where(iota((CY, EZ), 1) < CZ, f_z, 0.0)
    dif_y = mine_y - roll(mine_y, -1, 0)
    dif_z = mine_z - roll(mine_z, -1, 1)
    up_y = roll(f_y, -1, 0)[0:CY]
    up_z = roll(f_z, -1, 1)[:, 0:CZ]
    row_o = iota((CY, CZ), 0)
    lane_o = iota((CY, CZ), 1)
    s_d = s_y = s_z = jnp.zeros((CY, CZ), F32)
    for x in range(CX):
        b = cy[H + x, :, 0:CZ]
        c = cz[H + x, 0:CY]
        gy = b * dif_y
        gz = c * dif_z
        e = ((gy - roll(gy, 1, 0))[0:CY] + (gz - roll(gz, 1, 1))[:, 0:CZ]) * own_f
        low_y = roll(b * f_y, 1, 0)[0:CY]
        low_z = roll(c * f_z, 1, 1)[:, 0:CZ]
        cut_y = jnp.where(row_o == CY - 1, b[0:CY] * up_y, jnp.where(row_o == 0, low_y, 0.0)) * own_f
        cut_z = jnp.where(lane_o == CZ - 1, c[:, 0:CZ] * up_z, jnp.where(lane_o == 0, low_z, 0.0)) * own_f
        e0[x] = e
        ey_out[x] = cut_y
        ez_out[x] = cut_z
        s_d = s_d + e
        s_y = s_y + cut_y
        s_z = s_z + cut_z
    sums[0] = s_d
    sums[1] = jnp.where(row_o == CY - 1, s_y, 0.0)
    sums[2] = jnp.where(lane_o == CZ - 1, s_z, 0.0)


def main_kernel(
    left, right, ff, f1, fy, sums, *refs
):
    (e0, kap, rr, cx, cy, cz, i0, k1, i1, u1, u2) = refs[11:22]
    (d_out, t_out, n_out, an_out, r_out, ex_out, msg) = refs[22:29]
    dd, tt = refs[29:]
    unpack_message(left, True, 0, kap, rr, ff)
    unpack_message(right, False, 2, kap, rr, ff)
    coef_x(2 * CX - 1, kap, cx)

    def coefs(us):
        for u in us:
            for x in (u, u + 2 * CX):
                coef_yz(x, kap, cy, cz)
            coef_x(u, kap, cx)
            coef_x(jnp.minimum(u + 2 * CX, EX - 2), kap, cx)

    groups(0, CX, coefs)

    def inverses(us):
        for u in us:
            for x in (u, u + 2 * CX - 2):
                inverse_fine(x, cx, cy, cz, i0, rr, u1, ff)

    groups(1, CX + 1, inverses)
    for i in range(CX // 2):
        for j in (i, i + CX):
            coarse_cond(j, kap, k1)
    for i in range(1, CX // 2 + 1):
        for j in (i, i + CX - 2):
            inverse_coarse(j, k1, i1, f1, ff)

    def images(u, xs, masked=True):
        c = [u[xs[0] - 1]] + [u[x] for x in xs] + [u[xs[-1] + 1]]
        flux = [cx[x] * (c[i] - c[i + 1]) for i, x in enumerate([xs[0] - 1] + list(xs))]
        out = []
        for i, x in enumerate(xs):
            v = c[i + 1]
            gy = cy[x] * (v - roll(v, -1, 0))
            gz = cz[x] * (v - roll(v, -1, 1))
            w = (flux[i + 1] - flux[i]) + (gy - roll(gy, 1, 0)) + (gz - roll(gz, 1, 1))
            out.append(ff[x >> 3] * w if masked else w)
        return out

    def smooth(src, run_pairs, out_range, put):
        run_pairs()

        def last(xs):
            for x, w in zip(xs, images(u2, xs, False)):
                put(x, u2[x] + i0[x] * (src[x] - w))

        groups(*out_range, last)

    def put_d(x, v):
        dd[x] = v + fy[x >> 3]

    def outer(us):
        for skip in (0, CX // 2 + 2):
            pair_step([u + skip for u in us], rr, u1, u2, cx, cy, cz, ff, i1)

    smooth(rr, lambda: groups(1, CX // 2 + 1, outer), (3, EX - 3), put_d)

    def apply(xs):
        for x, w in zip(xs, images(dd, xs)):
            tt[x] = w
            u1[x] = i0[x] * w

    groups(4, EX - 4, apply)
    for x in range(CX):
        d_out[x] = dd[H + x, 0:CY, 0:CZ]

    def put_n(x, v):
        dd[x] = v

    zero = jnp.zeros((CY, CZ), F32)
    s_rz, s_dad = zero, zero
    for x in range(CX):
        s_rz = s_rz + rr[H + x, 0:CY, 0:CZ] * d_out[x]
        s_dad = s_dad + tt[H + x, 0:CY, 0:CZ] * d_out[x]
    def inner(ps):
        pair_step(ps, tt, u1, u2, cx, cy, cz, ff, i1)

    smooth(tt, lambda: groups(3, EX // 2 - 3, inner), (7, EX - 7), put_n)
    s_x, s_y, s_tau, s_om = (zero,) * 4
    own_f = ff[1, 0:CY, 0:CZ]
    image_n = images(dd, list(range(H, H + CX)))
    for x in range(CX):
        at = H + x
        an = image_n[x][0:CY, 0:CZ]
        n = dd[at, 0:CY, 0:CZ]
        t = tt[at, 0:CY, 0:CZ]
        an_out[x] = an
        n_out[x] = n
        t_out[x] = t
        r_out[x] = rr[at, 0:CY, 0:CZ]
        s_x = s_x + t * n
        s_y = s_y + n * an
        s_tau = s_tau + t
        s_om = s_om + an
    side0 = cx[H - 1, 0:CY, 0:CZ] * own_f
    side1 = cx[H + CX - 1, 0:CY, 0:CZ] * own_f
    e0[0] = e0[0] + side0
    e0[CX - 1] = e0[CX - 1] + side1
    ex0 = side0 * ff[0, 0:CY, 0:CZ]
    ex1 = side1 * ff[2, 0:CY, 0:CZ]
    ex_out[0] = ex0
    ex_out[1] = ex1
    at = iota((1, CZ), 1)
    z = lax.axis_index("gz")
    vectors = (s_tau, s_om, sums[0] + side0 + side1, ex1, sums[1], sums[2])
    line = jnp.zeros((1, CZ), F32)
    for i, v in enumerate(vectors):
        line = line + jnp.where(at == SLOT * i + z, total(v), 0.0)
    for i, v in enumerate((s_rz, s_dad, s_x, s_y)):
        line = line + jnp.where(at == 6 * SLOT + i, total(v), 0.0)
    msg[...] = jnp.broadcast_to(line[None], msg.shape)


def final_kernel(nx, ny, nz, gathered, inv, d_in, t_in, n_in, an_in, r_in, e0, ey, ez, ex, f_in, sol, res):
    vectors = [table(gathered, i, nx, ny, nz) for i in range(6)]
    tables = list(zip(*vectors))
    sums = jnp.sum(gathered[...], axis=0)
    at = iota((1, CZ), 1)

    def scalar(i):
        return jnp.sum(jnp.where(at == 6 * SLOT + i, sums, 0.0), axis=1, keepdims=True)

    rz, dad, xx, yy = (scalar(i) for i in range(4))
    tau = vectors[0]
    yt = coarse_solve(inv, [v * (1.0 / CELLS) for v in tau])
    add_x = jnp.zeros((1, CZ), F32)
    add_y = jnp.zeros((1, CZ), F32)
    for x in range(nx):
        y = yt[x]
        t = tables[x]
        add_x = add_x + t[0] * y
        cross = t[4] * roll(y, -nz, 1) + t[5] * roll(y, -1, 1)
        if x + 1 < nx:
            cross = cross + t[3] * yt[x + 1]
        add_y = add_y + y * (2.0 * t[1] + t[2] * y - 2.0 * cross)
    xx = xx + jnp.sum(add_x, axis=1, keepdims=True)
    yy = yy + jnp.sum(add_y, axis=1, keepdims=True)
    a0 = rz / dad
    new = a0 * a0 * xx - rz
    beta = new / rz
    zaz = dad - 2.0 * a0 * xx + a0 * a0 * yy
    a1 = new / (zaz - beta * beta * dad)
    near = neighbours(yt, nz, ny)
    shape = (CY, CZ)

    def wide(v, bx=1):
        return jnp.broadcast_to(v[bx : bx + 1], shape)

    y_own = wide(near[0, 0])
    y_y = jnp.where(iota(shape, 0) < CY // 2, wide(near[-1, 0]), wide(near[1, 0]))
    y_z = jnp.where(iota(shape, 1) < CZ // 2, wide(near[0, -1]), wide(near[0, 1]))
    f = f_in[...]
    c_d = jnp.broadcast_to(a0 + a1 * (1.0 + beta), shape)
    c_n = jnp.broadcast_to(a0 * a1, shape)
    for x in range(CX):
        n = n_in[x] + f * y_own
        an = an_in[x] + e0[x] * y_own - ey[x] * y_y - ez[x] * y_z
        if x == 0:
            an = an - ex[0] * wide(near[0, 0], 0)
        if x == CX - 1:
            an = an - ex[1] * wide(near[0, 0], 2)
        sol[x] = c_d * d_in[x] - c_n * n
        res[x] = r_in[x] - c_d * t_in[x] + c_n * an


def exchange(axis, to_low, to_high):
    size = lax.axis_size(axis)
    up = [(i, i + 1) for i in range(size - 1)]
    down = [(b, a) for a, b in up]
    return lax.ppermute(to_low, axis, down), lax.ppermute(to_high, axis, up)


def on_device(right_side, conductance, extents, coarse_factor):
    nx, ny, nz = (lax.axis_size(a) for a in ("gx", "gy", "gz"))
    sizes = (nx, ny, nz)
    any_space = pl.BlockSpec(memory_space=pl.ANY)
    msg = call(pack_kernel, [(nz, CY, CZ)], 3, name="pack", mib=PACK_MIB)(extents, right_side, conductance)[0]
    got = lax.all_to_all(msg, "gz", 0, 0, tiled=True)
    depth = 2 * CX + 2
    zh, to_low, to_high, line = call(
        rows_kernel, [(2, CY, CZ), (depth, H, CZ), (depth, H, CZ), (nx * ny, 1, CZ)], 3, name="rows"
    )(right_side, conductance, got)
    first = lax.all_to_all(line, ("gx", "gy"), 0, 0, tiled=True)
    y_high, y_low = exchange("gy", to_low, to_high)
    slab, to_low, to_high = call(
        slab_kernel, [(depth, EY, CZ)] + [(X_TILES, 8, CZ)] * 2, 6, in_specs=[VMEM] * 5 + [any_space], name="slab"
    )(right_side, conductance, zh, y_high, y_low, first)
    to_low, to_high, factor = lax.optimization_barrier((to_low, to_high, coarse_factor))
    nb = factor.shape[0] // CZ
    diagonal = call(diagonal_kernel, [(nb, CZ, CZ)], 1, name="diagonal")(factor)[0]
    x_high, x_low = exchange("gx", to_low, to_high)
    block = (CX, CY, CZ)
    wide = (EX, EY, EZ)
    half = (EX // 2, EY, EZ)
    third = (3, EY, EZ)
    arrays = [block] + [wide] * 6 + [half] * 2 + [wide] * 2
    inv, ff, f1, fy, ey, ez, fluid, sums, *fields = call(
        functools.partial(coarse_kernel, *sizes),
        [factor.shape] + [third] * 3 + [block] * 2 + [(CY, CZ), (3, CY, CZ)] + arrays, 4, name="coarse",
    )(factor, diagonal, first, slab)
    e0, *outs = call(
        main_kernel,
        arrays + [block] * 5 + [(2, CY, CZ), (nz, 1, CZ)],
        17,
        scratch=[wide] * 2,
        aliases={6 + i: i for i in range(11)},
        name="fields",
    )(x_low, x_high, ff, f1, fy, sums, *fields)
    d0, t0, n0, an0, r0, ex, msg = outs[10:]
    part = lax.all_to_all(msg, "gz", 0, 0, tiled=True)
    line = call(sum_kernel, [(nx * ny, 1, CZ)], 1, name="sum")(part)[0]
    second = lax.all_to_all(line, ("gx", "gy"), 0, 0, tiled=True)
    sol, res = call(functools.partial(final_kernel, *sizes), [block] * 2, 12, name="final")(
        second, inv, d0, t0, n0, an0, r0, e0, ey, ez, ex, fluid
    )
    return sol, res


def solution(mesh):
    spec = P("gx", "gy", "gz")
    return jax.shard_map(
        on_device, mesh=mesh, in_specs=(spec, spec, spec, P()), out_specs=(spec, spec), check_vma=False
    )
```

```python
import functools

import jax
import jax.numpy as jnp
from jax import lax
from jax.experimental import pallas as pl
from jax.experimental.pallas import tpu as pltpu
from jax.sharding import PartitionSpec as P

F32 = jnp.float32
PACK_MIB = 48
OMEGA = 0.8
CX, CY, CZ = 8, 16, 128
CELLS = CX * CY * CZ
H = 8
EX, EY, EZ = CX + 2 * H, CY + 2 * H, 2 * CZ
SLOT = 16
VMEM = pl.BlockSpec(memory_space=pltpu.VMEM)
SMEM = pl.BlockSpec(memory_space=pltpu.SMEM)


def call(kernel, out_shapes, n_in, scratch=(), in_specs=None, name=None, aliases=None, mib=24):
    outs = [jax.ShapeDtypeStruct(s, F32) for s in out_shapes]
    return pl.pallas_call(
        kernel,
        out_shape=outs,
        in_specs=in_specs or [VMEM] * n_in,
        out_specs=[VMEM] * len(outs),
        scratch_shapes=[pltpu.VMEM(s, F32) for s in scratch],
        input_output_aliases=aliases or {},
        compiler_params=pltpu.CompilerParams(vmem_limit_bytes=mib * 1024 * 1024),
        name=name,
    )


def roll(x, shift, axis):
    return pltpu.roll(x, shift % x.shape[axis], axis)


def iota(shape, dim):
    return lax.broadcasted_iota(jnp.int32, shape, dim)


def total(x):
    return jnp.sum(jnp.sum(x, axis=0, keepdims=True), axis=1, keepdims=True)


def pack_kernel(ext, rhs, cond, msg):
    nz = msg.shape[0]
    lane = iota((CY, CZ), 1)
    row = iota((CY, CZ), 0)
    a = jnp.zeros((CY, CZ), F32)
    b = jnp.zeros((CY, CZ), F32)
    acc = jnp.zeros((CY, CZ), F32)
    count = jnp.broadcast_to(ext[0], (CY, CZ))
    inside = lane < count
    z = lax.axis_index("gz")
    for x in range(CX):
        k = cond[x]
        r = rhs[x]
        acc = acc + jnp.where(inside, r, 0.0)
        hi = (lane >= 16 * x) & (lane < 16 * x + H)
        start = (16 * x - H) % CZ
        lo = (lane >= start) & (lane < start + H)
        a = jnp.where(hi, roll(k, 16 * x, 1), jnp.where(lo, roll(r, 16 * x - H, 1), a))
        b = jnp.where(lo, roll(k, 16 * x, 1), jnp.where(hi, roll(r, 16 * x + H, 1), b))
    info = jnp.where(row == 0, total(acc) / CELLS, count.astype(F32))
    a = jnp.where((lane == CZ - 1) & (row < 2), info, a)
    b = jnp.where((lane == 0) & (row < 2), info, b)
    for i in range(nz):
        msg[i] = b

    @pl.when(z > 0)
    def _():
        msg[z - 1] = a


def rows_kernel(rhs, cond, got, zh, to_low, to_high, line):
    nz = got.shape[0]
    z = lax.axis_index("gz")
    low_half = iota((CY, CZ), 1) % 16 < H
    up = jnp.minimum(z + 1, nz - 1)
    a = jnp.where(jnp.full((CY, CZ), z, jnp.int32) < nz - 1, got[up], 0.0)
    b = jnp.where(jnp.full((CY, CZ), z, jnp.int32) > 0, got[jnp.maximum(z - 1, 0)], 0.0)
    lane = iota((8, CZ), 1)
    info = jnp.zeros((8, CZ), F32)
    for i in range(nz):
        v = got[i, 0:8]
        info = jnp.where(lane == i, roll(v, i, 1), info)
    info = jnp.where(lane == z + 1, pltpu.roll(a[0:8], z + 2, 1), info)
    info = jnp.where(lane < nz, info, 0.0)
    line[...] = jnp.broadcast_to((info[0:1] + roll(info[1:2], SLOT, 1))[None], line.shape)
    zk = jnp.where(low_half, a, b)
    zr = jnp.where(low_half, roll(a, H, 1), roll(b, -H, 1))
    zh[0] = zk
    zh[1] = zr
    to_low[0:CX] = cond[:, 0:H, :]
    to_low[CX : 2 * CX] = rhs[:, 0:H, :]
    to_low[2 * CX] = zk[0:H]
    to_low[2 * CX + 1] = zr[0:H]
    to_high[0:CX] = cond[:, CY - H : CY, :]
    to_high[CX : 2 * CX] = rhs[:, CY - H : CY, :]
    to_high[2 * CX] = zk[CY - H : CY]
    to_high[2 * CX + 1] = zr[CY - H : CY]


def x_tiles():
    at = 0
    cond, rhs = {}, {}
    for layer in range(1, H + 1):
        for part, whole, none in ((cond, 5, 9), (rhs, 4, 8)):
            n = 4 if layer <= whole else 3 if layer < none else 0
            part[layer] = (at, n)
            at += n
    return cond, rhs, at


X_TILES = x_tiles()[2] + 8


def slab_kernel(rhs, cond, zh, from_high, from_low, after, slab, to_low, to_high):
    slab[0:CX, 0:CY] = cond[...]
    slab[CX : 2 * CX, 0:CY] = rhs[...]
    slab[2 * CX : 2 * CX + 2, 0:CY] = zh[...]
    slab[:, CY : CY + H] = from_high[...]
    slab[:, CY + H : EY] = from_low[...]
    in_cond, in_rhs, z_at = x_tiles()
    near = iota((8, CZ), 0) < 4
    for msg, flip in ((to_low, False), (to_high, True)):
        for x in range(CX):
            layer = H - x if flip else x + 1
            for part, base, src in ((in_cond, 0, cond), (in_rhs, CX, rhs)):
                at, n = part[layer]
                if n == 0:
                    continue
                msg[at] = src[x, 0:8]
                msg[at + 1] = src[x, 8:16]
                high, low = from_high[base + x], from_low[base + x]
                if n == 4:
                    msg[at + 2] = high
                    msg[at + 3] = low
                else:
                    msg[at + 2] = jnp.where(near, high, low)
        for i in range(2):
            at = z_at + 4 * i
            msg[at] = zh[i, 0:8]
            msg[at + 1] = zh[i, 8:16]
            msg[at + 2] = from_high[2 * CX + i]
            msg[at + 3] = from_low[2 * CX + i]


def sum_kernel(part, line):
    line[...] = jnp.broadcast_to(jnp.sum(part[...], axis=0, keepdims=True), line.shape)


def table(rows, i, nx, ny, nz):
    out = []
    for x in range(nx):
        v = rows[x * ny : (x + 1) * ny].reshape(ny, CZ)
        v = jnp.where(iota((ny, CZ), 1) < nz, roll(v, -SLOT * i, 1), 0.0)
        v = pltpu.roll(v, 0, 1, stride=nz, stride_axis=0)
        out.append(jnp.sum(v, axis=0, keepdims=True))
    return out


def dot(a, b):
    return jnp.dot(a, b, precision=lax.Precision.HIGHEST, preferred_element_type=F32)


def diagonal_kernel(factor, out):
    n = factor.shape[0]
    bs = CZ
    nb = n // bs
    i = iota((bs, bs), 0)
    j = iota((bs, bs), 1)
    eye = i == j
    low = [factor[b * bs : (b + 1) * bs, b * bs : (b + 1) * bs].astype(F32) for b in range(nb)]
    inv = []
    for lb in low:
        diag = jnp.where(eye, lb, 0.0)
        col = 1.0 / jnp.sum(diag, axis=1, keepdims=True)
        row = 1.0 / jnp.sum(diag, axis=0, keepdims=True)
        pair = (i // 2 == j // 2) & (i > j)
        inv.append(jnp.where(eye, col, 0.0) - jnp.where(pair, col * lb * row, 0.0))
    s = 2
    while s < bs:
        mask = (i // (2 * s) == j // (2 * s)) & (i // s > j // s)
        mid = [dot(jnp.where(mask, lb, 0.0), x) for lb, x in zip(low, inv)]
        inv = [x - dot(x, m) for x, m in zip(inv, mid)]
        s *= 2
    for b in range(nb):
        out[b] = inv[b]


def inverse_of(factor, diagonal, out):
    n = factor.shape[0]
    bs = CZ
    for b in range(n // bs):
        out[b * bs : (b + 1) * bs, b * bs : (b + 1) * bs] = diagonal[b]
    s = bs
    while s < n:
        for at in range(0, n, 2 * s):
            for lo in range(s, 2 * s, bs):
                for hi in range(lo - s + bs, s, bs):
                    out[at + lo - s : at + lo - s + bs, at + hi : at + hi + bs] = jnp.zeros((bs, bs), F32)
            if s > bs:
                for lo in range(s, 2 * s, bs):
                    for hi in range(lo + bs, 2 * s, bs):
                        out[at + lo : at + lo + bs, at + hi : at + hi + bs] = jnp.zeros((bs, bs), F32)
            mid = dot(factor[at + s : at + 2 * s, at : at + s].astype(F32), out[at : at + s, at : at + s])
            out[at + s : at + 2 * s, at : at + s] = -dot(out[at + s : at + 2 * s, at + s : at + 2 * s], mid)
        s *= 2


def coarse_solve(inv, means):
    nb = len(means)
    bs = CZ
    rows = [jnp.zeros((1, bs), F32) for _ in range(nb)]
    for a in range(nb):
        acc = inv[a * bs : (a + 1) * bs, 0:bs] * means[0]
        for c in range(1, a + 1):
            acc = acc + inv[a * bs : (a + 1) * bs, c * bs : (c + 1) * bs] * means[c]
        u = jnp.sum(acc, axis=1, keepdims=True)
        for c in range(a + 1):
            rows[c] = rows[c] + jnp.sum(inv[a * bs : (a + 1) * bs, c * bs : (c + 1) * bs] * u, axis=0, keepdims=True)
    return rows


def neighbours(rows, nz, ny):
    nx = len(rows)
    x = lax.axis_index("gx")
    y = lax.axis_index("gy")
    z = lax.axis_index("gz")
    zero = jnp.zeros((1, CZ), F32)
    picked = []
    for dx in (-1, 0, 1):
        v = zero
        for r in range(nx):
            v = v + jnp.where(jnp.full((1, CZ), x + dx, jnp.int32) == r, rows[r], 0.0)
        picked.append(v)
    row = iota((8, CZ), 0)
    stack = jnp.where(row == 0, picked[0], jnp.where(row == 1, picked[1], jnp.where(row == 2, picked[2], 0.0)))
    lane = iota((8, CZ), 1)
    out = {}
    for dy in (-1, 0, 1):
        for dz in (-1, 0, 1):
            ok = (y + dy >= 0) & (y + dy < ny) & (z + dz >= 0) & (z + dz < nz)
            target = jnp.where(ok, (y + dy) * nz + z + dz, -1)
            out[dy, dz] = jnp.sum(jnp.where(lane == target, stack, 0.0), axis=1, keepdims=True)
    return out


def groups(low, high, body, step=1):
    count = high - low
    size = max(u for u in range(1, count // 2 + 1) if count % u == 0)

    def go(i, carry):
        body([low + i * size + u for u in range(size)])
        return carry

    lax.fori_loop(0, count // size, go, 0)


def unpack(src, bx, kap, rr, ff):
    for x in range(CX):
        at = bx * CX + x
        kap[at, :, 0:CZ] = src[x]
        kap[at, :, CZ:EZ] = roll(src[2 * CX], -16 * x, 1)
        rr[at, :, 0:CZ] = src[CX + x] * ff[bx, :, 0:CZ]
        rr[at, :, CZ:EZ] = roll(src[2 * CX + 1], -16 * x, 1) * ff[bx, :, CZ:EZ]


def unpack_message(msg, flip, bx, kap, rr, ff):
    in_cond, in_rhs, z_at = x_tiles()
    for tile in range(4):
        rows = slice(8 * tile, 8 * tile + 8)
        for part, to, i in ((in_cond, kap, 0), (in_rhs, rr, 1)):
            packed = msg[z_at + 4 * i + tile]
            for x in range(CX):
                at, n = part[H - x if flip else x + 1]
                if n == 0:
                    continue
                v = msg[at + min(tile, n - 1)]
                q = roll(packed, -16 * x, 1)
                if i:
                    v = v * ff[bx, rows, 0:CZ]
                    q = q * ff[bx, rows, CZ:EZ]
                to[bx * CX + x, rows, 0:CZ] = v
                to[bx * CX + x, rows, CZ:EZ] = q


def pooled(s):
    even = iota(s.shape, 0) % 2 == 0
    s = s + jnp.where(even, roll(s, -1, 0), roll(s, 1, 0))
    even = iota(s.shape, 1) % 2 == 0
    return s + jnp.where(even, roll(s, -1, 1), roll(s, 1, 1))


def coef_x(x, kap, cx):
    cx[x] = 0.5 * (kap[x] + kap[x + 1])


def coef_yz(x, kap, cy, cz):
    k = kap[x]
    cy[x] = 0.5 * (k + roll(k, -1, 0))
    cz[x] = 0.5 * (k + roll(k, -1, 1))


def inverse_fine(x, cx, cy, cz, i0, rr, u1, ff):
    f = ff[x >> 3]
    b, c = cy[x], cz[x]
    s = cx[x] + cx[x - 1] + b + roll(b, 1, 0) + c + roll(c, 1, 1)
    v = OMEGA * f / (s + 1.0 - f)
    i0[x] = v
    u1[x] = v * rr[x]


def coarse_cond(i, kap, k1):
    k1[i] = pooled(kap[2 * i] + kap[2 * i + 1]) * 0.125


def inverse_coarse(i, k1, i1, f1, ff):
    k = k1[i]
    f = f1[i >> 2]
    s = k1[i - 1] + k1[i + 1] + roll(k, 2, 0) + roll(k, -2, 0) + roll(k, 2, 1) + roll(k, -2, 1)
    s = 3.0 * k + 0.5 * s
    i1[i] = OMEGA * f / (4.0 * s + 1.0 - f) * ff[i >> 2]


ROW_PARTS = ((0, 0), (8, 0), (16, 1), (24, -1))


def coarse_kernel(
    nx, ny, nz, factor, diagonal, gathered, slab,
    inv, ff, f1, fy, ey_out, ez_out, f_out, sums, e0, kap, rr, cx, cy, cz, i0, k1, i1, u1,
):
    inverse_of(factor, diagonal, inv)
    lane8 = iota((8, CZ), 1)
    lane8f = lane8.astype(F32)
    even8f = (lane8 - lane8 % 2).astype(F32)
    valid = (lane8 < H) | (lane8 >= CZ - H)
    ext = neighbours(table(gathered, 1, nx, ny, nz), nz, ny)
    y0 = neighbours(coarse_solve(inv, table(gathered, 0, nx, ny, nz)), nz, ny)
    for bx in range(3):
        for r, dy in ROW_PARTS:
            e = {dz: jnp.broadcast_to(ext[dy, dz][bx : bx + 1], (8, CZ)) for dz in (-1, 0, 1)}
            v = {dz: jnp.broadcast_to(y0[dy, dz][bx : bx + 1], (8, CZ)) for dz in (-1, 0, 1)}
            far = jnp.where(lane8 < CZ // 2, e[1], e[-1])
            m0 = jnp.where(lane8f < e[0], 1.0, 0.0)
            m1 = jnp.where(valid & (lane8f < far), 1.0, 0.0)
            ff[bx, r : r + 8, 0:CZ] = m0
            ff[bx, r : r + 8, CZ:EZ] = m1
            f1[bx, r : r + 8, 0:CZ] = jnp.where(even8f < e[0], 1.0, 0.0)
            f1[bx, r : r + 8, CZ:EZ] = jnp.where(valid & (even8f < far), 1.0, 0.0)
            fy[bx, r : r + 8, 0:CZ] = m0 * v[0]
            fy[bx, r : r + 8, CZ:EZ] = m1 * jnp.where(lane8 < CZ // 2, v[1], v[-1])


    unpack(slab, 1, kap, rr, ff)
    for x in range(CX, 2 * CX):
        coef_yz(x, kap, cy, cz)
        if x < 2 * CX - 1:
            coef_x(x, kap, cx)
    for x in range(CX + 1, 2 * CX - 1):
        inverse_fine(x, cx, cy, cz, i0, rr, u1, ff)
    for i in range(CX // 2, CX):
        coarse_cond(i, kap, k1)
    for i in range(CX // 2 + 1, CX - 1):
        inverse_coarse(i, k1, i1, f1, ff)
    f_y = ff[1, :, 0:CZ]
    f_z = ff[1, 0:CY]
    own_f = f_z[:, 0:CZ]
    f_out[...] = own_f
    mine_y = jnp.where(iota((EY, CZ), 0) < CY, f_y, 0.0)
    mine_z = jnp.where(iota((CY, EZ), 1) < CZ, f_z, 0.0)
    dif_y = mine_y - roll(mine_y, -1, 0)
    dif_z = mine_z - roll(mine_z, -1, 1)
    up_y = roll(f_y, -1, 0)[0:CY]
    up_z = roll(f_z, -1, 1)[:, 0:CZ]
    row_o = iota((CY, CZ), 0)
    lane_o = iota((CY, CZ), 1)
    s_d = s_y = s_z = jnp.zeros((CY, CZ), F32)
    for x in range(CX):
        b = cy[H + x, :, 0:CZ]
        c = cz[H + x, 0:CY]
        gy = b * dif_y
        gz = c * dif_z
        e = ((gy - roll(gy, 1, 0))[0:CY] + (gz - roll(gz, 1, 1))[:, 0:CZ]) * own_f
        low_y = roll(b * f_y, 1, 0)[0:CY]
        low_z = roll(c * f_z, 1, 1)[:, 0:CZ]
        cut_y = jnp.where(row_o == CY - 1, b[0:CY] * up_y, jnp.where(row_o == 0, low_y, 0.0)) * own_f
        cut_z = jnp.where(lane_o == CZ - 1, c[:, 0:CZ] * up_z, jnp.where(lane_o == 0, low_z, 0.0)) * own_f
        e0[x] = e
        ey_out[x] = cut_y
        ez_out[x] = cut_z
        s_d = s_d + e
        s_y = s_y + cut_y
        s_z = s_z + cut_z
    sums[0] = s_d
    sums[1] = jnp.where(row_o == CY - 1, s_y, 0.0)
    sums[2] = jnp.where(lane_o == CZ - 1, s_z, 0.0)


def main_kernel(
    left, right, ff, f1, fy, sums, *refs
):
    (e0, kap, rr, cx, cy, cz, i0, k1, i1, u1) = refs[10:20]
    (d_out, t_out, n_out, an_out, r_out, ex_out, msg) = refs[20:27]
    u2, dd, tt = refs[27:]
    unpack_message(left, True, 0, kap, rr, ff)
    unpack_message(right, False, 2, kap, rr, ff)
    coef_x(2 * CX - 1, kap, cx)

    def coefs(us):
        for u in us:
            for x in (u, u + 2 * CX):
                coef_yz(x, kap, cy, cz)
            coef_x(u, kap, cx)
            coef_x(jnp.minimum(u + 2 * CX, EX - 2), kap, cx)

    groups(0, CX, coefs)

    def inverses(us):
        for u in us:
            for x in (u, u + 2 * CX - 2):
                inverse_fine(x, cx, cy, cz, i0, rr, u1, ff)

    groups(1, CX + 1, inverses)
    for i in range(CX // 2):
        for j in (i, i + CX):
            coarse_cond(j, kap, k1)
    for i in range(1, CX // 2 + 1):
        for j in (i, i + CX - 2):
            inverse_coarse(j, k1, i1, f1, ff)

    def images(u, xs, masked=True):
        c = [u[xs[0] - 1]] + [u[x] for x in xs] + [u[xs[-1] + 1]]
        flux = [cx[x] * (c[i] - c[i + 1]) for i, x in enumerate([xs[0] - 1] + list(xs))]
        out = []
        for i, x in enumerate(xs):
            v = c[i + 1]
            gy = cy[x] * (v - roll(v, -1, 0))
            gz = cz[x] * (v - roll(v, -1, 1))
            w = (flux[i + 1] - flux[i]) + (gy - roll(gy, 1, 0)) + (gz - roll(gz, 1, 1))
            out.append(ff[x >> 3] * w if masked else w)
        return out

    def smooth(src, pair_range, out_range, put):
        def pairs(ps):
            faces = [2 * i - 1 for i in ps] + [2 * ps[-1] + 1]
            flux = [cx[x] * (u1[x] - u1[x + 1]) for x in faces]
            for j, i in enumerate(ps):
                x, y = 2 * i, 2 * i + 1
                v, w = u1[x], u1[y]
                gy = cy[x] * (v - roll(v, -1, 0)) + cy[y] * (w - roll(w, -1, 0))
                gz = cz[x] * (v - roll(v, -1, 1)) + cz[y] * (w - roll(w, -1, 1))
                both = (flux[j + 1] - flux[j]) + (gy - roll(gy, 1, 0)) + (gz - roll(gz, 1, 1))
                s = (src[x] + src[y]) - ff[x >> 3] * both
                below = i1[i] * pooled(s)
                u2[x] = u1[x] + below
                u2[y] = u1[y] + below

        groups(*pair_range, pairs)

        def last(xs):
            for x, w in zip(xs, images(u2, xs, False)):
                put(x, u2[x] + i0[x] * (src[x] - w))

        groups(*out_range, last)

    def put_d(x, v):
        dd[x] = v + fy[x >> 3]

    smooth(rr, (1, EX // 2 - 1), (3, EX - 3), put_d)

    def apply(xs):
        for x, w in zip(xs, images(dd, xs)):
            tt[x] = w
            u1[x] = i0[x] * w

    groups(4, EX - 4, apply)
    for x in range(CX):
        d_out[x] = dd[H + x, 0:CY, 0:CZ]

    def put_n(x, v):
        dd[x] = v

    zero = jnp.zeros((CY, CZ), F32)
    s_rz, s_dad = zero, zero
    for x in range(CX):
        s_rz = s_rz + rr[H + x, 0:CY, 0:CZ] * d_out[x]
        s_dad = s_dad + tt[H + x, 0:CY, 0:CZ] * d_out[x]
    smooth(tt, (3, EX // 2 - 3), (7, EX - 7), put_n)
    s_x, s_y, s_tau, s_om = (zero,) * 4
    own_f = ff[1, 0:CY, 0:CZ]
    image_n = images(dd, list(range(H, H + CX)))
    for x in range(CX):
        at = H + x
        an = image_n[x][0:CY, 0:CZ]
        n = dd[at, 0:CY, 0:CZ]
        t = tt[at, 0:CY, 0:CZ]
        an_out[x] = an
        n_out[x] = n
        t_out[x] = t
        r_out[x] = rr[at, 0:CY, 0:CZ]
        s_x = s_x + t * n
        s_y = s_y + n * an
        s_tau = s_tau + t
        s_om = s_om + an
    side0 = cx[H - 1, 0:CY, 0:CZ] * own_f
    side1 = cx[H + CX - 1, 0:CY, 0:CZ] * own_f
    e0[0] = e0[0] + side0
    e0[CX - 1] = e0[CX - 1] + side1
    ex0 = side0 * ff[0, 0:CY, 0:CZ]
    ex1 = side1 * ff[2, 0:CY, 0:CZ]
    ex_out[0] = ex0
    ex_out[1] = ex1
    at = iota((1, CZ), 1)
    z = lax.axis_index("gz")
    vectors = (s_tau, s_om, sums[0] + side0 + side1, ex1, sums[1], sums[2])
    line = jnp.zeros((1, CZ), F32)
    for i, v in enumerate(vectors):
        line = line + jnp.where(at == SLOT * i + z, total(v), 0.0)
    for i, v in enumerate((s_rz, s_dad, s_x, s_y)):
        line = line + jnp.where(at == 6 * SLOT + i, total(v), 0.0)
    msg[...] = jnp.broadcast_to(line[None], msg.shape)


def final_kernel(nx, ny, nz, gathered, inv, d_in, t_in, n_in, an_in, r_in, e0, ey, ez, ex, f_in, sol, res):
    vectors = [table(gathered, i, nx, ny, nz) for i in range(6)]
    tables = list(zip(*vectors))
    sums = jnp.sum(gathered[...], axis=0)
    at = iota((1, CZ), 1)

    def scalar(i):
        return jnp.sum(jnp.where(at == 6 * SLOT + i, sums, 0.0), axis=1, keepdims=True)

    rz, dad, xx, yy = (scalar(i) for i in range(4))
    tau = vectors[0]
    yt = coarse_solve(inv, [v * (1.0 / CELLS) for v in tau])
    add_x = jnp.zeros((1, CZ), F32)
    add_y = jnp.zeros((1, CZ), F32)
    for x in range(nx):
        y = yt[x]
        t = tables[x]
        add_x = add_x + t[0] * y
        cross = t[4] * roll(y, -nz, 1) + t[5] * roll(y, -1, 1)
        if x + 1 < nx:
            cross = cross + t[3] * yt[x + 1]
        add_y = add_y + y * (2.0 * t[1] + t[2] * y - 2.0 * cross)
    xx = xx + jnp.sum(add_x, axis=1, keepdims=True)
    yy = yy + jnp.sum(add_y, axis=1, keepdims=True)
    a0 = rz / dad
    new = a0 * a0 * xx - rz
    beta = new / rz
    zaz = dad - 2.0 * a0 * xx + a0 * a0 * yy
    a1 = new / (zaz - beta * beta * dad)
    near = neighbours(yt, nz, ny)
    shape = (CY, CZ)

    def wide(v, bx=1):
        return jnp.broadcast_to(v[bx : bx + 1], shape)

    y_own = wide(near[0, 0])
    y_y = jnp.where(iota(shape, 0) < CY // 2, wide(near[-1, 0]), wide(near[1, 0]))
    y_z = jnp.where(iota(shape, 1) < CZ // 2, wide(near[0, -1]), wide(near[0, 1]))
    f = f_in[...]
    c_d = jnp.broadcast_to(a0 + a1 * (1.0 + beta), shape)
    c_n = jnp.broadcast_to(a0 * a1, shape)
    for x in range(CX):
        n = n_in[x] + f * y_own
        an = an_in[x] + e0[x] * y_own - ey[x] * y_y - ez[x] * y_z
        if x == 0:
            an = an - ex[0] * wide(near[0, 0], 0)
        if x == CX - 1:
            an = an - ex[1] * wide(near[0, 0], 2)
        sol[x] = c_d * d_in[x] - c_n * n
        res[x] = r_in[x] - c_d * t_in[x] + c_n * an


def exchange(axis, to_low, to_high):
    size = lax.axis_size(axis)
    up = [(i, i + 1) for i in range(size - 1)]
    down = [(b, a) for a, b in up]
    return lax.ppermute(to_low, axis, down), lax.ppermute(to_high, axis, up)


def on_device(right_side, conductance, extents, coarse_factor):
    nx, ny, nz = (lax.axis_size(a) for a in ("gx", "gy", "gz"))
    sizes = (nx, ny, nz)
    any_space = pl.BlockSpec(memory_space=pl.ANY)
    msg = call(pack_kernel, [(nz, CY, CZ)], 3, name="pack", mib=PACK_MIB)(extents, right_side, conductance)[0]
    got = lax.all_to_all(msg, "gz", 0, 0, tiled=True)
    depth = 2 * CX + 2
    zh, to_low, to_high, line = call(
        rows_kernel, [(2, CY, CZ), (depth, H, CZ), (depth, H, CZ), (nx * ny, 1, CZ)], 3, name="rows"
    )(right_side, conductance, got)
    first = lax.all_to_all(line, ("gx", "gy"), 0, 0, tiled=True)
    y_high, y_low = exchange("gy", to_low, to_high)
    slab, to_low, to_high = call(
        slab_kernel, [(depth, EY, CZ)] + [(X_TILES, 8, CZ)] * 2, 6, in_specs=[VMEM] * 5 + [any_space], name="slab"
    )(right_side, conductance, zh, y_high, y_low, first)
    to_low, to_high, factor = lax.optimization_barrier((to_low, to_high, coarse_factor))
    nb = factor.shape[0] // CZ
    diagonal = call(diagonal_kernel, [(nb, CZ, CZ)], 1, name="diagonal")(factor)[0]
    x_high, x_low = exchange("gx", to_low, to_high)
    block = (CX, CY, CZ)
    wide = (EX, EY, EZ)
    half = (EX // 2, EY, EZ)
    third = (3, EY, EZ)
    arrays = [block] + [wide] * 6 + [half] * 2 + [wide]
    inv, ff, f1, fy, ey, ez, fluid, sums, *fields = call(
        functools.partial(coarse_kernel, *sizes),
        [factor.shape] + [third] * 3 + [block] * 2 + [(CY, CZ), (3, CY, CZ)] + arrays, 4, name="coarse",
    )(factor, diagonal, first, slab)
    e0, *outs = call(
        main_kernel,
        arrays + [block] * 5 + [(2, CY, CZ), (nz, 1, CZ)],
        16,
        scratch=[wide] * 3,
        aliases={6 + i: i for i in range(10)},
        name="fields",
    )(x_low, x_high, ff, f1, fy, sums, *fields)
    d0, t0, n0, an0, r0, ex, msg = outs[9:]
    part = lax.all_to_all(msg, "gz", 0, 0, tiled=True)
    line = call(sum_kernel, [(nx * ny, 1, CZ)], 1, name="sum")(part)[0]
    second = lax.all_to_all(line, ("gx", "gy"), 0, 0, tiled=True)
    sol, res = call(functools.partial(final_kernel, *sizes), [block] * 2, 12, name="final")(
        second, inv, d0, t0, n0, an0, r0, e0, ey, ez, ex, fluid
    )
    return sol, res


def solution(mesh):
    spec = P("gx", "gy", "gz")
    return jax.shard_map(
        on_device, mesh=mesh, in_specs=(spec, spec, spec, P()), out_specs=(spec, spec), check_vma=False
    )
```
